128 devices in a mesh: group: 4 (over y_hi, core), freq: 32 (over z, x, y_lo).
Axes of the slice: x: 4, y: 4 (y_hi: 2, y_lo: 2; y = y_hi * 2 + y_lo), z: 4, core: 2. Of those that a mesh axis runs over, the one named last changes fastest.
Arguments:
- spectra: bfloat16 [2048, 2, 16], P('freq', None, 'group'), may hold values from -6 to 6
- templates: bfloat16 [2048, 2, 2560], P('freq', None, 'group'), may hold values from -600 to 600
- valid_start: int32 [16], replicated, may hold values from 0 to 2048
Outputs:
- peaks: float32 [2560, 16], P('group')
The draws below stay inside these ranges and needn't reach their ends.
All inputs are finite; a program needn't handle non-finite values.
Results may differ from the reference program's by a relative error of at most 0.0019.
Values may be sent and summed in bfloat16 or wider, within the bound.
A program may use at most 256 MiB of HBM per device.

```python
import math
import jax
import jax.numpy as jnp
from jax import lax

N = 4096
K = 2048
VALID = 2048
SEG = 16
TEMPLATES = 2560


def draw_templates(key, part):
    base_key, row_key, col_key = jax.random.split(jax.random.fold_in(key, 11), 3)
    base = jnp.clip(jax.random.normal(base_key, (K, 2, TEMPLATES), jnp.float32), -6.0, 6.0)
    row_scale = jnp.exp(jax.random.uniform(row_key, (TEMPLATES,), jnp.float32, 0.0, math.log(10.0)))
    col_scale = jnp.exp(jax.random.uniform(col_key, (K,), jnp.float32, 0.0, math.log(10.0)))
    return (base * row_scale[None, None, :] * col_scale[:, None, None]).astype(jnp.bfloat16)


def with_ends(values, own_key, smallest, top_value):
    spot = [jax.random.randint(jax.random.fold_in(own_key, axis), (), 0, length) for axis, length in enumerate(values.shape)]
    widest = values.shape.index(max(values.shape))
    beside = spot[:widest] + [(spot[widest] + 1) % values.shape[widest]] + spot[widest + 1:]
    return values.at[tuple(spot)].set(smallest).at[tuple(beside)].set(top_value)


def steps_of(own_key, extent, cuts, smallest, high):
    factor_of = 1.0
    for position, blocks in cuts:
        heights = jax.random.uniform(jax.random.fold_in(jax.random.fold_in(own_key, 6), position), (blocks,), jnp.float32, smallest / len(cuts), high / len(cuts))
        factor_of = factor_of * jnp.repeat(jnp.exp(heights), extent[position] // blocks).reshape((-1,) + (1,) * (len(extent) - 1 - position))
    return factor_of


def noise(own_key, shape, deviation, most, cuts=(), kind=jnp.bfloat16):
    array = jax.random.normal(own_key, shape, jnp.float32) * deviation
    if len(cuts) > 0:
        array = steps_of(own_key, shape, cuts, -0.22, 0.18) * array
    return jnp.clip(array, min=-most, max=most).astype(kind)


def setup_inputs(seed: int = 0) -> dict:
    seeds = jax.random.split(jax.random.key(seed), 4)
    return {
        "spectra": noise(seeds[0], (K, 2, SEG), 1.0, 6.0, ((0, 32), (2, 4))),
        "templates": draw_templates(jax.random.fold_in(seeds[3], 71), 0),
        "valid_start": with_ends(jax.random.randint(seeds[2], (SEG,), 0, N - VALID + 1), jax.random.fold_in(seeds[2], 1), 0, N - VALID).astype(jnp.int32),
    }


def reference(spectra, templates, valid_start):
    bank = jnp.transpose(templates, (1, 2, 0)).astype(jnp.float32)
    strain_all = jnp.transpose(spectra, (1, 2, 0))
    template_norm = jnp.sum(bank[0] * bank[0] + bank[1] * bank[1], axis=1)
    bins_index = jnp.arange(K, dtype=jnp.int32)
    lag_index = jnp.arange(N, dtype=jnp.int32)
    angle = ((bins_index[:, None] * lag_index[None, :]) % N).astype(jnp.float32) * (2.0 * math.pi / N)
    cosine = jnp.cos(angle)
    sine_part = jnp.sin(angle)
    table = jnp.concatenate([jnp.concatenate([cosine, sine_part], 1), jnp.concatenate([-sine_part, cosine], 1)], 0).astype(jnp.bfloat16)

    def one_segment(segment):
        strain = lax.dynamic_index_in_dim(strain_all, segment, 1, False).astype(jnp.float32)
        cross_re = bank[0] * strain[0][None, :] + bank[1] * strain[1][None, :]
        cross_im = bank[0] * strain[1][None, :] - bank[1] * strain[0][None, :]
        cross = jnp.concatenate([cross_re, cross_im], 1).astype(jnp.bfloat16)
        series = jnp.dot(cross, table, preferred_element_type=jnp.float32)
        power = (series[:, :N] * series[:, :N] + series[:, N:] * series[:, N:]) / template_norm[:, None]
        first = valid_start[segment]
        inside = (lag_index >= first) & (lag_index < first + VALID)
        return jnp.max(jnp.where(inside[None, :], power, jnp.float32(0.0)), axis=1)

    peaks = lax.map(one_segment, jnp.arange(SEG, dtype=jnp.int32))
    return peaks.T
```

```python
import math

import jax
import jax.numpy as jnp
import numpy as np
from jax import lax
from jax.experimental import pallas as pl
from jax.experimental.pallas import tpu as pltpu
from jax.sharding import PartitionSpec as P

N = 4096
VALID = 2048
SIDE = 64
ACROSS = 32
PAIRS = 10
SEGS = 16
MESH = pl.DeviceIdType.MESH
F32 = jnp.float32
BF16 = jnp.bfloat16


def rounded_roots(index):
    exact = np.exp(2j * np.pi * (index % SIDE) / SIDE)
    least = np.full(index.shape[0], np.inf)
    table = np.zeros_like(exact)
    gain = np.ones(index.shape[0])
    for scale in np.linspace(1.0, 2.0, 2001)[:-1]:
        parts = [(x * scale).astype(jnp.bfloat16).astype(np.float64) for x in (exact.real, exact.imag)]
        tried = parts[0] + 1j * parts[1]
        level = (tried * exact.conj()).mean(1).real
        rest = (np.abs(tried / level[:, None] - exact) ** 2).mean(1)
        better = rest < least - 1e-15
        least = np.where(better, rest, least)
        table = np.where(better[:, None], tried, table)
        gain = np.where(better, level, gain)
    return table, gain


def tables():
    side = np.arange(SIDE)
    root, gain = rounded_roots(side[:, None] * np.arange(ACROSS)[None, :])
    first = np.concatenate(
        [np.concatenate([root.real, -root.imag], 1), np.concatenate([root.imag, root.real], 1)], 0
    )
    turn = np.exp(2j * np.pi * side[:, None] * side[None, :] / N) / gain[:, None]
    root, gain = rounded_roots(side[:, None] * side[None, :])
    c, s = np.kron(np.eye(2), root.real.T), np.kron(np.eye(2), root.imag.T)
    second = np.concatenate([np.concatenate([c, s], 1), np.concatenate([-s, c], 1)], 0)
    weight = np.tile(1.0 / gain ** 2, (SIDE, 2))
    turn = np.stack([np.tile(turn.real, (1, 2)), np.tile(turn.imag, (1, 2)), weight], 0)
    return jnp.asarray(first, BF16), jnp.asarray(turn, F32), jnp.asarray(second, BF16)


def kernel(
    start_ref, tpl_hbm, spec_hbm, first_hbm, turn_hbm, second_hbm, out_ref,
    tpl, spec, first, turn, second, rows, mine, got, other, beside, beside2, flat,
    bank, strain, mask, mid, peak, norm, sent, back, wide,
    load_sem, send_sem, recv_sem, recv2_sem, side_sem, side_recv, last_send, last_recv,
):
    g = lax.axis_index("group")
    f = lax.axis_index("freq")
    far = lax.rem(g + 2, 4)
    near = g + 1 - 2 * lax.rem(g, 2)
    count = 32

    loads = [
        pltpu.make_async_copy(src, dst, load_sem.at[i])
        for i, (src, dst) in enumerate(
            [(tpl_hbm, tpl), (spec_hbm, spec), (first_hbm, first), (turn_hbm, turn), (second_hbm, second)]
        )
    ]
    for load in loads:
        load.start()

    barrier = pltpu.get_barrier_semaphore()

    def greet(i, carry):
        to = lax.rem(f + i, count)
        pl.semaphore_signal(barrier, inc=1, device_id=(g, to), device_id_type=MESH)
        return carry

    def greet_far(i, carry):
        to = lax.rem(f + i, count)
        pl.semaphore_signal(barrier, inc=1, device_id=(far, to), device_id_type=MESH)
        return carry

    lax.fori_loop(1, count, greet, 0)
    lax.fori_loop(0, count, greet_far, 0)
    pl.semaphore_signal(barrier, inc=1, device_id=(near, f), device_id_type=MESH)

    for load in loads:
        load.wait()

    peak[...] = jnp.zeros_like(peak)
    norm[...] = jnp.ones_like(norm)

    for j in range(5):
        block = jnp.concatenate(
            [tpl[0, :, 128 * j:128 * (j + 1)].astype(F32), tpl[1, :, 128 * j:128 * (j + 1)].astype(F32)], 0
        )
        rows[128 * j:128 * (j + 1), :] = block.T
    own = jnp.concatenate([spec[0].astype(F32), spec[1].astype(F32)], 1).astype(BF16)

    def fill(i, carry):
        for q in range(5):
            mine[i, q] = rows[pl.ds(i + 128 * q, 4, stride=32), :].astype(BF16)
        mine[i, 5] = own
        return carry

    lax.fori_loop(0, count, fill, 0)

    lag = lax.broadcasted_iota(jnp.int32, (SIDE, 128), 0) + SIDE * (
        lax.broadcasted_iota(jnp.int32, (SIDE, 128), 1) & (SIDE - 1)
    )
    for s in range(SEGS):
        since = lag - start_ref[s]
        mask[s] = jnp.where((since >= 0) & (since < VALID), turn[2], 0.0)

    got[f] = mine[f]

    pl.semaphore_wait(barrier, 2 * count)

    def to_group(i, carry):
        to = lax.rem(f + i, count)
        pltpu.make_async_remote_copy(
            src_ref=mine.at[to], dst_ref=got.at[f], send_sem=send_sem.at[0, to], recv_sem=recv_sem.at[f],
            device_id=(g, to), device_id_type=MESH,
        ).start()
        return carry

    def to_far(i, carry):
        to = lax.rem(f + i, count)
        pltpu.make_async_remote_copy(
            src_ref=mine.at[f, 5], dst_ref=other.at[f], send_sem=send_sem.at[1, to], recv_sem=recv2_sem.at[f],
            device_id=(far, to), device_id_type=MESH,
        ).start()
        return carry

    lax.fori_loop(1, count, to_group, 0)
    lax.fori_loop(0, count, to_far, 0)

    def from_group(i, carry):
        at = lax.rem(f + i, count)
        pltpu.make_async_remote_copy(
            src_ref=mine.at[at], dst_ref=got.at[at], send_sem=send_sem.at[0, at], recv_sem=recv_sem.at[at],
            device_id=(g, at), device_id_type=MESH,
        ).wait_recv()
        return carry

    def from_far(i, carry):
        pltpu.make_async_remote_copy(
            src_ref=mine.at[f, 5], dst_ref=other.at[i], send_sem=send_sem.at[1, i], recv_sem=recv2_sem.at[i],
            device_id=(far, i), device_id_type=MESH,
        ).wait_recv()
        return carry

    lax.fori_loop(1, count, from_group, 0)
    lax.fori_loop(0, count, from_far, 0)

    side = [
        pltpu.make_async_remote_copy(
            src_ref=got.at[:, 5], dst_ref=beside, send_sem=side_sem.at[0], recv_sem=side_recv.at[0],
            device_id=(near, f), device_id_type=MESH,
        ),
        pltpu.make_async_remote_copy(
            src_ref=other, dst_ref=beside2, send_sem=side_sem.at[1], recv_sem=side_recv.at[1],
            device_id=(near, f), device_id_type=MESH,
        ),
    ]
    for copy in side:
        copy.start()

    left = lax.broadcasted_iota(jnp.int32, (ACROSS, 128), 1) < SIDE

    def swapped(x):
        return pltpu.roll(x, SIDE, 1)

    for i in range(ACROSS):
        for q in range(5):
            flat[24 * i + 4 * q:24 * i + 4 * q + 4, :] = got[i, q].astype(F32)
    for p in range(PAIRS):
        one = flat[pl.ds(p, ACROSS, stride=24), :]
        two = flat[pl.ds(p + PAIRS, ACROSS, stride=24), :]
        re = jnp.where(left, one, swapped(two))
        im = jnp.where(left, swapped(one), two)
        bank[p, 0] = re
        bank[p, 1] = im
        total = jnp.sum(re * re + im * im, axis=0, keepdims=True)
        norm[SEGS * p:SEGS * (p + 1), :] = jnp.broadcast_to(total, (SEGS, 128))

    def place(source, home):
        for i in range(ACROSS):
            flat[24 * i:24 * i + 4, :] = source(i).astype(F32)
        for q in range(4):
            row = flat[pl.ds(q, ACROSS, stride=24), :]
            turned = swapped(row)
            strain[4 * home + q, 0] = jnp.where(left, row, turned)
            strain[4 * home + q, 1] = jnp.where(left, turned, row)

    table = first[...]
    table2 = second[...]

    def correlate(groups):
        def pair(p, carry):
            h0, h1 = bank[p, 0], bank[p, 1]
            n = 0
            for home in groups:
                for half in range(2):
                    crosses = []
                    for q in range(2):
                        s = 4 * home + 2 * half + q
                        d0, d1 = strain[s, 0], strain[s, 1]
                        crosses.append(jnp.concatenate([h0 * d0 + h1 * d1, h0 * d1 - h1 * d0], 0).astype(BF16))
                    y = jnp.dot(table, jnp.concatenate(crosses, 1), preferred_element_type=F32)
                    for q in range(2):
                        re, im = y[:SIDE, 128 * q:128 * (q + 1)], y[SIDE:, 128 * q:128 * (q + 1)]
                        w0, w1 = turn[0], turn[1]
                        mid[n, :, 0:128] = (re * w0 - im * w1).astype(BF16)
                        mid[n, :, 128:256] = (re * w1 + im * w0).astype(BF16)
                        n += 1
            n = 0
            for home in groups:
                z = jnp.dot(mid[n:n + 4].reshape(4 * SIDE, 256), table2, preferred_element_type=F32)
                for q in range(4):
                    s = 4 * home + q
                    re, im = z[SIDE * q:SIDE * (q + 1), 0:128], z[SIDE * q:SIDE * (q + 1), 128:256]
                    power = (re * re + im * im) * mask[s]
                    peak[pl.ds(SEGS * p + s, 1), :] = jnp.max(power, axis=0, keepdims=True)
                    n += 1
            return carry

        lax.fori_loop(0, PAIRS, pair, 0)

    place(lambda i: got[i, 5], g)
    place(lambda i: other[i], far)
    correlate((g, far))
    for copy in side:
        copy.wait_recv()
    place(lambda i: beside[i], near)
    place(lambda i: beside2[i], lax.rem(near + 2, 4))
    correlate((near, lax.rem(near + 2, 4)))

    def halves(x, fold):
        return jnp.concatenate([fold(x[:SIDE], axis=0, keepdims=True), fold(x[SIDE:], axis=0, keepdims=True)], 0)

    for j in range(2):
        best = halves(peak[128 * j:128 * (j + 1), :].T, jnp.max)
        power = halves(norm[128 * j:128 * (j + 1), :].T, jnp.sum)
        sent[:, 128 * j:128 * (j + 1)] = best / power
    back[f] = sent[...]

    def share(i, carry):
        to = lax.rem(f + i, count)
        pltpu.make_async_remote_copy(
            src_ref=sent, dst_ref=back.at[f], send_sem=last_send.at[to], recv_sem=last_recv.at[f],
            device_id=(g, to), device_id_type=MESH,
        ).start()
        return carry

    lax.fori_loop(1, count, share, 0)

    def collect(i, carry):
        at = lax.rem(f + i, count)
        pltpu.make_async_remote_copy(
            src_ref=sent, dst_ref=back.at[at], send_sem=last_send.at[at], recv_sem=last_recv.at[at],
            device_id=(g, at), device_id_type=MESH,
        ).wait_recv()
        return carry

    lax.fori_loop(1, count, collect, 0)

    for i in range(count):
        for q in range(2):
            wide[32 * q + i:32 * q + i + 1, :] = back[i, q:q + 1, :]
    turned = [wide[:, 0:128].T, wide[:, 128:256].T]
    lane = lax.broadcasted_iota(jnp.int32, (SEGS, 128), 1)
    for c in range(5):
        block = None
        for k in range(4):
            j = 4 * c + k
            q, p = j // PAIRS, j % PAIRS
            piece = turned[p // 8][SEGS * (p % 8):SEGS * (p % 8 + 1), :]
            shift = (32 * k - 32 * q) % 128
            piece = pltpu.roll(piece, shift, 1) if shift else piece
            block = piece if block is None else jnp.where(lane >= 32 * k, piece, block)
        out_ref[:, 128 * c:128 * (c + 1)] = block

    def drain(i, carry):
        at = lax.rem(f + i, count)
        pltpu.make_async_remote_copy(
            src_ref=mine.at[at], dst_ref=got.at[f], send_sem=send_sem.at[0, at], recv_sem=recv_sem.at[f],
            device_id=(g, at), device_id_type=MESH,
        ).wait_send()
        pltpu.make_async_remote_copy(
            src_ref=sent, dst_ref=back.at[f], send_sem=last_send.at[at], recv_sem=last_recv.at[f],
            device_id=(g, at), device_id_type=MESH,
        ).wait_send()
        return carry

    def drain_far(i, carry):
        pltpu.make_async_remote_copy(
            src_ref=mine.at[f, 5], dst_ref=other.at[f], send_sem=send_sem.at[1, i], recv_sem=recv2_sem.at[f],
            device_id=(far, i), device_id_type=MESH,
        ).wait_send()
        return carry

    lax.fori_loop(1, count, drain, 0)
    lax.fori_loop(0, count, drain_far, 0)
    for copy in side:
        copy.wait_send()


def on_device(spectra, templates, valid_start):
    first, turn, second = tables()
    anywhere = pl.BlockSpec(memory_space=pl.ANY)
    dma = pltpu.SemaphoreType.DMA
    out = pl.pallas_call(
        kernel,
        out_shape=jax.ShapeDtypeStruct((SEGS, 640), F32),
        in_specs=[pl.BlockSpec(memory_space=pltpu.SMEM)] + [anywhere] * 5,
        out_specs=pl.BlockSpec(memory_space=pltpu.VMEM),
        scratch_shapes=[
            pltpu.VMEM((2, 64, 640), BF16),
            pltpu.VMEM((2, 4, 64), BF16),
            pltpu.VMEM(first.shape, BF16),
            pltpu.VMEM(turn.shape, F32),
            pltpu.VMEM(second.shape, BF16),
            pltpu.VMEM((640, 128), F32),
            pltpu.VMEM((32, 6, 4, 128), BF16),
            pltpu.VMEM((32, 6, 4, 128), BF16),
            pltpu.VMEM((32, 4, 128), BF16),
            pltpu.VMEM((32, 4, 128), BF16),
            pltpu.VMEM((32, 4, 128), BF16),
            pltpu.VMEM((32 * 24, 128), F32),
            pltpu.VMEM((PAIRS, 2, ACROSS, 128), F32),
            pltpu.VMEM((SEGS, 2, ACROSS, 128), F32),
            pltpu.VMEM((SEGS, SIDE, 128), F32),
            pltpu.VMEM((8, SIDE, 256), BF16),
            pltpu.VMEM((256, 128), F32),
            pltpu.VMEM((256, 128), F32),
            pltpu.VMEM((2, 256), F32),
            pltpu.VMEM((32, 2, 256), F32),
            pltpu.VMEM((128, 256), F32),
            dma((5,)),
            dma((2, 32)),
            dma((32,)),
            dma((32,)),
            dma((2,)),
            dma((2,)),
            dma((32,)),
            dma((32,)),
        ],
        compiler_params=pltpu.CompilerParams(collective_id=0, has_side_effects=True),
        name="matched_filter",
    )(valid_start, jnp.transpose(templates, (1, 0, 2)), jnp.transpose(spectra, (1, 2, 0)), first, turn, second)
    return out.T


def solution(mesh):
    return jax.shard_map(
        on_device, mesh=mesh, in_specs=(P("freq", None, "group"), P("freq", None, "group"), P()),
        out_specs=P("group", None), check_vma=False,
    )
```

```python
import math

import jax
import jax.numpy as jnp
import numpy as np
from jax import lax
from jax.experimental import pallas as pl
from jax.experimental.pallas import tpu as pltpu
from jax.sharding import PartitionSpec as P

N = 4096
VALID = 2048
SIDE = 64
ACROSS = 32
PAIRS = 10
SEGS = 16
MESH = pl.DeviceIdType.MESH
F32 = jnp.float32
BF16 = jnp.bfloat16


def rounded_roots(index):
    exact = np.exp(2j * np.pi * (index % SIDE) / SIDE)
    least = np.full(index.shape[0], np.inf)
    table = np.zeros_like(exact)
    gain = np.ones(index.shape[0])
    for scale in np.linspace(1.0, 2.0, 2001)[:-1]:
        parts = [(x * scale).astype(jnp.bfloat16).astype(np.float64) for x in (exact.real, exact.imag)]
        tried = parts[0] + 1j * parts[1]
        level = (tried * exact.conj()).mean(1).real
        rest = (np.abs(tried / level[:, None] - exact) ** 2).mean(1)
        better = rest < least - 1e-15
        least = np.where(better, rest, least)
        table = np.where(better[:, None], tried, table)
        gain = np.where(better, level, gain)
    return table, gain


def tables():
    side = np.arange(SIDE)
    root, gain = rounded_roots(side[:, None] * np.arange(ACROSS)[None, :])
    first = np.concatenate(
        [np.concatenate([root.real, -root.imag], 1), np.concatenate([root.imag, root.real], 1)], 0
    )
    turn = np.exp(2j * np.pi * side[:, None] * side[None, :] / N) / gain[:, None]
    root, gain = rounded_roots(side[:, None] * side[None, :])
    c, s = np.kron(np.eye(2), root.real.T), np.kron(np.eye(2), root.imag.T)
    second = np.concatenate([np.concatenate([c, s], 1), np.concatenate([-s, c], 1)], 0)
    weight = np.tile(1.0 / gain ** 2, (SIDE, 2))
    turn = np.stack([np.tile(turn.real, (1, 2)), np.tile(turn.imag, (1, 2)), weight], 0)
    return jnp.asarray(first, BF16), jnp.asarray(turn, F32), jnp.asarray(second, BF16)


def far_first(distance):
    offsets = [(dz, dx, dy) for dz in range(4) for dx in range(4) for dy in range(2)]
    return sorted(offsets, key=lambda o: -(min(o[0], 4 - o[0]) + min(o[1], 4 - o[1]) + distance(o[2])))


IN_GROUP = [o for o in far_first(lambda dy: dy) if o != (0, 0, 0)]
IN_FAR = far_first(lambda dy: 2 - dy)


def kernel(
    start_hbm, tpl_hbm, spec_hbm, first_hbm, turn_hbm, second_hbm, out_ref,
    start, tpl, spec, first, turn, second, rows, mine, got, other, beside, beside2, flat,
    bank, strain, mask, mid, mid2, peak, norm, sent, back, wide,
    load_sem, send_sem, recv_sem, side_sem, side_recv,
):
    g = lax.axis_index("group")
    f = lax.axis_index("freq")
    far = lax.rem(g + 2, 4)
    near = g + 1 - 2 * lax.rem(g, 2)
    count = 32
    peers = count - 1
    z, x, y = f // 8, lax.rem(f, 8) // 2, lax.rem(f, 2)
    part_z = [8 * lax.rem(z + d, 4) for d in range(4)]
    part_x = [2 * lax.rem(x + d, 4) for d in range(4)]
    part_y = [y, 1 - y]

    def at(offset):
        return part_z[offset[0]] + part_x[offset[1]] + part_y[offset[2]]

    loads = [
        pltpu.make_async_copy(src, dst, load_sem.at[i])
        for i, (src, dst) in enumerate(
            [
                (tpl_hbm, tpl), (spec_hbm, spec), (start_hbm, start),
                (first_hbm, first), (turn_hbm, turn), (second_hbm, second),
            ]
        )
    ]
    for load in loads:
        load.start()

    barrier = pltpu.get_barrier_semaphore()
    for o in IN_FAR:
        pl.semaphore_signal(barrier, inc=1, device_id=(far, at(o)), device_id_type=MESH)
    for o in IN_GROUP:
        pl.semaphore_signal(barrier, inc=1, device_id=(g, at(o)), device_id_type=MESH)
    pl.semaphore_signal(barrier, inc=1, device_id=(near, f), device_id_type=MESH)

    for load in loads:
        load.wait()

    peak[...] = jnp.zeros_like(peak)
    norm[...] = jnp.ones_like(norm)

    for j in range(5):
        block = jnp.concatenate(
            [tpl[:, q, 128 * j:128 * (j + 1)].astype(F32) for q in range(2)], 0
        )
        rows[128 * j:128 * (j + 1), :] = block.T
    own = jnp.concatenate([spec[0].astype(F32), spec[1].astype(F32)], 1).astype(BF16)

    def fill(i, carry):
        for q in range(5):
            mine[i, q] = rows[pl.ds(i + 128 * q, 4, stride=32), :].astype(BF16)
        mine[i, 5] = own
        return carry

    lax.fori_loop(0, count, fill, 0)

    lag = lax.broadcasted_iota(jnp.int32, (SIDE, 128), 0) + SIDE * (
        lax.broadcasted_iota(jnp.int32, (SIDE, 128), 1) & (SIDE - 1)
    )
    for s in range(SEGS):
        since = lag - start[s]
        mask[s] = jnp.where((since >= 0) & (since < VALID), turn[2], 0.0)

    got[f] = mine[f]

    pl.semaphore_wait(barrier, 2 * count)

    def to_far(to):
        return pltpu.make_async_remote_copy(
            src_ref=mine.at[f, 5], dst_ref=other.at[f], send_sem=send_sem.at[1], recv_sem=recv_sem.at[1],
            device_id=(far, to), device_id_type=MESH,
        )

    def to_group(to):
        return pltpu.make_async_remote_copy(
            src_ref=mine.at[to], dst_ref=got.at[f], send_sem=send_sem.at[0], recv_sem=recv_sem.at[0],
            device_id=(g, to), device_id_type=MESH,
        )

    for o in IN_FAR[:1]:
        to_far(at(o)).start()
    for o in IN_GROUP:
        to_group(at(o)).start()
    for o in IN_FAR[1:]:
        to_far(at(o)).start()

    all_group = pltpu.make_async_remote_copy(
        src_ref=mine.at[pl.ds(0, peers)], dst_ref=got.at[pl.ds(0, peers)], send_sem=send_sem.at[0],
        recv_sem=recv_sem.at[0], device_id=(near, f), device_id_type=MESH,
    )
    all_far = pltpu.make_async_remote_copy(
        src_ref=other, dst_ref=other, send_sem=send_sem.at[1],
        recv_sem=recv_sem.at[1], device_id=(near, f), device_id_type=MESH,
    )
    side = [
        pltpu.make_async_remote_copy(
            src_ref=src, dst_ref=dst, send_sem=side_sem.at[i], recv_sem=side_recv.at[i],
            device_id=(near, f), device_id_type=MESH,
        )
        for i, (src, dst) in enumerate([(got.at[:, 5], beside), (other, beside2)])
    ]
    all_group.wait_recv()
    side[0].start()

    left = lax.broadcasted_iota(jnp.int32, (ACROSS, 128), 1) < SIDE

    def swapped(x):
        return pltpu.roll(x, SIDE, 1)

    for i in range(ACROSS):
        for q in range(5):
            flat[24 * i + 4 * q:24 * i + 4 * q + 4, :] = got[i, q].astype(F32)
    for p in range(PAIRS):
        one = flat[pl.ds(p, ACROSS, stride=24), :]
        two = flat[pl.ds(p + PAIRS, ACROSS, stride=24), :]
        re = jnp.where(left, one, swapped(two))
        im = jnp.where(left, swapped(one), two)
        bank[p, 0] = re
        bank[p, 1] = im
        total = jnp.sum(re * re + im * im, axis=0, keepdims=True)
        norm[SEGS * p:SEGS * (p + 1), :] = jnp.broadcast_to(total, (SEGS, 128))

    def place(source, home):
        for i in range(ACROSS):
            flat[24 * i:24 * i + 4, :] = source(i).astype(F32)
        for q in range(4):
            row = flat[pl.ds(q, ACROSS, stride=24), :]
            turned = swapped(row)
            strain[4 * home + q, 0] = jnp.where(left, row, turned)
            strain[4 * home + q, 1] = jnp.where(left, turned, row)

    table = first[...]
    table2 = second[...]

    def across(p, homes, dst):
        h0, h1 = bank[p, 0], bank[p, 1]
        for n in range(2 * len(homes)):
            crosses = []
            for q in range(2):
                s = 4 * homes[n // 2] + 2 * (n % 2) + q
                d0, d1 = strain[s, 0], strain[s, 1]
                crosses.append(jnp.concatenate([h0 * d0 + h1 * d1, h0 * d1 - h1 * d0], 0).astype(BF16))
            y = jnp.dot(table, jnp.concatenate(crosses, 1), preferred_element_type=F32)
            for q in range(2):
                re, im = y[:SIDE, 128 * q:128 * (q + 1)], y[SIDE:, 128 * q:128 * (q + 1)]
                w0, w1 = turn[0], turn[1]
                dst[2 * n + q, :, 0:128] = (re * w0 - im * w1).astype(BF16)
                dst[2 * n + q, :, 128:256] = (re * w1 + im * w0).astype(BF16)

    def along(p, homes, src):
        for n, home in enumerate(homes):
            z = jnp.dot(src[4 * n:4 * n + 4].reshape(4 * SIDE, 256), table2, preferred_element_type=F32)
            for q in range(4):
                s = 4 * home + q
                re, im = z[SIDE * q:SIDE * (q + 1), 0:128], z[SIDE * q:SIDE * (q + 1), 128:256]
                power = (re * re + im * im) * mask[s]
                peak[pl.ds(SEGS * p + s, 1), :] = jnp.max(power, axis=0, keepdims=True)

    def steps(homes):
        def pair(i, carry):
            across(2 * i + 1, homes, mid2)
            along(2 * i, homes, mid)
            across(2 * i + 2, homes, mid)
            along(2 * i + 1, homes, mid2)
            return carry

        lax.fori_loop(0, PAIRS // 2 - 1, pair, 0)

    here, there = (g, far), (near, lax.rem(near + 2, 4))
    place(lambda i: got[i, 5], g)
    all_far.wait_recv()
    side[1].start()
    place(lambda i: other[i], far)
    across(0, here, mid)
    steps(here)
    for copy in side:
        copy.wait_recv()
    place(lambda i: beside[i], there[0])
    place(lambda i: beside2[i], there[1])
    across(PAIRS - 1, here, mid2)
    along(PAIRS - 2, here, mid)
    across(0, there, mid)
    along(PAIRS - 1, here, mid2)
    steps(there)
    across(PAIRS - 1, there, mid2)
    along(PAIRS - 2, there, mid)
    along(PAIRS - 1, there, mid2)

    def halves(x, fold):
        return jnp.concatenate([fold(x[:SIDE], axis=0, keepdims=True), fold(x[SIDE:], axis=0, keepdims=True)], 0)

    for j in range(2):
        best = halves(peak[128 * j:128 * (j + 1), :].T, jnp.max)
        power = halves(norm[128 * j:128 * (j + 1), :].T, jnp.sum)
        sent[:, 128 * j:128 * (j + 1)] = best / power
    back[f] = sent[...]

    def share(to):
        return pltpu.make_async_remote_copy(
            src_ref=sent, dst_ref=back.at[f], send_sem=send_sem.at[2], recv_sem=recv_sem.at[2],
            device_id=(g, to), device_id_type=MESH,
        )

    for o in IN_GROUP:
        share(at(o)).start()
    all_group.wait_send()
    all_far.wait_send()
    for copy in side:
        copy.wait_send()
    all_shared = pltpu.make_async_remote_copy(
        src_ref=back.at[pl.ds(0, peers)], dst_ref=back.at[pl.ds(0, peers)], send_sem=send_sem.at[2],
        recv_sem=recv_sem.at[2], device_id=(near, f), device_id_type=MESH,
    )
    all_shared.wait_recv()

    for i in range(count):
        for q in range(2):
            wide[32 * q + i:32 * q + i + 1, :] = back[i, q:q + 1, :]
    turned = [wide[:, 0:128].T, wide[:, 128:256].T]
    lane = lax.broadcasted_iota(jnp.int32, (SEGS, 128), 1)
    for c in range(5):
        block = None
        for k in range(4):
            j = 4 * c + k
            q, p = j // PAIRS, j % PAIRS
            piece = turned[p // 8][SEGS * (p % 8):SEGS * (p % 8 + 1), :]
            shift = (32 * k - 32 * q) % 128
            piece = pltpu.roll(piece, shift, 1) if shift else piece
            block = piece if block is None else jnp.where(lane >= 32 * k, piece, block)
        out_ref[:, 128 * c:128 * (c + 1)] = block

    all_shared.wait_send()


def on_device(spectra, templates, valid_start):
    first, turn, second = tables()
    anywhere = pl.BlockSpec(memory_space=pl.ANY)
    dma = pltpu.SemaphoreType.DMA
    out = pl.pallas_call(
        kernel,
        out_shape=jax.ShapeDtypeStruct((SEGS, 640), F32),
        in_specs=[anywhere] * 6,
        out_specs=pl.BlockSpec(memory_space=pltpu.VMEM),
        scratch_shapes=[
            pltpu.SMEM((SEGS,), jnp.int32),
            pltpu.VMEM((64, 2, 640), BF16),
            pltpu.VMEM((2, 4, 64), BF16),
            pltpu.VMEM(first.shape, BF16),
            pltpu.VMEM(turn.shape, F32),
            pltpu.VMEM(second.shape, BF16),
            pltpu.VMEM((640, 128), F32),
            pltpu.VMEM((32, 6, 4, 128), BF16),
            pltpu.VMEM((32, 6, 4, 128), BF16),
            pltpu.VMEM((32, 4, 128), BF16),
            pltpu.VMEM((32, 4, 128), BF16),
            pltpu.VMEM((32, 4, 128), BF16),
            pltpu.VMEM((32 * 24, 128), F32),
            pltpu.VMEM((PAIRS, 2, ACROSS, 128), F32),
            pltpu.VMEM((SEGS, 2, ACROSS, 128), F32),
            pltpu.VMEM((SEGS, SIDE, 128), F32),
            pltpu.VMEM((8, SIDE, 256), BF16),
            pltpu.VMEM((8, SIDE, 256), BF16),
            pltpu.VMEM((256, 128), F32),
            pltpu.VMEM((256, 128), F32),
            pltpu.VMEM((2, 256), F32),
            pltpu.VMEM((32, 2, 256), F32),
            pltpu.VMEM((128, 256), F32),
            dma((6,)),
            dma((3,)),
            dma((3,)),
            dma((2,)),
            dma((2,)),
        ],
        compiler_params=pltpu.CompilerParams(collective_id=0, has_side_effects=True),
        name="matched_filter",
    )(valid_start, templates, jnp.transpose(spectra, (1, 2, 0)), first, turn, second)
    return jnp.maximum(out, 0.0).T


def solution(mesh):
    return jax.shard_map(
        on_device, mesh=mesh, in_specs=(P("freq", None, "group"), P("freq", None, "group"), P()),
        out_specs=P("group", None), check_vma=False,
    )
```

```python
import math

import jax
import jax.numpy as jnp
import numpy as np
from jax import lax
from jax.experimental import pallas as pl
from jax.experimental.pallas import tpu as pltpu
from jax.sharding import PartitionSpec as P

N = 4096
VALID = 2048
SIDE = 64
ACROSS = 32
PAIRS = 10
SEGS = 16
MESH = pl.DeviceIdType.MESH
F32 = jnp.float32
BF16 = jnp.bfloat16


def rounded_roots(index):
    exact = np.exp(2j * np.pi * (index % SIDE) / SIDE)
    least = np.full(index.shape[0], np.inf)
    table = np.zeros_like(exact)
    gain = np.ones(index.shape[0])
    for scale in np.linspace(1.0, 2.0, 2001)[:-1]:
        parts = [(x * scale).astype(jnp.bfloat16).astype(np.float64) for x in (exact.real, exact.imag)]
        tried = parts[0] + 1j * parts[1]
        level = (tried * exact.conj()).mean(1).real
        rest = (np.abs(tried / level[:, None] - exact) ** 2).mean(1)
        better = rest < least - 1e-15
        least = np.where(better, rest, least)
        table = np.where(better[:, None], tried, table)
        gain = np.where(better, level, gain)
    return table, gain


def tables():
    side = np.arange(SIDE)
    root, gain = rounded_roots(side[:, None] * np.arange(ACROSS)[None, :])
    first = np.stack([np.concatenate([root.real, -root.imag], 1), np.concatenate([root.imag, root.real], 1)], 0)
    first = np.tile(first, (1, 2, 1))
    lag = np.arange(2 * SIDE)
    turn = np.exp(2j * np.pi * lag[:, None] * side[None, :] / N) / np.tile(gain, 2)[:, None]
    turn = np.tile(np.stack([turn.real, turn.imag], 0), (1, 1, 2))
    root, gain = rounded_roots(side[:VALID // SIDE, None] * side[None, :])
    c, s = np.kron(np.eye(2), root.real.T), np.kron(np.eye(2), root.imag.T)
    none = np.zeros_like(c)
    second = np.concatenate(
        [
            np.concatenate([c, none, s, none], 1), np.concatenate([-s, none, c, none], 1),
            np.concatenate([none, c, none, s], 1), np.concatenate([none, -s, none, c], 1),
        ], 0,
    )
    jump = np.exp(2j * np.pi * np.arange(40)[:, None] * side[None, :] / SIDE)
    jump = np.tile(np.stack([jump.real, jump.imag], 0), (1, 1, 2))
    weight = np.tile(1.0 / gain ** 2, (2, 8, 4))
    jump = np.concatenate([jump, weight], 1)
    return jnp.asarray(first, F32), jnp.asarray(turn, F32), jnp.asarray(jump, F32), jnp.asarray(second, BF16)


def far_first(distance):
    offsets = [(dz, dx, dy) for dz in range(4) for dx in range(4) for dy in range(2)]
    return sorted(offsets, key=lambda o: -(min(o[0], 4 - o[0]) + min(o[1], 4 - o[1]) + distance(o[2])))


IN_GROUP = [o for o in far_first(lambda dy: dy) if o != (0, 0, 0)]
IN_FAR = far_first(lambda dy: 2 - dy)


def kernel(
    start_hbm, tpl_hbm, spec_hbm, first_hbm, turn_hbm, jump_hbm, second_hbm, out_ref,
    start, tpl, spec, first, turn, jump, second, rows, mine, got, other, beside, beside2, flat,
    bank, strain, firsts, turns, mid, mid2, peak, norm, sent, back, wide,
    load_sem, send_sem, recv_sem, side_sem, side_recv,
):
    g = lax.axis_index("group")
    f = lax.axis_index("freq")
    far = lax.rem(g + 2, 4)
    near = g + 1 - 2 * lax.rem(g, 2)
    count = 32
    peers = count - 1
    z, x, y = f // 8, lax.rem(f, 8) // 2, lax.rem(f, 2)
    part_z = [8 * lax.rem(z + d, 4) for d in range(4)]
    part_x = [2 * lax.rem(x + d, 4) for d in range(4)]
    part_y = [y, 1 - y]

    def at(offset):
        return part_z[offset[0]] + part_x[offset[1]] + part_y[offset[2]]

    loads = [
        pltpu.make_async_copy(src, dst, load_sem.at[i])
        for i, (src, dst) in enumerate(
            [
                (tpl_hbm, tpl), (spec_hbm, spec), (start_hbm, start),
                (first_hbm, first), (turn_hbm, turn), (jump_hbm, jump), (second_hbm, second),
            ]
        )
    ]
    for load in loads:
        load.start()

    barrier = pltpu.get_barrier_semaphore()
    for o in IN_FAR:
        pl.semaphore_signal(barrier, inc=1, device_id=(far, at(o)), device_id_type=MESH)
    for o in IN_GROUP:
        pl.semaphore_signal(barrier, inc=1, device_id=(g, at(o)), device_id_type=MESH)
    pl.semaphore_signal(barrier, inc=1, device_id=(near, f), device_id_type=MESH)

    for load in loads:
        load.wait()

    peak[...] = jnp.zeros_like(peak)
    norm[...] = jnp.ones_like(norm)

    for j in range(5):
        block = jnp.concatenate(
            [tpl[:, q, 128 * j:128 * (j + 1)].astype(F32) for q in range(2)], 0
        )
        rows[128 * j:128 * (j + 1), :] = block.T
    own = jnp.concatenate([spec[0].astype(F32), spec[1].astype(F32)], 1).astype(BF16)

    def fill(i, carry):
        for q in range(5):
            mine[i, q] = rows[pl.ds(i + 128 * q, 4, stride=32), :].astype(BF16)
        mine[i, 5] = own
        return carry

    lax.fori_loop(0, count, fill, 0)

    got[f] = mine[f]

    pl.semaphore_wait(barrier, 2 * count)

    def to_far(to):
        return pltpu.make_async_remote_copy(
            src_ref=mine.at[f, 5], dst_ref=other.at[f], send_sem=send_sem.at[1], recv_sem=recv_sem.at[1],
            device_id=(far, to), device_id_type=MESH,
        )

    def to_group(to):
        return pltpu.make_async_remote_copy(
            src_ref=mine.at[to], dst_ref=got.at[f], send_sem=send_sem.at[0], recv_sem=recv_sem.at[0],
            device_id=(g, to), device_id_type=MESH,
        )

    for o in IN_FAR:
        to_far(at(o)).start()
    for o in IN_GROUP:
        to_group(at(o)).start()

    all_group = pltpu.make_async_remote_copy(
        src_ref=mine.at[pl.ds(0, peers)], dst_ref=got.at[pl.ds(0, peers)], send_sem=send_sem.at[0],
        recv_sem=recv_sem.at[0], device_id=(near, f), device_id_type=MESH,
    )
    all_far = pltpu.make_async_remote_copy(
        src_ref=other, dst_ref=other, send_sem=send_sem.at[1],
        recv_sem=recv_sem.at[1], device_id=(near, f), device_id_type=MESH,
    )
    side = [
        pltpu.make_async_remote_copy(
            src_ref=src, dst_ref=dst, send_sem=side_sem.at[i], recv_sem=side_recv.at[i],
            device_id=(near, f), device_id_type=MESH,
        )
        for i, (src, dst) in enumerate([(got.at[:, 5], beside), (other, beside2)])
    ]
    def shift(s, carry):
        begin = start[s]
        low, high = lax.rem(begin, SIDE), lax.div(begin, SIDE)
        for q in range(2):
            firsts[s, SIDE * q:SIDE * (q + 1), :] = first[q, pl.ds(low, SIDE), :].astype(BF16)
        w0, w1 = turn[0, pl.ds(low, SIDE), :], turn[1, pl.ds(low, SIDE), :]
        r0, r1 = jump[0, pl.ds(high, 1), :], jump[1, pl.ds(high, 1), :]
        turns[s, 0] = w0 * r0 - w1 * r1
        turns[s, 1] = w0 * r1 + w1 * r0
        return carry

    lax.fori_loop(0, SEGS, shift, 0)

    all_group.wait_recv()
    side[0].start()

    left = lax.broadcasted_iota(jnp.int32, (ACROSS, 128), 1) < SIDE

    def swapped(x):
        return pltpu.roll(x, SIDE, 1)

    for i in range(ACROSS):
        for q in range(5):
            flat[24 * i + 4 * q:24 * i + 4 * q + 4, :] = got[i, q].astype(F32)
    for p in range(PAIRS):
        one = flat[pl.ds(p, ACROSS, stride=24), :]
        two = flat[pl.ds(p + PAIRS, ACROSS, stride=24), :]
        re = jnp.where(left, one, swapped(two))
        im = jnp.where(left, swapped(one), two)
        bank[p, 0] = re
        bank[p, 1] = im
        total = jnp.sum(re * re + im * im, axis=0, keepdims=True)
        norm[8 * p:8 * (p + 1), :] = jnp.broadcast_to(total, (8, 128))

    def place(source, home):
        for i in range(ACROSS):
            flat[24 * i:24 * i + 4, :] = source(i).astype(F32)
        for q in range(4):
            row = flat[pl.ds(q, ACROSS, stride=24), :]
            turned = swapped(row)
            strain[4 * home + q, 0] = jnp.where(left, row, turned)
            strain[4 * home + q, 1] = jnp.where(left, turned, row)

    table2 = second[...]
    half = lax.rem(g, 2)

    def across(u, low, dst):
        held = [(bank[2 * u + i, 0], bank[2 * u + i, 1]) for i in range(2)]
        for q in range(4):
            for k in range(2):
                s = low + q + 8 * k
                d0, d1 = strain[s, 0], strain[s, 1]
                crosses = [
                    jnp.concatenate([h0 * d0 + h1 * d1, h0 * d1 - h1 * d0], 0).astype(BF16) for h0, h1 in held
                ]
                y = jnp.dot(firsts[s], jnp.concatenate(crosses, 1), preferred_element_type=F32)
                w0, w1 = turns[s, 0], turns[s, 1]
                for i in range(2):
                    re, im = y[:SIDE, 128 * i:128 * (i + 1)], y[SIDE:, 128 * i:128 * (i + 1)]
                    dst[4 * i + q, :, 256 * k:256 * k + 128] = (re * w0 - im * w1).astype(BF16)
                    dst[4 * i + q, :, 256 * k + 128:256 * k + 256] = (re * w1 + im * w0).astype(BF16)

    def along(u, low, src):
        for i in range(2):
            z = jnp.dot(src[4 * i:4 * i + 4].reshape(4 * SIDE, 512), table2, preferred_element_type=F32)
            for q in range(4):
                re, im = z[SIDE * q:SIDE * (q + 1), 0:128], z[SIDE * q:SIDE * (q + 1), 128:256]
                peak[pl.ds(16 * u + 8 * i + low + q, 1), :] = jnp.max(re * re + im * im, axis=0, keepdims=True)

    def steps(low, one, two):
        def pair(i, carry):
            across(2 * i + 1, low, two)
            along(2 * i, low, one)
            across(2 * i + 2, low, one)
            along(2 * i + 1, low, two)
            return carry

        lax.fori_loop(0, 2, pair, 0)

    here, there = 4 * half, 4 - 4 * half
    place(lambda i: got[i, 5], g)
    all_far.wait_recv()
    side[1].start()
    place(lambda i: other[i], far)
    across(0, here, mid)
    steps(here, mid, mid2)
    for copy in side:
        copy.wait_recv()
    place(lambda i: beside[i], near)
    place(lambda i: beside2[i], lax.rem(near + 2, 4))
    across(0, there, mid2)
    along(4, here, mid)
    steps(there, mid2, mid)
    along(4, there, mid2)
    best = (peak[...] * jump[0, 40:41, :]).T
    power = norm[...].T
    power = [jnp.sum(power[SIDE * q:SIDE * (q + 1)], axis=0, keepdims=True) for q in range(2)]
    for k in range(4):
        sent[k:k + 1, :] = jnp.max(best[32 * k:32 * (k + 1)], axis=0, keepdims=True) / power[k % 2]
    back[f] = sent[...]

    def share(to):
        return pltpu.make_async_remote_copy(
            src_ref=sent, dst_ref=back.at[f], send_sem=send_sem.at[2], recv_sem=recv_sem.at[2],
            device_id=(g, to), device_id_type=MESH,
        )

    for o in IN_GROUP:
        share(at(o)).start()
    all_group.wait_send()
    all_far.wait_send()
    for copy in side:
        copy.wait_send()
    all_shared = pltpu.make_async_remote_copy(
        src_ref=back.at[pl.ds(0, peers)], dst_ref=back.at[pl.ds(0, peers)], send_sem=send_sem.at[2],
        recv_sem=recv_sem.at[2], device_id=(near, f), device_id_type=MESH,
    )
    all_shared.wait_recv()

    for i in range(count):
        for k in range(4):
            wide[32 * k + i:32 * k + i + 1, :] = back[i, k:k + 1, :]
    turned = wide[...].T
    lane = lax.broadcasted_iota(jnp.int32, (8, 128), 1)
    for c in range(5):
        for k in range(2):
            block = None
            for n in range(4):
                q, p = divmod(4 * c + n, PAIRS)
                piece = turned[8 * p:8 * (p + 1), :]
                shift = (32 * n - 32 * q - 64 * k) % 128
                piece = pltpu.roll(piece, shift, 1) if shift else piece
                block = piece if block is None else jnp.where(lane >= 32 * n, piece, block)
            out_ref[8 * k:8 * (k + 1), 128 * c:128 * (c + 1)] = block

    all_shared.wait_send()


def on_device(spectra, templates, valid_start):
    first, turn, jump, second = tables()
    anywhere = pl.BlockSpec(memory_space=pl.ANY)
    dma = pltpu.SemaphoreType.DMA
    out = pl.pallas_call(
        kernel,
        out_shape=pltpu.VMEM((SEGS, 640), F32),
        in_specs=[anywhere] * 7,
        out_specs=pl.BlockSpec(memory_space=pltpu.VMEM),
        scratch_shapes=[
            pltpu.SMEM((SEGS,), jnp.int32),
            pltpu.VMEM((64, 2, 640), BF16),
            pltpu.VMEM((2, 4, 64), BF16),
            pltpu.VMEM(first.shape, F32),
            pltpu.VMEM(turn.shape, F32),
            pltpu.VMEM(jump.shape, F32),
            pltpu.VMEM(second.shape, BF16),
            pltpu.VMEM((640, 128), F32),
            pltpu.VMEM((32, 6, 4, 128), BF16),
            pltpu.VMEM((32, 6, 4, 128), BF16),
            pltpu.VMEM((32, 4, 128), BF16),
            pltpu.VMEM((32, 4, 128), BF16),
            pltpu.VMEM((32, 4, 128), BF16),
            pltpu.VMEM((32 * 24, 128), F32),
            pltpu.VMEM((PAIRS, 2, ACROSS, 128), F32),
            pltpu.VMEM((SEGS, 2, ACROSS, 128), F32),
            pltpu.VMEM((SEGS, 128, 64), BF16),
            pltpu.VMEM((SEGS, 2, SIDE, 128), F32),
            pltpu.VMEM((8, SIDE, 512), BF16),
            pltpu.VMEM((8, SIDE, 512), BF16),
            pltpu.VMEM((128, 128), F32),
            pltpu.VMEM((128, 128), F32),
            pltpu.VMEM((4, 128), F32),
            pltpu.VMEM((32, 4, 128), F32),
            pltpu.VMEM((128, 128), F32),
            dma((7,)),
            dma((3,)),
            dma((3,)),
            dma((2,)),
            dma((2,)),
        ],
        compiler_params=pltpu.CompilerParams(collective_id=0, has_side_effects=True),
        name="matched_filter",
    )(valid_start, templates, jnp.transpose(spectra, (1, 2, 0)), first, turn, jump, second)
    return out.T


def solution(mesh):
    return jax.shard_map(
        on_device, mesh=mesh, in_specs=(P("freq", None, "group"), P("freq", None, "group"), P()),
        out_specs=P("group", None), check_vma=False,
    )
```

```python
import math

import jax
import jax.numpy as jnp
import numpy as np
from jax import lax
from jax.experimental import pallas as pl
from jax.experimental.pallas import tpu as pltpu
from jax.sharding import PartitionSpec as P

N = 4096
VALID = 2048
SIDE = 64
ACROSS = 32
PAIRS = 10
SEGS = 16
MESH = pl.DeviceIdType.MESH
F32 = jnp.float32
BF16 = jnp.bfloat16


def rounded_roots(index):
    exact = np.exp(2j * np.pi * (index % SIDE) / SIDE)
    least = np.full(index.shape[0], np.inf)
    table = np.zeros_like(exact)
    gain = np.ones(index.shape[0])
    for scale in np.linspace(1.0, 2.0, 2001)[:-1]:
        parts = [(x * scale).astype(jnp.bfloat16).astype(np.float64) for x in (exact.real, exact.imag)]
        tried = parts[0] + 1j * parts[1]
        level = (tried * exact.conj()).mean(1).real
        rest = (np.abs(tried / level[:, None] - exact) ** 2).mean(1)
        better = rest < least - 1e-15
        least = np.where(better, rest, least)
        table = np.where(better[:, None], tried, table)
        gain = np.where(better, level, gain)
    return table, gain


def tables():
    side = np.arange(SIDE)
    root, gain = rounded_roots(side[:, None] * np.arange(ACROSS)[None, :])
    first = np.stack([np.concatenate([root.real, -root.imag], 1), np.concatenate([root.imag, root.real], 1)], 0)
    first = np.tile(first, (1, 2, 1))
    lag = np.arange(2 * SIDE)
    turn = np.exp(2j * np.pi * lag[:, None] * side[None, :] / N) / np.tile(gain, 2)[:, None]
    turn = np.tile(np.stack([turn.real, turn.imag], 0), (1, 1, 2))
    root, gain = rounded_roots(side[:VALID // SIDE, None] * side[None, :])
    c, s = np.kron(np.eye(2), root.real.T), np.kron(np.eye(2), root.imag.T)
    none = np.zeros_like(c)
    second = np.concatenate(
        [
            np.concatenate([c, none, s, none], 1), np.concatenate([-s, none, c, none], 1),
            np.concatenate([none, c, none, s], 1), np.concatenate([none, -s, none, c], 1),
        ], 0,
    )
    jump = np.exp(2j * np.pi * np.arange(40)[:, None] * side[None, :] / SIDE)
    jump = np.tile(np.stack([jump.real, jump.imag], 0), (1, 1, 2))
    weight = np.tile(1.0 / gain ** 2, (2, 8, 4))
    jump = np.concatenate([jump, weight], 1)
    return jnp.asarray(first, F32), jnp.asarray(turn, F32), jnp.asarray(jump, F32), jnp.asarray(second, BF16)


def far_first(distance):
    offsets = [(dz, dx, dy) for dz in range(4) for dx in range(4) for dy in range(2)]
    return sorted(offsets, key=lambda o: -(min(o[0], 4 - o[0]) + min(o[1], 4 - o[1]) + distance(o[2])))


IN_GROUP = [o for o in far_first(lambda dy: dy) if o != (0, 0, 0)]
IN_NEAR = far_first(lambda dy: dy)


def kernel(
    start_hbm, tpl_hbm, spec_hbm, first_hbm, turn_hbm, jump_hbm, second_hbm, out_ref,
    start, tpl, spec, first, turn, jump, second, rows, mine, got, other, chunk, beside, beside2, flat,
    bank, strain, firsts, turns, mid, mid2, peak, norm, sent, back, wide,
    load_sem, send_sem, recv_sem,
):
    g = lax.axis_index("group")
    f = lax.axis_index("freq")
    far = lax.rem(g + 2, 4)
    near = g + 1 - 2 * lax.rem(g, 2)
    count = 32
    peers = count - 1
    z, x, y = f // 8, lax.rem(f, 8) // 2, lax.rem(f, 2)
    part_z = [8 * lax.rem(z + d, 4) for d in range(4)]
    part_x = [2 * lax.rem(x + d, 4) for d in range(4)]
    part_y = [y, 1 - y]

    def at(offset):
        return part_z[offset[0]] + part_x[offset[1]] + part_y[offset[2]]

    loads = [
        pltpu.make_async_copy(src, dst, load_sem.at[i])
        for i, (src, dst) in enumerate(
            [
                (tpl_hbm, tpl), (spec_hbm, spec), (start_hbm, start),
                (first_hbm, first), (turn_hbm, turn), (jump_hbm, jump), (second_hbm, second),
            ]
        )
    ]
    for load in loads:
        load.start()

    barrier = pltpu.get_barrier_semaphore()
    pl.semaphore_signal(barrier, inc=1, device_id=(far, f), device_id_type=MESH)
    for o in IN_NEAR:
        pl.semaphore_signal(barrier, inc=1, device_id=(near, at(o)), device_id_type=MESH)
        if o in IN_GROUP:
            pl.semaphore_signal(barrier, inc=1, device_id=(g, at(o)), device_id_type=MESH)

    for load in loads:
        load.wait()

    peak[...] = jnp.zeros_like(peak)
    norm[...] = jnp.ones_like(norm)

    for j in range(5):
        block = jnp.concatenate(
            [tpl[:, q, 128 * j:128 * (j + 1)].astype(F32) for q in range(2)], 0
        )
        rows[128 * j:128 * (j + 1), :] = block.T
    own = jnp.concatenate([spec[0].astype(F32), spec[1].astype(F32)], 1).astype(BF16)

    def fill(i, carry):
        for q in range(5):
            mine[i, q] = rows[pl.ds(i + 128 * q, 4, stride=32), :].astype(BF16)
        mine[i, 5] = own
        return carry

    lax.fori_loop(0, count, fill, 0)

    got[f] = mine[f]

    pl.semaphore_wait(barrier, 2 * count)

    def copy(src, dst, kind, to):
        return pltpu.make_async_remote_copy(
            src_ref=src, dst_ref=dst, send_sem=send_sem.at[kind], recv_sem=recv_sem.at[kind],
            device_id=to, device_id_type=MESH,
        )

    to_far = copy(mine.at[f, 5], chunk, 0, (far, f))
    to_far.start()
    for o in IN_NEAR:
        if o in IN_GROUP:
            copy(mine.at[at(o)], got.at[f], 1, (g, at(o))).start()
        copy(mine.at[f, 5], other.at[f], 2, (near, at(o))).start()

    all_group = copy(mine.at[pl.ds(0, peers)], got.at[pl.ds(0, peers)], 1, (near, f))
    all_near = copy(other, other, 2, (near, f))
    all_beside = copy(beside.at[pl.ds(0, peers)], beside.at[pl.ds(0, peers)], 3, (near, f))
    all_beside2 = copy(beside2, beside2, 4, (near, f))
    all_shared = copy(back.at[pl.ds(0, peers)], back.at[pl.ds(0, peers)], 5, (near, f))
    def shift(s, carry):
        begin = start[s]
        low, high = lax.rem(begin, SIDE), lax.div(begin, SIDE)
        for q in range(2):
            firsts[s, SIDE * q:SIDE * (q + 1), :] = first[q, pl.ds(low, SIDE), :].astype(BF16)
        w0, w1 = turn[0, pl.ds(low, SIDE), :], turn[1, pl.ds(low, SIDE), :]
        r0, r1 = jump[0, pl.ds(high, 1), :], jump[1, pl.ds(high, 1), :]
        turns[s, 0] = w0 * r0 - w1 * r1
        turns[s, 1] = w0 * r1 + w1 * r0
        return carry

    lax.fori_loop(0, SEGS, shift, 0)

    to_far.wait_recv()
    for o in IN_NEAR:
        if o in IN_GROUP:
            copy(chunk, beside.at[f], 3, (g, at(o))).start()
        copy(chunk, beside2.at[f], 4, (near, at(o))).start()
    beside[f] = chunk[...]

    all_group.wait_recv()

    left = lax.broadcasted_iota(jnp.int32, (ACROSS, 128), 1) < SIDE

    def swapped(x):
        return pltpu.roll(x, SIDE, 1)

    for i in range(ACROSS):
        for q in range(5):
            flat[24 * i + 4 * q:24 * i + 4 * q + 4, :] = got[i, q].astype(F32)
    for p in range(PAIRS):
        one = flat[pl.ds(p, ACROSS, stride=24), :]
        two = flat[pl.ds(p + PAIRS, ACROSS, stride=24), :]
        re = jnp.where(left, one, swapped(two))
        im = jnp.where(left, swapped(one), two)
        bank[p, 0] = re
        bank[p, 1] = im
        total = jnp.sum(re * re + im * im, axis=0, keepdims=True)
        norm[8 * p:8 * (p + 1), :] = jnp.broadcast_to(total, (8, 128))

    def place(source, home):
        for i in range(ACROSS):
            flat[24 * i:24 * i + 4, :] = source(i).astype(F32)
        for q in range(4):
            row = flat[pl.ds(q, ACROSS, stride=24), :]
            turned = swapped(row)
            strain[4 * home + q, 0] = jnp.where(left, row, turned)
            strain[4 * home + q, 1] = jnp.where(left, turned, row)

    table2 = second[...]
    half = g // 2

    def across(u, low, dst):
        held = [(bank[2 * u + i, 0], bank[2 * u + i, 1]) for i in range(2)]
        for q in range(4):
            for k in range(2):
                s = 2 * low + q + 4 * k
                d0, d1 = strain[s, 0], strain[s, 1]
                crosses = [
                    jnp.concatenate([h0 * d0 + h1 * d1, h0 * d1 - h1 * d0], 0).astype(BF16) for h0, h1 in held
                ]
                y = jnp.dot(firsts[s], jnp.concatenate(crosses, 1), preferred_element_type=F32)
                w0, w1 = turns[s, 0], turns[s, 1]
                for i in range(2):
                    re, im = y[:SIDE, 128 * i:128 * (i + 1)], y[SIDE:, 128 * i:128 * (i + 1)]
                    dst[4 * i + q, :, 256 * k:256 * k + 128] = (re * w0 - im * w1).astype(BF16)
                    dst[4 * i + q, :, 256 * k + 128:256 * k + 256] = (re * w1 + im * w0).astype(BF16)

    def along(u, low, src):
        for i in range(2):
            z = jnp.dot(src[4 * i:4 * i + 4].reshape(4 * SIDE, 512), table2, preferred_element_type=F32)
            for q in range(4):
                re, im = z[SIDE * q:SIDE * (q + 1), 0:128], z[SIDE * q:SIDE * (q + 1), 128:256]
                peak[pl.ds(16 * u + 8 * i + low + q, 1), :] = jnp.max(re * re + im * im, axis=0, keepdims=True)

    def steps(low, one, two):
        def pair(i, carry):
            across(2 * i + 1, low, two)
            along(2 * i, low, one)
            across(2 * i + 2, low, one)
            along(2 * i + 1, low, two)
            return carry

        lax.fori_loop(0, 2, pair, 0)

    here, there = 4 * half, 4 - 4 * half
    place(lambda i: got[i, 5], g)
    all_near.wait_recv()
    place(lambda i: other[i], near)
    across(0, here, mid)
    steps(here, mid, mid2)
    all_beside.wait_recv()
    all_beside2.wait_recv()
    place(lambda i: beside[i], far)
    place(lambda i: beside2[i], lax.rem(near + 2, 4))
    across(0, there, mid2)
    along(4, here, mid)
    steps(there, mid2, mid)
    along(4, there, mid2)
    best = (peak[...] * jump[0, 40:41, :]).T
    power = norm[...].T
    power = [jnp.sum(power[SIDE * q:SIDE * (q + 1)], axis=0, keepdims=True) for q in range(2)]
    for k in range(4):
        sent[k:k + 1, :] = jnp.max(best[32 * k:32 * (k + 1)], axis=0, keepdims=True) / power[k % 2]
    back[f] = sent[...]

    for o in IN_GROUP:
        copy(sent, back.at[f], 5, (g, at(o))).start()
    for whole in (to_far, all_group, all_near, all_beside, all_beside2):
        whole.wait_send()
    all_shared.wait_recv()

    for i in range(count):
        for k in range(4):
            wide[32 * k + i:32 * k + i + 1, :] = back[i, k:k + 1, :]
    turned = wide[...].T
    lane = lax.broadcasted_iota(jnp.int32, (8, 128), 1)
    upper = lax.broadcasted_iota(jnp.int32, (8, 128), 0) < 4
    for c in range(5):
        blocks = []
        for k in range(2):
            block = None
            for n in range(4):
                q, p = divmod(4 * c + n, PAIRS)
                piece = turned[8 * p:8 * (p + 1), :]
                shift = (32 * n - 32 * q - 64 * k) % 128
                piece = pltpu.roll(piece, shift, 1) if shift else piece
                block = piece if block is None else jnp.where(lane >= 32 * n, piece, block)
            blocks.append(block)
        one, two = blocks
        out_ref[0:8, 128 * c:128 * (c + 1)] = jnp.where(upper, one, pltpu.roll(two, 4, 0))
        out_ref[8:16, 128 * c:128 * (c + 1)] = jnp.where(upper, pltpu.roll(one, 4, 0), two)

    all_shared.wait_send()


def on_device(spectra, templates, valid_start):
    first, turn, jump, second = tables()
    anywhere = pl.BlockSpec(memory_space=pl.ANY)
    dma = pltpu.SemaphoreType.DMA
    out = pl.pallas_call(
        kernel,
        out_shape=pltpu.VMEM((SEGS, 640), F32),
        in_specs=[anywhere] * 7,
        out_specs=pl.BlockSpec(memory_space=pltpu.VMEM),
        scratch_shapes=[
            pltpu.SMEM((SEGS,), jnp.int32),
            pltpu.VMEM((64, 2, 640), BF16),
            pltpu.VMEM((2, 4, 64), BF16),
            pltpu.VMEM(first.shape, F32),
            pltpu.VMEM(turn.shape, F32),
            pltpu.VMEM(jump.shape, F32),
            pltpu.VMEM(second.shape, BF16),
            pltpu.VMEM((640, 128), F32),
            pltpu.VMEM((32, 6, 4, 128), BF16),
            pltpu.VMEM((32, 6, 4, 128), BF16),
            pltpu.VMEM((32, 4, 128), BF16),
            pltpu.VMEM((4, 128), BF16),
            pltpu.VMEM((32, 4, 128), BF16),
            pltpu.VMEM((32, 4, 128), BF16),
            pltpu.VMEM((32 * 24, 128), F32),
            pltpu.VMEM((PAIRS, 2, ACROSS, 128), F32),
            pltpu.VMEM((SEGS, 2, ACROSS, 128), F32),
            pltpu.VMEM((SEGS, 128, 64), BF16),
            pltpu.VMEM((SEGS, 2, SIDE, 128), F32),
            pltpu.VMEM((8, SIDE, 512), BF16),
            pltpu.VMEM((8, SIDE, 512), BF16),
            pltpu.VMEM((128, 128), F32),
            pltpu.VMEM((128, 128), F32),
            pltpu.VMEM((4, 128), F32),
            pltpu.VMEM((32, 4, 128), F32),
            pltpu.VMEM((128, 128), F32),
            dma((7,)),
            dma((6,)),
            dma((6,)),
        ],
        compiler_params=pltpu.CompilerParams(collective_id=0, has_side_effects=True),
        name="matched_filter",
    )(valid_start, templates, jnp.transpose(spectra, (1, 2, 0)), first, turn, jump, second)
    return out.T


def solution(mesh):
    return jax.shard_map(
        on_device, mesh=mesh, in_specs=(P("freq", None, "group"), P("freq", None, "group"), P()),
        out_specs=P("group", None), check_vma=False,
    )
```

```python
import math

import jax
import jax.numpy as jnp
import numpy as np
from jax import lax
from jax.experimental import pallas as pl
from jax.experimental.pallas import tpu as pltpu
from jax.sharding import PartitionSpec as P

N = 4096
VALID = 2048
SIDE = 64
ACROSS = 32
PAIRS = 10
SEGS = 16
MESH = pl.DeviceIdType.MESH
F32 = jnp.float32
BF16 = jnp.bfloat16


def rounded_roots(index):
    exact = np.exp(2j * np.pi * (index % SIDE) / SIDE)
    least = np.full(index.shape[0], np.inf)
    table = np.zeros_like(exact)
    gain = np.ones(index.shape[0])
    for scale in np.linspace(1.0, 2.0, 2001)[:-1]:
        parts = [(x * scale).astype(jnp.bfloat16).astype(np.float64) for x in (exact.real, exact.imag)]
        tried = parts[0] + 1j * parts[1]
        level = (tried * exact.conj()).mean(1).real
        rest = (np.abs(tried / level[:, None] - exact) ** 2).mean(1)
        better = rest < least - 1e-15
        least = np.where(better, rest, least)
        table = np.where(better[:, None], tried, table)
        gain = np.where(better, level, gain)
    return table, gain


def tables():
    side = np.arange(SIDE)
    root, gain = rounded_roots(side[:, None] * np.arange(ACROSS)[None, :])
    first = np.stack([np.concatenate([root.real, -root.imag], 1), np.concatenate([root.imag, root.real], 1)], 0)
    first = np.tile(first, (1, 2, 1))
    lag = np.arange(2 * SIDE)
    turn = np.exp(2j * np.pi * lag[:, None] * side[None, :] / N) / np.tile(gain, 2)[:, None]
    turn = np.tile(np.stack([turn.real, turn.imag], 0), (1, 1, 2))
    root, gain = rounded_roots(side[:VALID // SIDE, None] * side[None, :])
    c, s = np.kron(np.eye(2), root.real.T), np.kron(np.eye(2), root.imag.T)
    none = np.zeros_like(c)
    second = np.concatenate(
        [
            np.concatenate([c, none, s, none], 1), np.concatenate([-s, none, c, none], 1),
            np.concatenate([none, c, none, s], 1), np.concatenate([none, -s, none, c], 1),
        ], 0,
    )
    jump = np.exp(2j * np.pi * np.arange(40)[:, None] * side[None, :] / SIDE)
    jump = np.tile(np.stack([jump.real, jump.imag], 0), (1, 1, 2))
    weight = np.tile(1.0 / gain ** 2, (2, 8, 4))
    jump = np.concatenate([jump, weight], 1)
    return jnp.asarray(first, F32), jnp.asarray(turn, F32), jnp.asarray(jump, F32), jnp.asarray(second, BF16)


def far_first(distance):
    offsets = [(dz, dx, dy) for dz in range(4) for dx in range(4) for dy in range(2)]
    return sorted(offsets, key=lambda o: -(min(o[0], 4 - o[0]) + min(o[1], 4 - o[1]) + distance(o[2])))


IN_GROUP = [o for o in far_first(lambda dy: dy) if o != (0, 0, 0)]
IN_NEAR = far_first(lambda dy: dy)
IN_FAR = far_first(lambda dy: 2 - dy)


def kernel(
    start_hbm, tpl_hbm, spec_hbm, first_hbm, turn_hbm, jump_hbm, second_hbm, out_ref,
    start, tpl, spec, first, turn, jump, second, rows, mine, got, other, chunk, beside, beside2, flat,
    bank, strain, firsts, turns, mid, mid2, peak, norm, sent, back, wide,
    load_sem, send_sem, recv_sem,
):
    g = lax.axis_index("group")
    f = lax.axis_index("freq")
    far = lax.rem(g + 2, 4)
    near = g + 1 - 2 * lax.rem(g, 2)
    count = 32
    peers = count - 1
    z, x, y = f // 8, lax.rem(f, 8) // 2, lax.rem(f, 2)
    part_z = [8 * lax.rem(z + d, 4) for d in range(4)]
    part_x = [2 * lax.rem(x + d, 4) for d in range(4)]
    part_y = [y, 1 - y]

    def at(offset):
        return part_z[offset[0]] + part_x[offset[1]] + part_y[offset[2]]

    loads = [
        pltpu.make_async_copy(src, dst, load_sem.at[i])
        for i, (src, dst) in enumerate(
            [
                (tpl_hbm, tpl), (spec_hbm, spec), (start_hbm, start),
                (first_hbm, first), (turn_hbm, turn), (jump_hbm, jump), (second_hbm, second),
            ]
        )
    ]
    for load in loads:
        load.start()

    barrier = pltpu.get_barrier_semaphore()
    across_g = lax.rem(near + 2, 4)
    late = g // 2
    pl.semaphore_signal(barrier, inc=1, device_id=(far, f), device_id_type=MESH)
    for o in IN_NEAR:
        pl.semaphore_signal(barrier, inc=1, device_id=(near, at(o)), device_id_type=MESH)
        if o in IN_GROUP:
            pl.semaphore_signal(barrier, inc=1, device_id=(g, at(o)), device_id_type=MESH)

    @pl.when(late == 0)
    def _():
        for o in IN_FAR:
            pl.semaphore_signal(barrier, inc=1, device_id=(across_g, at(o)), device_id_type=MESH)
            if o != (0, 0, 0):
                pl.semaphore_signal(barrier, inc=1, device_id=(far, at(o)), device_id_type=MESH)


    for load in loads:
        load.wait()

    peak[...] = jnp.zeros_like(peak)
    norm[...] = jnp.ones_like(norm)

    for j in range(5):
        block = jnp.concatenate(
            [tpl[:, q, 128 * j:128 * (j + 1)].astype(F32) for q in range(2)], 0
        )
        rows[128 * j:128 * (j + 1), :] = block.T
    own = jnp.concatenate([spec[0].astype(F32), spec[1].astype(F32)], 1).astype(BF16)

    def fill(i, carry):
        for q in range(5):
            mine[i, q] = rows[pl.ds(i + 128 * q, 4, stride=32), :].astype(BF16)
        mine[i, 5] = own
        return carry

    lax.fori_loop(0, count, fill, 0)

    got[f] = mine[f]

    pl.semaphore_wait(barrier, 2 * count + (2 * count - 1) * late)

    def copy(src, dst, kind, to):
        return pltpu.make_async_remote_copy(
            src_ref=src, dst_ref=dst, send_sem=send_sem.at[kind], recv_sem=recv_sem.at[kind],
            device_id=to, device_id_type=MESH,
        )

    own_chunk = mine.at[f, 5]
    to_far = copy(own_chunk, chunk, 0, (far, f))

    @pl.when(late == 0)
    def _():
        to_far.start()

    @pl.when(late == 1)
    def _():
        for o in IN_FAR:
            copy(own_chunk, beside.at[f], 3, (far, at(o))).start()
            copy(own_chunk, beside2.at[f], 4, (across_g, at(o))).start()

    for o in IN_NEAR:
        if o in IN_GROUP:
            copy(mine.at[at(o)], got.at[f], 1, (g, at(o))).start()
        copy(own_chunk, other.at[f], 2, (near, at(o))).start()

    all_group = copy(mine.at[pl.ds(0, peers)], got.at[pl.ds(0, peers)], 1, (near, f))
    all_near = copy(other, other, 2, (near, f))
    all_beside = copy(beside, beside, 3, (near, f))
    most_beside = copy(beside.at[pl.ds(0, peers)], beside.at[pl.ds(0, peers)], 3, (near, f))
    all_beside2 = copy(beside2, beside2, 4, (near, f))
    all_shared = copy(back.at[pl.ds(0, peers)], back.at[pl.ds(0, peers)], 5, (near, f))
    def shift(s, carry):
        begin = start[s]
        low, high = lax.rem(begin, SIDE), lax.div(begin, SIDE)
        for q in range(2):
            firsts[s, SIDE * q:SIDE * (q + 1), :] = first[q, pl.ds(low, SIDE), :].astype(BF16)
        w0, w1 = turn[0, pl.ds(low, SIDE), :], turn[1, pl.ds(low, SIDE), :]
        r0, r1 = jump[0, pl.ds(high, 1), :], jump[1, pl.ds(high, 1), :]
        turns[s, 0] = w0 * r0 - w1 * r1
        turns[s, 1] = w0 * r1 + w1 * r0
        return carry

    lax.fori_loop(0, SEGS, shift, 0)

    @pl.when(late == 1)
    def _():
        to_far.wait_recv()
        for o in IN_NEAR:
            if o in IN_GROUP:
                copy(chunk, beside.at[f], 3, (g, at(o))).start()
            copy(chunk, beside2.at[f], 4, (near, at(o))).start()
        beside[f] = chunk[...]

    all_group.wait_recv()

    left = lax.broadcasted_iota(jnp.int32, (ACROSS, 128), 1) < SIDE

    def swapped(x):
        return pltpu.roll(x, SIDE, 1)

    for i in range(ACROSS):
        for q in range(5):
            flat[24 * i + 4 * q:24 * i + 4 * q + 4, :] = got[i, q].astype(F32)
    for p in range(PAIRS):
        one = flat[pl.ds(p, ACROSS, stride=24), :]
        two = flat[pl.ds(p + PAIRS, ACROSS, stride=24), :]
        re = jnp.where(left, one, swapped(two))
        im = jnp.where(left, swapped(one), two)
        bank[p, 0] = re
        bank[p, 1] = im
        total = jnp.sum(re * re + im * im, axis=0, keepdims=True)
        norm[8 * p:8 * (p + 1), :] = jnp.broadcast_to(total, (8, 128))

    def place(source, home):
        for i in range(ACROSS):
            flat[24 * i:24 * i + 4, :] = source(i).astype(F32)
        for q in range(4):
            row = flat[pl.ds(q, ACROSS, stride=24), :]
            turned = swapped(row)
            strain[4 * home + q, 0] = jnp.where(left, row, turned)
            strain[4 * home + q, 1] = jnp.where(left, turned, row)

    table2 = second[...]
    half = g // 2

    def across(u, low, dst):
        held = [(bank[2 * u + i, 0], bank[2 * u + i, 1]) for i in range(2)]
        for q in range(4):
            for k in range(2):
                s = 2 * low + q + 4 * k
                d0, d1 = strain[s, 0], strain[s, 1]
                crosses = [
                    jnp.concatenate([h0 * d0 + h1 * d1, h0 * d1 - h1 * d0], 0).astype(BF16) for h0, h1 in held
                ]
                y = jnp.dot(firsts[s], jnp.concatenate(crosses, 1), preferred_element_type=F32)
                w0, w1 = turns[s, 0], turns[s, 1]
                for i in range(2):
                    re, im = y[:SIDE, 128 * i:128 * (i + 1)], y[SIDE:, 128 * i:128 * (i + 1)]
                    dst[4 * i + q, :, 256 * k:256 * k + 128] = (re * w0 - im * w1).astype(BF16)
                    dst[4 * i + q, :, 256 * k + 128:256 * k + 256] = (re * w1 + im * w0).astype(BF16)

    def along(u, low, src):
        for i in range(2):
            z = jnp.dot(src[4 * i:4 * i + 4].reshape(4 * SIDE, 512), table2, preferred_element_type=F32)
            for q in range(4):
                re, im = z[SIDE * q:SIDE * (q + 1), 0:128], z[SIDE * q:SIDE * (q + 1), 128:256]
                peak[pl.ds(16 * u + 8 * i + low + q, 1), :] = jnp.max(re * re + im * im, axis=0, keepdims=True)

    def steps(low, one, two):
        def pair(i, carry):
            across(2 * i + 1, low, two)
            along(2 * i, low, one)
            across(2 * i + 2, low, one)
            along(2 * i + 1, low, two)
            return carry

        lax.fori_loop(0, 2, pair, 0)

    here, there = 4 * half, 4 - 4 * half
    place(lambda i: got[i, 5], g)
    all_near.wait_recv()
    place(lambda i: other[i], near)
    across(0, here, mid)
    steps(here, mid, mid2)
    @pl.when(late == 0)
    def _():
        all_beside.wait_recv()

    @pl.when(late == 1)
    def _():
        most_beside.wait_recv()

    all_beside2.wait_recv()
    place(lambda i: beside[i], far)
    place(lambda i: beside2[i], across_g)
    across(0, there, mid2)
    along(4, here, mid)
    steps(there, mid2, mid)
    along(4, there, mid2)
    best = (peak[...] * jump[0, 40:41, :]).T
    power = norm[...].T
    power = [jnp.sum(power[SIDE * q:SIDE * (q + 1)], axis=0, keepdims=True) for q in range(2)]
    for k in range(4):
        sent[k:k + 1, :] = jnp.max(best[32 * k:32 * (k + 1)], axis=0, keepdims=True) / power[k % 2]
    back[f] = sent[...]

    for o in IN_GROUP:
        copy(sent, back.at[f], 5, (g, at(o))).start()
    all_group.wait_send()
    all_near.wait_send()

    @pl.when(late == 0)
    def _():
        to_far.wait_send()

    @pl.when(late == 1)
    def _():
        for whole in (all_beside, most_beside, all_beside2, all_beside2):
            whole.wait_send()

    all_shared.wait_recv()

    for i in range(count):
        for k in range(4):
            wide[32 * k + i:32 * k + i + 1, :] = back[i, k:k + 1, :]
    turned = wide[...].T
    lane = lax.broadcasted_iota(jnp.int32, (8, 128), 1)
    upper = lax.broadcasted_iota(jnp.int32, (8, 128), 0) < 4
    for c in range(5):
        blocks = []
        for k in range(2):
            block = None
            for n in range(4):
                q, p = divmod(4 * c + n, PAIRS)
                piece = turned[8 * p:8 * (p + 1), :]
                shift = (32 * n - 32 * q - 64 * k) % 128
                piece = pltpu.roll(piece, shift, 1) if shift else piece
                block = piece if block is None else jnp.where(lane >= 32 * n, piece, block)
            blocks.append(block)
        one, two = blocks
        out_ref[0:8, 128 * c:128 * (c + 1)] = jnp.where(upper, one, pltpu.roll(two, 4, 0))
        out_ref[8:16, 128 * c:128 * (c + 1)] = jnp.where(upper, pltpu.roll(one, 4, 0), two)

    all_shared.wait_send()


def on_device(spectra, templates, valid_start):
    first, turn, jump, second = tables()
    anywhere = pl.BlockSpec(memory_space=pl.ANY)
    dma = pltpu.SemaphoreType.DMA
    out = pl.pallas_call(
        kernel,
        out_shape=pltpu.VMEM((SEGS, 640), F32),
        in_specs=[anywhere] * 7,
        out_specs=pl.BlockSpec(memory_space=pltpu.VMEM),
        scratch_shapes=[
            pltpu.SMEM((SEGS,), jnp.int32),
            pltpu.VMEM((64, 2, 640), BF16),
            pltpu.VMEM((2, 4, 64), BF16),
            pltpu.VMEM(first.shape, F32),
            pltpu.VMEM(turn.shape, F32),
            pltpu.VMEM(jump.shape, F32),
            pltpu.VMEM(second.shape, BF16),
            pltpu.VMEM((640, 128), F32),
            pltpu.VMEM((32, 6, 4, 128), BF16),
            pltpu.VMEM((32, 6, 4, 128), BF16),
            pltpu.VMEM((32, 4, 128), BF16),
            pltpu.VMEM((4, 128), BF16),
            pltpu.VMEM((32, 4, 128), BF16),
            pltpu.VMEM((32, 4, 128), BF16),
            pltpu.VMEM((32 * 24, 128), F32),
            pltpu.VMEM((PAIRS, 2, ACROSS, 128), F32),
            pltpu.VMEM((SEGS, 2, ACROSS, 128), F32),
            pltpu.VMEM((SEGS, 128, 64), BF16),
            pltpu.VMEM((SEGS, 2, SIDE, 128), F32),
            pltpu.VMEM((8, SIDE, 512), BF16),
            pltpu.VMEM((8, SIDE, 512), BF16),
            pltpu.VMEM((128, 128), F32),
            pltpu.VMEM((128, 128), F32),
            pltpu.VMEM((4, 128), F32),
            pltpu.VMEM((32, 4, 128), F32),
            pltpu.VMEM((128, 128), F32),
            dma((7,)),
            dma((6,)),
            dma((6,)),
        ],
        compiler_params=pltpu.CompilerParams(collective_id=0, has_side_effects=True),
        name="matched_filter",
    )(valid_start, templates, jnp.transpose(spectra, (1, 2, 0)), first, turn, jump, second)
    return out.T


def solution(mesh):
    return jax.shard_map(
        on_device, mesh=mesh, in_specs=(P("freq", None, "group"), P("freq", None, "group"), P()),
        out_specs=P("group", None), check_vma=False,
    )
```

```python
import math

import jax
import jax.numpy as jnp
import numpy as np
from jax import lax
from jax.experimental import pallas as pl
from jax.experimental.pallas import tpu as pltpu
from jax.sharding import PartitionSpec as P

N = 4096
VALID = 2048
SIDE = 64
ACROSS = 32
PAIRS = 10
SEGS = 16
MESH = pl.DeviceIdType.MESH
F32 = jnp.float32
BF16 = jnp.bfloat16


def rounded_roots(index):
    exact = np.exp(2j * np.pi * (index % SIDE) / SIDE)
    least = np.full(index.shape[0], np.inf)
    table = np.zeros_like(exact)
    gain = np.ones(index.shape[0])
    for scale in np.linspace(1.0, 2.0, 2001)[:-1]:
        parts = [(x * scale).astype(jnp.bfloat16).astype(np.float64) for x in (exact.real, exact.imag)]
        tried = parts[0] + 1j * parts[1]
        level = (tried * exact.conj()).mean(1).real
        rest = (np.abs(tried / level[:, None] - exact) ** 2).mean(1)
        better = rest < least - 1e-15
        least = np.where(better, rest, least)
        table = np.where(better[:, None], tried, table)
        gain = np.where(better, level, gain)
    return table, gain


def tables():
    side = np.arange(SIDE)
    root, gain = rounded_roots(side[:, None] * np.arange(ACROSS)[None, :])
    first = np.stack([np.concatenate([root.real, -root.imag], 1), np.concatenate([root.imag, root.real], 1)], 0)
    first = np.tile(first, (1, 2, 1))
    lag = np.arange(2 * SIDE)
    turn = np.exp(2j * np.pi * lag[:, None] * side[None, :] / N) / np.tile(gain, 2)[:, None]
    turn = np.tile(np.stack([turn.real, turn.imag], 0), (1, 1, 2))
    root, gain = rounded_roots(side[:VALID // SIDE, None] * side[None, :])
    c, s = np.kron(np.eye(2), root.real.T), np.kron(np.eye(2), root.imag.T)
    none = np.zeros_like(c)
    second = np.concatenate(
        [
            np.concatenate([c, none, s, none], 1), np.concatenate([-s, none, c, none], 1),
            np.concatenate([none, c, none, s], 1), np.concatenate([none, -s, none, c], 1),
        ], 0,
    )
    jump = np.exp(2j * np.pi * np.arange(40)[:, None] * side[None, :] / SIDE)
    jump = np.tile(np.stack([jump.real, jump.imag], 0), (1, 1, 2))
    weight = np.tile(1.0 / gain ** 2, (2, 8, 4))
    jump = np.concatenate([jump, weight], 1)
    return jnp.asarray(first, F32), jnp.asarray(turn, F32), jnp.asarray(jump, F32), jnp.asarray(second, BF16)


def far_first(kinds):
    def hops(entry):
        (kind, (dz, dx, dy)) = entry
        return min(dz, 4 - dz) + min(dx, 4 - dx) + (2 - dy if kind in (FAR, BEYOND) else dy)

    offsets = [(dz, dx, dy) for dz in range(4) for dx in range(4) for dy in range(2)]
    entries = [(kind, o) for o in offsets for kind in kinds if (kind, o) != (GROUP, (0, 0, 0))]
    return sorted(entries, key=lambda entry: (-hops(entry), kinds.index(entry[0])))


GROUP, NEAR, FAR, BEYOND = range(4)


def kernel(
    start_hbm, tpl_hbm, spec_hbm, first_hbm, turn_hbm, jump_hbm, second_hbm, out_ref,
    start, tpl, spec, first, turn, jump, second, rows, mine, got, other, chunk, beside, beside2, flat,
    bank, strain, firsts, turns, mid, mid2, peak, norm, sent, back, wide,
    load_sem, send_sem, recv_sem,
):
    g = lax.axis_index("group")
    f = lax.axis_index("freq")
    far = lax.rem(g + 2, 4)
    near = g + 1 - 2 * lax.rem(g, 2)
    count = 32
    peers = count - 1
    z, x, y = f // 8, lax.rem(f, 8) // 2, lax.rem(f, 2)
    part_z = [8 * lax.rem(z + d, 4) for d in range(4)]
    part_x = [2 * lax.rem(x + d, 4) for d in range(4)]
    part_y = [y, 1 - y]

    def at(offset):
        return part_z[offset[0]] + part_x[offset[1]] + part_y[offset[2]]

    loads = [
        pltpu.make_async_copy(src, dst, load_sem.at[i])
        for i, (src, dst) in enumerate(
            [
                (tpl_hbm, tpl), (spec_hbm, spec), (start_hbm, start),
                (first_hbm, first), (turn_hbm, turn), (jump_hbm, jump), (second_hbm, second),
            ]
        )
    ]
    for load in loads:
        load.start()

    barrier = pltpu.get_barrier_semaphore()
    across_g = lax.rem(near + 2, 4)
    late = g // 2
    group_of = (g, near, far, across_g)
    pl.semaphore_signal(barrier, inc=1, device_id=(far, f), device_id_type=MESH)
    for kind, o in far_first((GROUP, NEAR)):
        pl.semaphore_signal(barrier, inc=1, device_id=(group_of[kind], at(o)), device_id_type=MESH)

    @pl.when(late == 0)
    def _():
        for kind, o in far_first((FAR, BEYOND)):
            if (kind, o) != (FAR, (0, 0, 0)):
                pl.semaphore_signal(barrier, inc=1, device_id=(group_of[kind], at(o)), device_id_type=MESH)

    for load in loads:
        load.wait()

    peak[...] = jnp.zeros_like(peak)
    norm[...] = jnp.ones_like(norm)

    for j in range(5):
        block = jnp.concatenate(
            [tpl[:, q, 128 * j:128 * (j + 1)].astype(F32) for q in range(2)], 0
        )
        rows[128 * j:128 * (j + 1), :] = block.T
    own = jnp.concatenate([spec[0].astype(F32), spec[1].astype(F32)], 1).astype(BF16)

    def fill(i, carry):
        for q in range(5):
            mine[i, q] = rows[pl.ds(i + 128 * q, 4, stride=32), :].astype(BF16)
        mine[i, 5] = own
        return carry

    lax.fori_loop(0, count, fill, 0)

    got[f] = mine[f]

    pl.semaphore_wait(barrier, 2 * count + (2 * count - 1) * late)

    def copy(src, dst, kind, to):
        return pltpu.make_async_remote_copy(
            src_ref=src, dst_ref=dst, send_sem=send_sem.at[kind], recv_sem=recv_sem.at[kind],
            device_id=to, device_id_type=MESH,
        )

    own_chunk = mine.at[f, 5]
    to_far = copy(own_chunk, chunk, 0, (far, f))

    def give(kind, to):
        if kind == GROUP:
            return copy(mine.at[to], got.at[f], 1, (g, to))
        return copy(own_chunk, (other, beside, beside2)[kind - 1].at[f], kind + 1, (group_of[kind], to))

    @pl.when(late == 0)
    def _():
        to_far.start()
        for kind, o in far_first((GROUP, NEAR)):
            give(kind, at(o)).start()

    @pl.when(late == 1)
    def _():
        for kind, o in far_first((GROUP, NEAR, FAR, BEYOND)):
            give(kind, at(o)).start()

    all_group = copy(mine.at[pl.ds(0, peers)], got.at[pl.ds(0, peers)], 1, (near, f))
    all_near = copy(other, other, 2, (near, f))
    all_beside = copy(beside, beside, 3, (near, f))
    most_beside = copy(beside.at[pl.ds(0, peers)], beside.at[pl.ds(0, peers)], 3, (near, f))
    all_beside2 = copy(beside2, beside2, 4, (near, f))
    all_shared = copy(back.at[pl.ds(0, peers)], back.at[pl.ds(0, peers)], 5, (near, f))
    def shift(s, carry):
        begin = start[s]
        low, high = lax.rem(begin, SIDE), lax.div(begin, SIDE)
        for q in range(2):
            firsts[s, SIDE * q:SIDE * (q + 1), :] = first[q, pl.ds(low, SIDE), :].astype(BF16)
        w0, w1 = turn[0, pl.ds(low, SIDE), :], turn[1, pl.ds(low, SIDE), :]
        r0, r1 = jump[0, pl.ds(high, 1), :], jump[1, pl.ds(high, 1), :]
        turns[s, 0] = w0 * r0 - w1 * r1
        turns[s, 1] = w0 * r1 + w1 * r0
        return carry

    lax.fori_loop(0, SEGS, shift, 0)

    @pl.when(late == 1)
    def _():
        to_far.wait_recv()
        for kind, o in far_first((GROUP, NEAR)):
            copy(chunk, (beside, beside2)[kind].at[f], 3 + kind, (group_of[kind], at(o))).start()
        beside[f] = chunk[...]

    all_group.wait_recv()

    left = lax.broadcasted_iota(jnp.int32, (ACROSS, 128), 1) < SIDE

    def swapped(x):
        return pltpu.roll(x, SIDE, 1)

    for i in range(ACROSS):
        for q in range(5):
            flat[24 * i + 4 * q:24 * i + 4 * q + 4, :] = got[i, q].astype(F32)
    for p in range(PAIRS):
        one = flat[pl.ds(p, ACROSS, stride=24), :]
        two = flat[pl.ds(p + PAIRS, ACROSS, stride=24), :]
        re = jnp.where(left, one, swapped(two))
        im = jnp.where(left, swapped(one), two)
        bank[p, 0] = re
        bank[p, 1] = im
        total = jnp.sum(re * re + im * im, axis=0, keepdims=True)
        norm[8 * p:8 * (p + 1), :] = jnp.broadcast_to(total, (8, 128))

    def place(source, home):
        for i in range(ACROSS):
            flat[24 * i:24 * i + 4, :] = source(i).astype(F32)
        for q in range(4):
            row = flat[pl.ds(q, ACROSS, stride=24), :]
            turned = swapped(row)
            strain[4 * home + q, 0] = jnp.where(left, row, turned)
            strain[4 * home + q, 1] = jnp.where(left, turned, row)

    table2 = second[...]
    half = g // 2

    def across(u, low, dst):
        held = [(bank[2 * u + i, 0], bank[2 * u + i, 1]) for i in range(2)]
        for q in range(4):
            for k in range(2):
                s = 2 * low + q + 4 * k
                d0, d1 = strain[s, 0], strain[s, 1]
                crosses = [
                    jnp.concatenate([h0 * d0 + h1 * d1, h0 * d1 - h1 * d0], 0).astype(BF16) for h0, h1 in held
                ]
                y = jnp.dot(firsts[s], jnp.concatenate(crosses, 1), preferred_element_type=F32)
                w0, w1 = turns[s, 0], turns[s, 1]
                for i in range(2):
                    re, im = y[:SIDE, 128 * i:128 * (i + 1)], y[SIDE:, 128 * i:128 * (i + 1)]
                    dst[4 * i + q, :, 256 * k:256 * k + 128] = (re * w0 - im * w1).astype(BF16)
                    dst[4 * i + q, :, 256 * k + 128:256 * k + 256] = (re * w1 + im * w0).astype(BF16)

    def along(u, low, src):
        for i in range(2):
            z = jnp.dot(src[4 * i:4 * i + 4].reshape(4 * SIDE, 512), table2, preferred_element_type=F32)
            for q in range(4):
                re, im = z[SIDE * q:SIDE * (q + 1), 0:128], z[SIDE * q:SIDE * (q + 1), 128:256]
                peak[pl.ds(16 * u + 8 * i + low + q, 1), :] = jnp.max(re * re + im * im, axis=0, keepdims=True)

    def steps(low, one, two):
        for i in range(2):
            across(2 * i + 1, low, two)
            along(2 * i, low, one)
            across(2 * i + 2, low, one)
            along(2 * i + 1, low, two)

    here, there = 4 * half, 4 - 4 * half
    place(lambda i: got[i, 5], g)
    all_near.wait_recv()
    place(lambda i: other[i], near)
    across(0, here, mid)
    steps(here, mid, mid2)
    @pl.when(late == 0)
    def _():
        all_beside.wait_recv()

    @pl.when(late == 1)
    def _():
        most_beside.wait_recv()

    all_beside2.wait_recv()
    place(lambda i: beside[i], far)
    place(lambda i: beside2[i], across_g)
    across(0, there, mid2)
    along(4, here, mid)
    steps(there, mid2, mid)
    along(4, there, mid2)
    best = (peak[...] * jump[0, 40:41, :]).T
    power = norm[...].T
    power = [jnp.sum(power[SIDE * q:SIDE * (q + 1)], axis=0, keepdims=True) for q in range(2)]
    for k in range(4):
        sent[k:k + 1, :] = jnp.max(best[32 * k:32 * (k + 1)], axis=0, keepdims=True) / power[k % 2]
    back[f] = sent[...]

    for _, o in far_first((GROUP,)):
        copy(sent, back.at[f], 5, (g, at(o))).start()
    all_group.wait_send()
    all_near.wait_send()

    @pl.when(late == 0)
    def _():
        to_far.wait_send()

    @pl.when(late == 1)
    def _():
        for whole in (all_beside, most_beside, all_beside2, all_beside2):
            whole.wait_send()

    all_shared.wait_recv()

    for i in range(count):
        for k in range(4):
            wide[32 * k + i:32 * k + i + 1, :] = back[i, k:k + 1, :]
    turned = wide[...].T
    lane = lax.broadcasted_iota(jnp.int32, (8, 128), 1)
    upper = lax.broadcasted_iota(jnp.int32, (8, 128), 0) < 4
    for c in range(5):
        blocks = []
        for k in range(2):
            block = None
            for n in range(4):
                q, p = divmod(4 * c + n, PAIRS)
                piece = turned[8 * p:8 * (p + 1), :]
                shift = (32 * n - 32 * q - 64 * k) % 128
                piece = pltpu.roll(piece, shift, 1) if shift else piece
                block = piece if block is None else jnp.where(lane >= 32 * n, piece, block)
            blocks.append(block)
        one, two = blocks
        out_ref[0:8, 128 * c:128 * (c + 1)] = jnp.where(upper, one, pltpu.roll(two, 4, 0))
        out_ref[8:16, 128 * c:128 * (c + 1)] = jnp.where(upper, pltpu.roll(one, 4, 0), two)

    all_shared.wait_send()


def on_device(spectra, templates, valid_start):
    first, turn, jump, second = tables()
    anywhere = pl.BlockSpec(memory_space=pl.ANY)
    dma = pltpu.SemaphoreType.DMA
    out = pl.pallas_call(
        kernel,
        out_shape=pltpu.VMEM((SEGS, 640), F32),
        in_specs=[anywhere] * 7,
        out_specs=pl.BlockSpec(memory_space=pltpu.VMEM),
        scratch_shapes=[
            pltpu.SMEM((SEGS,), jnp.int32),
            pltpu.VMEM((64, 2, 640), BF16),
            pltpu.VMEM((2, 4, 64), BF16),
            pltpu.VMEM(first.shape, F32),
            pltpu.VMEM(turn.shape, F32),
            pltpu.VMEM(jump.shape, F32),
            pltpu.VMEM(second.shape, BF16),
            pltpu.VMEM((640, 128), F32),
            pltpu.VMEM((32, 6, 4, 128), BF16),
            pltpu.VMEM((32, 6, 4, 128), BF16),
            pltpu.VMEM((32, 4, 128), BF16),
            pltpu.VMEM((4, 128), BF16),
            pltpu.VMEM((32, 4, 128), BF16),
            pltpu.VMEM((32, 4, 128), BF16),
            pltpu.VMEM((32 * 24, 128), F32),
            pltpu.VMEM((PAIRS, 2, ACROSS, 128), F32),
            pltpu.VMEM((SEGS, 2, ACROSS, 128), F32),
            pltpu.VMEM((SEGS, 128, 64), BF16),
            pltpu.VMEM((SEGS, 2, SIDE, 128), F32),
            pltpu.VMEM((8, SIDE, 512), BF16),
            pltpu.VMEM((8, SIDE, 512), BF16),
            pltpu.VMEM((128, 128), F32),
            pltpu.VMEM((128, 128), F32),
            pltpu.VMEM((4, 128), F32),
            pltpu.VMEM((32, 4, 128), F32),
            pltpu.VMEM((128, 128), F32),
            dma((7,)),
            dma((6,)),
            dma((6,)),
        ],
        compiler_params=pltpu.CompilerParams(collective_id=0, has_side_effects=True),
        name="matched_filter",
    )(valid_start, templates, jnp.transpose(spectra, (1, 2, 0)), first, turn, jump, second)
    return out.T


def solution(mesh):
    return jax.shard_map(
        on_device, mesh=mesh, in_specs=(P("freq", None, "group"), P("freq", None, "group"), P()),
        out_specs=P("group", None), check_vma=False,
    )
```

```python
import math

import jax
import jax.numpy as jnp
import numpy as np
from jax import lax
from jax.experimental import pallas as pl
from jax.experimental.pallas import tpu as pltpu
from jax.sharding import PartitionSpec as P

N = 4096
VALID = 2048
SIDE = 64
ACROSS = 32
PAIRS = 10
SEGS = 16
MESH = pl.DeviceIdType.MESH
F32 = jnp.float32
BF16 = jnp.bfloat16


def rounded_roots(index):
    exact = np.exp(2j * np.pi * (index % SIDE) / SIDE)
    least = np.full(index.shape[0], np.inf)
    table = np.zeros_like(exact)
    gain = np.ones(index.shape[0])
    for scale in np.linspace(1.0, 2.0, 2001)[:-1]:
        parts = [(x * scale).astype(jnp.bfloat16).astype(np.float64) for x in (exact.real, exact.imag)]
        tried = parts[0] + 1j * parts[1]
        level = (tried * exact.conj()).mean(1).real
        rest = (np.abs(tried / level[:, None] - exact) ** 2).mean(1)
        better = rest < least - 1e-15
        least = np.where(better, rest, least)
        table = np.where(better[:, None], tried, table)
        gain = np.where(better, level, gain)
    return table, gain


def tables():
    side = np.arange(SIDE)
    root, gain = rounded_roots(side[:, None] * np.arange(ACROSS)[None, :])
    first = np.stack([np.concatenate([root.real, -root.imag], 1), np.concatenate([root.imag, root.real], 1)], 0)
    first = np.tile(first, (1, 2, 1))
    lag = np.arange(2 * SIDE)
    turn = np.exp(2j * np.pi * lag[:, None] * side[None, :] / N) / np.tile(gain, 2)[:, None]
    turn = np.tile(np.stack([turn.real, turn.imag], 0), (1, 1, 2))
    root, gain = rounded_roots(side[:VALID // SIDE, None] * side[None, :])
    c, s = np.kron(np.eye(2), root.real.T), np.kron(np.eye(2), root.imag.T)
    none = np.zeros_like(c)
    second = np.concatenate(
        [
            np.concatenate([c, none, s, none], 1), np.concatenate([-s, none, c, none], 1),
            np.concatenate([none, c, none, s], 1), np.concatenate([none, -s, none, c], 1),
        ], 0,
    )
    jump = np.exp(2j * np.pi * np.arange(40)[:, None] * side[None, :] / SIDE)
    jump = np.tile(np.stack([jump.real, jump.imag], 0), (1, 1, 2))
    weight = np.tile(1.0 / gain ** 2, (2, 8, 4))
    jump = np.concatenate([jump, weight], 1)
    return jnp.asarray(first, F32), jnp.asarray(turn, F32), jnp.asarray(jump, F32), jnp.asarray(second, BF16)


def far_first(kinds):
    def hops(entry):
        (kind, (dz, dx, dy)) = entry
        return min(dz, 4 - dz) + min(dx, 4 - dx) + (2 - dy if kind == FAR else dy)

    offsets = [(dz, dx, dy) for dz in range(4) for dx in range(4) for dy in range(2)]
    entries = [(kind, o) for o in offsets for kind in kinds if (kind, o) != (GROUP, (0, 0, 0))]
    return sorted(entries, key=lambda entry: (-hops(entry), kinds.index(entry[0])))


GROUP, FAR = range(2)


def kernel(
    start_hbm, tpl_hbm, spec_hbm, first_hbm, turn_hbm, jump_hbm, second_hbm, out_ref,
    start, tpl, spec, first, turn, jump, second, rows, mine, got, other, chunk, beside, beside2, flat,
    bank, strain, firsts, turns, mid, mid2, peak, norm, sent, back, wide,
    load_sem, send_sem, recv_sem,
):
    g = lax.axis_index("group")
    f = lax.axis_index("freq")
    far = lax.rem(g + 2, 4)
    near = g + 1 - 2 * lax.rem(g, 2)
    count = 32
    peers = count - 1
    z, x, y = f // 8, lax.rem(f, 8) // 2, lax.rem(f, 2)
    part_z = [8 * lax.rem(z + d, 4) for d in range(4)]
    part_x = [2 * lax.rem(x + d, 4) for d in range(4)]
    part_y = [y, 1 - y]

    def at(offset):
        return part_z[offset[0]] + part_x[offset[1]] + part_y[offset[2]]

    loads = [
        pltpu.make_async_copy(src, dst, load_sem.at[i])
        for i, (src, dst) in enumerate(
            [
                (tpl_hbm, tpl), (spec_hbm, spec), (start_hbm, start),
                (first_hbm, first), (turn_hbm, turn), (jump_hbm, jump), (second_hbm, second),
            ]
        )
    ]
    for load in loads:
        load.start()

    barrier = pltpu.get_barrier_semaphore()
    across_g = lax.rem(near + 2, 4)
    late = g // 2
    group_of = (g, far)
    pl.semaphore_signal(barrier, inc=1, device_id=(far, f), device_id_type=MESH)
    for _, o in far_first((GROUP,)):
        pl.semaphore_signal(barrier, inc=1, device_id=(g, at(o)), device_id_type=MESH)
    pl.semaphore_signal(barrier, inc=1, device_id=(near, f), device_id_type=MESH)

    @pl.when(late == 0)
    def _():
        for _, o in far_first((FAR,)):
            if o != (0, 0, 0):
                pl.semaphore_signal(barrier, inc=1, device_id=(far, at(o)), device_id_type=MESH)

    for load in loads:
        load.wait()

    peak[...] = jnp.zeros_like(peak)
    norm[...] = jnp.ones_like(norm)

    for j in range(5):
        block = jnp.concatenate(
            [tpl[:, q, 128 * j:128 * (j + 1)].astype(F32) for q in range(2)], 0
        )
        rows[128 * j:128 * (j + 1), :] = block.T
    own = jnp.concatenate([spec[0].astype(F32), spec[1].astype(F32)], 1).astype(BF16)

    def fill(i, carry):
        for q in range(5):
            mine[i, q] = rows[pl.ds(i + 128 * q, 4, stride=32), :].astype(BF16)
        mine[i, 5] = own
        return carry

    lax.fori_loop(0, count, fill, 0)

    got[f] = mine[f]

    pl.semaphore_wait(barrier, count + 1 + peers * late)

    def copy(src, dst, kind, to):
        return pltpu.make_async_remote_copy(
            src_ref=src, dst_ref=dst, send_sem=send_sem.at[kind], recv_sem=recv_sem.at[kind],
            device_id=to, device_id_type=MESH,
        )

    own_chunk = mine.at[f, 5]
    to_far = copy(own_chunk, chunk, 0, (far, f))

    def give(kind, to):
        if kind == GROUP:
            return copy(mine.at[to], got.at[f], 1, (g, to))
        return copy(own_chunk, beside.at[f], 3, (far, to))

    @pl.when(late == 0)
    def _():
        to_far.start()
        for kind, o in far_first((GROUP,)):
            give(kind, at(o)).start()

    @pl.when(late == 1)
    def _():
        for kind, o in far_first((GROUP, FAR)):
            give(kind, at(o)).start()

    all_group = copy(mine.at[pl.ds(0, peers)], got.at[pl.ds(0, peers)], 1, (near, f))
    all_beside = copy(beside, beside, 3, (near, f))
    most_beside = copy(beside.at[pl.ds(0, peers)], beside.at[pl.ds(0, peers)], 3, (near, f))
    all_shared = copy(back.at[pl.ds(0, peers)], back.at[pl.ds(0, peers)], 5, (near, f))
    own_over = copy(got.at[:, 5], other, 2, (near, f))
    far_over = copy(beside, beside2, 4, (near, f))

    def shift(s, carry):
        begin = start[s]
        low, high = lax.rem(begin, SIDE), lax.div(begin, SIDE)
        for q in range(2):
            firsts[s, SIDE * q:SIDE * (q + 1), :] = first[q, pl.ds(low, SIDE), :].astype(BF16)
        w0, w1 = turn[0, pl.ds(low, SIDE), :], turn[1, pl.ds(low, SIDE), :]
        r0, r1 = jump[0, pl.ds(high, 1), :], jump[1, pl.ds(high, 1), :]
        turns[s, 0] = w0 * r0 - w1 * r1
        turns[s, 1] = w0 * r1 + w1 * r0
        return carry

    lax.fori_loop(0, SEGS, shift, 0)

    @pl.when(late == 1)
    def _():
        to_far.wait_recv()
        for _, o in far_first((GROUP,)):
            copy(chunk, beside.at[f], 3, (g, at(o))).start()
        beside[f] = chunk[...]

    all_group.wait_recv()
    own_over.start()

    left = lax.broadcasted_iota(jnp.int32, (ACROSS, 128), 1) < SIDE

    def swapped(x):
        return pltpu.roll(x, SIDE, 1)

    for i in range(ACROSS):
        for q in range(5):
            flat[24 * i + 4 * q:24 * i + 4 * q + 4, :] = got[i, q].astype(F32)
    for p in range(PAIRS):
        one = flat[pl.ds(p, ACROSS, stride=24), :]
        two = flat[pl.ds(p + PAIRS, ACROSS, stride=24), :]
        re = jnp.where(left, one, swapped(two))
        im = jnp.where(left, swapped(one), two)
        bank[p, 0] = re
        bank[p, 1] = im
        total = jnp.sum(re * re + im * im, axis=0, keepdims=True)
        norm[8 * p:8 * (p + 1), :] = jnp.broadcast_to(total, (8, 128))

    def place(source, home):
        for i in range(ACROSS):
            flat[24 * i:24 * i + 4, :] = source(i).astype(F32)
        for q in range(4):
            row = flat[pl.ds(q, ACROSS, stride=24), :]
            turned = swapped(row)
            strain[4 * home + q, 0] = jnp.where(left, row, turned)
            strain[4 * home + q, 1] = jnp.where(left, turned, row)

    table2 = second[...]

    def across(u, home, dst):
        held = [(bank[2 * u + i, 0], bank[2 * u + i, 1]) for i in range(2)]
        for q in range(2):
            for k in range(2):
                s = 4 * home + q + 2 * k
                d0, d1 = strain[s, 0], strain[s, 1]
                crosses = [
                    jnp.concatenate([h0 * d0 + h1 * d1, h0 * d1 - h1 * d0], 0).astype(BF16) for h0, h1 in held
                ]
                y = jnp.dot(firsts[s], jnp.concatenate(crosses, 1), preferred_element_type=F32)
                w0, w1 = turns[s, 0], turns[s, 1]
                for i in range(2):
                    re, im = y[:SIDE, 128 * i:128 * (i + 1)], y[SIDE:, 128 * i:128 * (i + 1)]
                    dst[2 * i + q, :, 256 * k:256 * k + 128] = (re * w0 - im * w1).astype(BF16)
                    dst[2 * i + q, :, 256 * k + 128:256 * k + 256] = (re * w1 + im * w0).astype(BF16)

    def along(u, home, src):
        z = jnp.dot(src[...].reshape(4 * SIDE, 512), table2, preferred_element_type=F32)
        for n in range(4):
            re, im = z[SIDE * n:SIDE * (n + 1), 0:128], z[SIDE * n:SIDE * (n + 1), 128:256]
            row = 16 * u + 8 * (n // 2) + 2 * home + n % 2
            peak[pl.ds(row, 1), :] = jnp.max(re * re + im * im, axis=0, keepdims=True)

    homes = (g, near, far, across_g)
    parts = (lambda i: got[i, 5], lambda i: other[i], lambda i: beside[i], lambda i: beside2[i])

    def arrive(n):
        if n == 1:
            own_over.wait_recv()
        if n == 2:
            @pl.when(late == 0)
            def _():
                all_beside.wait_recv()

            @pl.when(late == 1)
            def _():
                most_beside.wait_recv()

            far_over.start()
        if n == 3:
            far_over.wait_recv()

    steps = [(u, home) for home in range(4) for u in range(PAIRS // 2)]
    mids = (mid, mid2)
    for n, (u, home) in enumerate(steps):
        if u == 0:

            arrive(home)

            place(parts[home], homes[home])

        across(u, homes[home], mids[n % 2])
        if n > 0:
            along(steps[n - 1][0], homes[steps[n - 1][1]], mids[(n - 1) % 2])
    along(steps[-1][0], homes[-1], mids[(len(steps) - 1) % 2])

    best = (peak[...] * jump[0, 40:41, :]).T
    power = norm[...].T
    power = [jnp.sum(power[SIDE * q:SIDE * (q + 1)], axis=0, keepdims=True) for q in range(2)]
    for k in range(4):
        sent[k:k + 1, :] = jnp.max(best[32 * k:32 * (k + 1)], axis=0, keepdims=True) / power[k % 2]
    back[f] = sent[...]

    for _, o in far_first((GROUP,)):
        copy(sent, back.at[f], 5, (g, at(o))).start()
    for whole in (all_group, own_over, far_over):
        whole.wait_send()

    @pl.when(late == 0)
    def _():
        to_far.wait_send()

    @pl.when(late == 1)
    def _():
        all_beside.wait_send()
        most_beside.wait_send()

    all_shared.wait_recv()

    for i in range(count):
        for k in range(4):
            wide[32 * k + i:32 * k + i + 1, :] = back[i, k:k + 1, :]
    turned = wide[...].T
    lane = lax.broadcasted_iota(jnp.int32, (8, 128), 1)
    row = lax.broadcasted_iota(jnp.int32, (8, 128), 0)
    for c in range(5):
        blocks = []
        for k in range(2):
            block = None
            for n in range(4):
                q, p = divmod(4 * c + n, PAIRS)
                piece = turned[8 * p:8 * (p + 1), :]
                shift = (32 * n - 32 * q - 64 * k) % 128
                piece = pltpu.roll(piece, shift, 1) if shift else piece
                block = piece if block is None else jnp.where(lane >= 32 * n, piece, block)
            blocks.append(block)
        one, two = blocks
        for n, shifts in enumerate(((0, 2, 2, 4), (4, 6, 6, 0))):
            moved = [pltpu.roll(x, d, 0) if d else x for x, d in zip((one, two, one, two), shifts)]
            low = jnp.where(row < 2, moved[0], moved[1])
            high = jnp.where(row < 6, moved[2], moved[3])
            out_ref[8 * n:8 * (n + 1), 128 * c:128 * (c + 1)] = jnp.where(row < 4, low, high)

    all_shared.wait_send()


def on_device(spectra, templates, valid_start):
    first, turn, jump, second = tables()
    anywhere = pl.BlockSpec(memory_space=pl.ANY)
    dma = pltpu.SemaphoreType.DMA
    out = pl.pallas_call(
        kernel,
        out_shape=pltpu.VMEM((SEGS, 640), F32),
        in_specs=[anywhere] * 7,
        out_specs=pl.BlockSpec(memory_space=pltpu.VMEM),
        scratch_shapes=[
            pltpu.SMEM((SEGS,), jnp.int32),
            pltpu.VMEM((64, 2, 640), BF16),
            pltpu.VMEM((2, 4, 64), BF16),
            pltpu.VMEM(first.shape, F32),
            pltpu.VMEM(turn.shape, F32),
            pltpu.VMEM(jump.shape, F32),
            pltpu.VMEM(second.shape, BF16),
            pltpu.VMEM((640, 128), F32),
            pltpu.VMEM((32, 6, 4, 128), BF16),
            pltpu.VMEM((32, 6, 4, 128), BF16),
            pltpu.VMEM((32, 4, 128), BF16),
            pltpu.VMEM((4, 128), BF16),
            pltpu.VMEM((32, 4, 128), BF16),
            pltpu.VMEM((32, 4, 128), BF16),
            pltpu.VMEM((32 * 24, 128), F32),
            pltpu.VMEM((PAIRS, 2, ACROSS, 128), F32),
            pltpu.VMEM((SEGS, 2, ACROSS, 128), F32),
            pltpu.VMEM((SEGS, 128, 64), BF16),
            pltpu.VMEM((SEGS, 2, SIDE, 128), F32),
            pltpu.VMEM((4, SIDE, 512), BF16),
            pltpu.VMEM((4, SIDE, 512), BF16),
            pltpu.VMEM((128, 128), F32),
            pltpu.VMEM((128, 128), F32),
            pltpu.VMEM((4, 128), F32),
            pltpu.VMEM((32, 4, 128), F32),
            pltpu.VMEM((128, 128), F32),
            dma((7,)),
            dma((6,)),
            dma((6,)),
        ],
        compiler_params=pltpu.CompilerParams(collective_id=0, has_side_effects=True),
        name="matched_filter",
    )(valid_start, templates, jnp.transpose(spectra, (1, 2, 0)), first, turn, jump, second)
    return out.T


def solution(mesh):
    return jax.shard_map(
        on_device, mesh=mesh, in_specs=(P("freq", None, "group"), P("freq", None, "group"), P()),
        out_specs=P("group", None), check_vma=False,
    )
```

```python
import math

import jax
import jax.numpy as jnp
import numpy as np
from jax import lax
from jax.experimental import pallas as pl
from jax.experimental.pallas import tpu as pltpu
from jax.sharding import PartitionSpec as P

N = 4096
VALID = 2048
SIDE = 64
ACROSS = 32
PAIRS = 10
SEGS = 16
MESH = pl.DeviceIdType.MESH
F32 = jnp.float32
BF16 = jnp.bfloat16


def rounded_roots(index):
    exact = np.exp(2j * np.pi * (index % SIDE) / SIDE)
    least = np.full(index.shape[0], np.inf)
    table = np.zeros_like(exact)
    gain = np.ones(index.shape[0])
    for scale in np.linspace(1.0, 2.0, 2001)[:-1]:
        parts = [(x * scale).astype(jnp.bfloat16).astype(np.float64) for x in (exact.real, exact.imag)]
        tried = parts[0] + 1j * parts[1]
        level = (tried * exact.conj()).mean(1).real
        rest = (np.abs(tried / level[:, None] - exact) ** 2).mean(1)
        better = rest < least - 1e-15
        least = np.where(better, rest, least)
        table = np.where(better[:, None], tried, table)
        gain = np.where(better, level, gain)
    return table, gain


def tables():
    side = np.arange(SIDE)
    root, gain = rounded_roots(side[:, None] * np.arange(ACROSS)[None, :])
    first = np.stack([np.concatenate([root.real, -root.imag], 1), np.concatenate([root.imag, root.real], 1)], 0)
    first = np.tile(first, (1, 2, 1))
    lag = np.arange(2 * SIDE)
    turn = np.exp(2j * np.pi * lag[:, None] * side[None, :] / N) / np.tile(gain, 2)[:, None]
    turn = np.tile(np.stack([turn.real, turn.imag], 0), (1, 1, 2))
    root, gain = rounded_roots(side[:VALID // SIDE, None] * side[None, :])
    c, s = np.kron(np.eye(2), root.real.T), np.kron(np.eye(2), root.imag.T)
    none = np.zeros_like(c)
    second = np.concatenate(
        [
            np.concatenate([c, none, s, none], 1), np.concatenate([-s, none, c, none], 1),
            np.concatenate([none, c, none, s], 1), np.concatenate([none, -s, none, c], 1),
        ], 0,
    )
    jump = np.exp(2j * np.pi * np.arange(40)[:, None] * side[None, :] / SIDE)
    jump = np.tile(np.stack([jump.real, jump.imag], 0), (1, 1, 2))
    weight = np.tile(1.0 / gain ** 2, (2, 8, 4))
    jump = np.concatenate([jump, weight], 1)
    return jnp.asarray(first, F32), jnp.asarray(turn, F32), jnp.asarray(jump, F32), jnp.asarray(second, BF16)


def far_first(kinds):
    def hops(entry):
        (kind, (dz, dx, dy)) = entry
        return min(dz, 4 - dz) + min(dx, 4 - dx) + (2 - dy if kind == FAR else dy)

    offsets = [(dz, dx, dy) for dz in range(4) for dx in range(4) for dy in range(2)]
    entries = [(kind, o) for o in offsets for kind in kinds if (kind, o) != (GROUP, (0, 0, 0))]
    return sorted(entries, key=lambda entry: (-hops(entry), kinds.index(entry[0])))


GROUP, FAR = range(2)


def kernel(
    start_hbm, tpl_hbm, spec_hbm, first_hbm, turn_hbm, jump_hbm, second_hbm, out_ref,
    start, tpl, spec, first, turn, jump, second, rows, mine, got, other, chunk, beside, beside2, flat, loose,
    bank, strain, firsts, turns, mid, mid2, peak, norm, sent, back,
    load_sem, send_sem, recv_sem,
):
    g = lax.axis_index("group")
    f = lax.axis_index("freq")
    far = lax.rem(g + 2, 4)
    near = g + 1 - 2 * lax.rem(g, 2)
    count = 32
    peers = count - 1
    z, x, y = f // 8, lax.rem(f, 8) // 2, lax.rem(f, 2)
    part_z = [8 * lax.rem(z + d, 4) for d in range(4)]
    part_x = [2 * lax.rem(x + d, 4) for d in range(4)]
    part_y = [y, 1 - y]

    def at(offset):
        return part_z[offset[0]] + part_x[offset[1]] + part_y[offset[2]]

    loads = [
        pltpu.make_async_copy(src, dst, load_sem.at[i])
        for i, (src, dst) in enumerate(
            [
                (tpl_hbm, tpl), (spec_hbm, spec), (start_hbm, start),
                (first_hbm, first), (turn_hbm, turn), (jump_hbm, jump), (second_hbm, second),
            ]
        )
    ]
    for load in loads:
        load.start()

    barrier = pltpu.get_barrier_semaphore()
    across_g = lax.rem(near + 2, 4)
    late = g // 2
    group_of = (g, far)
    pl.semaphore_signal(barrier, inc=1, device_id=(far, f), device_id_type=MESH)
    for _, o in far_first((GROUP,)):
        pl.semaphore_signal(barrier, inc=1, device_id=(g, at(o)), device_id_type=MESH)
    pl.semaphore_signal(barrier, inc=1, device_id=(near, f), device_id_type=MESH)

    @pl.when(late == 0)
    def _():
        for _, o in far_first((FAR,)):
            if o != (0, 0, 0):
                pl.semaphore_signal(barrier, inc=1, device_id=(far, at(o)), device_id_type=MESH)

    for load in loads:
        load.wait()

    peak[...] = jnp.zeros_like(peak)
    norm[...] = jnp.ones_like(norm)

    for j in range(5):
        block = jnp.concatenate(
            [tpl[:, q, 128 * j:128 * (j + 1)].astype(F32) for q in range(2)], 0
        )
        rows[128 * j:128 * (j + 1), :] = block.T
    own = jnp.concatenate([spec[0].astype(F32), spec[1].astype(F32)], 1).astype(BF16)

    def fill(i, carry):
        for q in range(5):
            mine[i, q] = rows[pl.ds(i + 128 * q, 4, stride=32), :].astype(BF16)
        mine[i, 5] = own
        return carry

    lax.fori_loop(0, count, fill, 0)

    got[f] = mine[f]

    pl.semaphore_wait(barrier, count + 1 + peers * late)

    def copy(src, dst, kind, to):
        return pltpu.make_async_remote_copy(
            src_ref=src, dst_ref=dst, send_sem=send_sem.at[kind], recv_sem=recv_sem.at[kind],
            device_id=to, device_id_type=MESH,
        )

    own_chunk = mine.at[f, 5]
    to_far = copy(own_chunk, chunk, 0, (far, f))

    def give(kind, to):
        if kind == GROUP:
            return copy(mine.at[to], got.at[f], 1, (g, to))
        return copy(own_chunk, beside.at[f], 3, (far, to))

    @pl.when(late == 0)
    def _():
        to_far.start()
        for kind, o in far_first((GROUP,)):
            give(kind, at(o)).start()

    @pl.when(late == 1)
    def _():
        for kind, o in far_first((GROUP, FAR)):
            give(kind, at(o)).start()

    all_group = copy(mine.at[pl.ds(0, peers)], got.at[pl.ds(0, peers)], 1, (near, f))
    all_beside = copy(beside, beside, 3, (near, f))
    most_beside = copy(beside.at[pl.ds(0, peers)], beside.at[pl.ds(0, peers)], 3, (near, f))
    all_shared = copy(back.at[pl.ds(0, peers)], back.at[pl.ds(0, peers)], 5, (near, f))
    own_over = copy(got.at[:, 5], other, 2, (near, f))
    far_over = copy(beside, beside2, 4, (near, f))

    def shift(s, carry):
        begin = start[s]
        low, high = lax.rem(begin, SIDE), lax.div(begin, SIDE)
        for q in range(2):
            firsts[s, SIDE * q:SIDE * (q + 1), :] = first[q, pl.ds(low, SIDE), :].astype(BF16)
        w0, w1 = turn[0, pl.ds(low, SIDE), :], turn[1, pl.ds(low, SIDE), :]
        r0, r1 = jump[0, pl.ds(high, 1), :], jump[1, pl.ds(high, 1), :]
        turns[s, 0] = w0 * r0 - w1 * r1
        turns[s, 1] = w0 * r1 + w1 * r0
        return carry

    lax.fori_loop(0, SEGS, shift, 0)

    @pl.when(late == 1)
    def _():
        to_far.wait_recv()
        for _, o in far_first((GROUP,)):
            copy(chunk, beside.at[f], 3, (g, at(o))).start()
        beside[f] = chunk[...]

    all_group.wait_recv()
    own_over.start()

    left = lax.broadcasted_iota(jnp.int32, (ACROSS, 128), 1) < SIDE

    def swapped(x):
        return pltpu.roll(x, SIDE, 1)

    for i in range(ACROSS):
        for q in range(5):
            flat[24 * i + 4 * q:24 * i + 4 * q + 4, :] = got[i, q].astype(F32)
    for p in range(PAIRS):
        one = flat[pl.ds(p, ACROSS, stride=24), :]
        two = flat[pl.ds(p + PAIRS, ACROSS, stride=24), :]
        re = jnp.where(left, one, swapped(two))
        im = jnp.where(left, swapped(one), two)
        bank[p, 0] = re
        bank[p, 1] = im
        total = jnp.sum(re * re + im * im, axis=0, keepdims=True)
        norm[8 * p:8 * (p + 1), :] = jnp.broadcast_to(total, (8, 128))

    def place(source, home):
        for i in range(ACROSS):
            loose[4 * i:4 * i + 4, :] = source(i).astype(F32)
        for q in range(4):
            row = loose[pl.ds(q, ACROSS, stride=4), :]
            turned = swapped(row)
            strain[4 * home + q, 0] = jnp.where(left, row, turned)
            strain[4 * home + q, 1] = jnp.where(left, turned, row)

    table2 = second[...]

    def across(u, home, dst):
        held = [(bank[2 * u + i, 0], bank[2 * u + i, 1]) for i in range(2)]
        for q in range(2):
            for k in range(2):
                s = 4 * home + q + 2 * k
                d0, d1 = strain[s, 0], strain[s, 1]
                crosses = [
                    jnp.concatenate([h0 * d0 + h1 * d1, h0 * d1 - h1 * d0], 0).astype(BF16) for h0, h1 in held
                ]
                y = jnp.dot(firsts[s], jnp.concatenate(crosses, 1), preferred_element_type=F32)
                w0, w1 = turns[s, 0], turns[s, 1]
                for i in range(2):
                    re, im = y[:SIDE, 128 * i:128 * (i + 1)], y[SIDE:, 128 * i:128 * (i + 1)]
                    dst[2 * i + q, :, 256 * k:256 * k + 128] = (re * w0 - im * w1).astype(BF16)
                    dst[2 * i + q, :, 256 * k + 128:256 * k + 256] = (re * w1 + im * w0).astype(BF16)

    def along(u, home, src):
        z = jnp.dot(src[...].reshape(4 * SIDE, 512), table2, preferred_element_type=F32)
        for n in range(4):
            re, im = z[SIDE * n:SIDE * (n + 1), 0:128], z[SIDE * n:SIDE * (n + 1), 128:256]
            row = 16 * u + 8 * (n // 2) + 2 * home + n % 2
            peak[pl.ds(row, 1), :] = jnp.max(re * re + im * im, axis=0, keepdims=True)

    homes = (g, near, far, across_g)
    parts = (lambda i: got[i, 5], lambda i: other[i], lambda i: beside[i], lambda i: beside2[i])

    def arrive(n):
        if n == 1:
            own_over.wait_recv()
        if n == 2:
            @pl.when(late == 0)
            def _():
                all_beside.wait_recv()

            @pl.when(late == 1)
            def _():
                most_beside.wait_recv()

            far_over.start()
        if n == 3:
            far_over.wait_recv()

    steps = [(u, home) for home in range(4) for u in range(PAIRS // 2)]
    mids = (mid, mid2)
    for n, (u, home) in enumerate(steps):
        if u == 0:

            arrive(home)

            place(parts[home], homes[home])

        across(u, homes[home], mids[n % 2])
        if n > 0:
            along(steps[n - 1][0], homes[steps[n - 1][1]], mids[(n - 1) % 2])
    along(steps[-1][0], homes[-1], mids[(len(steps) - 1) % 2])

    best = (peak[...] * jump[0, 40:41, :]).T
    power = norm[...].T
    power = [jnp.sum(power[SIDE * q:SIDE * (q + 1)], axis=0, keepdims=True) for q in range(2)]
    result = [jnp.max(best[32 * k:32 * (k + 1)], axis=0, keepdims=True) / power[k % 2] for k in range(4)]
    used = lax.broadcasted_iota(jnp.int32, (1, 128), 1) < 80
    sent[0:1, :] = jnp.where(used, result[0], pltpu.roll(result[3], 80, 1))
    sent[1:2, :] = jnp.where(used, result[1], pltpu.roll(result[3], 32, 1))
    sent[2:3, :] = result[2]
    back[f] = sent[...]

    for _, o in far_first((GROUP,)):
        copy(sent, back.at[f], 5, (g, at(o))).start()
    for whole in (all_group, own_over, far_over):
        whole.wait_send()

    @pl.when(late == 0)
    def _():
        to_far.wait_send()

    @pl.when(late == 1)
    def _():
        all_beside.wait_send()
        most_beside.wait_send()

    all_shared.wait_recv()

    parted = [back[:, k, :] for k in range(3)]
    lead = lax.broadcasted_iota(jnp.int32, (ACROSS, 128), 1) < 48
    parted.append(jnp.where(lead, pltpu.roll(parted[0], 48, 1), pltpu.roll(parted[1], 96, 1)))
    turned = jnp.concatenate(parted, 0).T
    lane = lax.broadcasted_iota(jnp.int32, (8, 128), 1)
    row = lax.broadcasted_iota(jnp.int32, (8, 128), 0)
    for c in range(5):
        blocks = []
        for k in range(2):
            block = None
            for n in range(4):
                q, p = divmod(4 * c + n, PAIRS)
                piece = turned[8 * p:8 * (p + 1), :]
                shift = (32 * n - 32 * q - 64 * k) % 128
                piece = pltpu.roll(piece, shift, 1) if shift else piece
                block = piece if block is None else jnp.where(lane >= 32 * n, piece, block)
            blocks.append(block)
        one, two = blocks
        for n, shifts in enumerate(((0, 2, 2, 4), (4, 6, 6, 0))):
            moved = [pltpu.roll(x, d, 0) if d else x for x, d in zip((one, two, one, two), shifts)]
            low = jnp.where(row < 2, moved[0], moved[1])
            high = jnp.where(row < 6, moved[2], moved[3])
            out_ref[8 * n:8 * (n + 1), 128 * c:128 * (c + 1)] = jnp.where(row < 4, low, high)

    all_shared.wait_send()


def on_device(spectra, templates, valid_start):
    first, turn, jump, second = tables()
    anywhere = pl.BlockSpec(memory_space=pl.ANY)
    dma = pltpu.SemaphoreType.DMA
    out = pl.pallas_call(
        kernel,
        out_shape=pltpu.VMEM((SEGS, 640), F32),
        in_specs=[anywhere] * 7,
        out_specs=pl.BlockSpec(memory_space=pltpu.VMEM),
        scratch_shapes=[
            pltpu.SMEM((SEGS,), jnp.int32),
            pltpu.VMEM((64, 2, 640), BF16),
            pltpu.VMEM((2, 4, 64), BF16),
            pltpu.VMEM(first.shape, F32),
            pltpu.VMEM(turn.shape, F32),
            pltpu.VMEM(jump.shape, F32),
            pltpu.VMEM(second.shape, BF16),
            pltpu.VMEM((640, 128), F32),
            pltpu.VMEM((32, 6, 4, 128), BF16),
            pltpu.VMEM((32, 6, 4, 128), BF16),
            pltpu.VMEM((32, 4, 128), BF16),
            pltpu.VMEM((4, 128), BF16),
            pltpu.VMEM((32, 4, 128), BF16),
            pltpu.VMEM((32, 4, 128), BF16),
            pltpu.VMEM((32 * 24, 128), F32),
            pltpu.VMEM((32 * 4, 128), F32),
            pltpu.VMEM((PAIRS, 2, ACROSS, 128), F32),
            pltpu.VMEM((SEGS, 2, ACROSS, 128), F32),
            pltpu.VMEM((SEGS, 128, 64), BF16),
            pltpu.VMEM((SEGS, 2, SIDE, 128), F32),
            pltpu.VMEM((4, SIDE, 512), BF16),
            pltpu.VMEM((4, SIDE, 512), BF16),
            pltpu.VMEM((128, 128), F32),
            pltpu.VMEM((128, 128), F32),
            pltpu.VMEM((3, 128), F32),
            pltpu.VMEM((32, 3, 128), F32),
            dma((7,)),
            dma((6,)),
            dma((6,)),
        ],
        compiler_params=pltpu.CompilerParams(collective_id=0, has_side_effects=True),
        name="matched_filter",
    )(valid_start, templates, jnp.transpose(spectra, (1, 2, 0)), first, turn, jump, second)
    return out.T


def solution(mesh):
    return jax.shard_map(
        on_device, mesh=mesh, in_specs=(P("freq", None, "group"), P("freq", None, "group"), P()),
        out_specs=P("group", None), check_vma=False,
    )
```

```python
import math

import jax
import jax.numpy as jnp
import numpy as np
from jax import lax
from jax.experimental import pallas as pl
from jax.experimental.pallas import tpu as pltpu
from jax.sharding import PartitionSpec as P

N = 4096
VALID = 2048
SIDE = 64
ACROSS = 32
PAIRS = 10
SEGS = 16
MESH = pl.DeviceIdType.MESH
F32 = jnp.float32
BF16 = jnp.bfloat16


def rounded_roots(index):
    exact = np.exp(2j * np.pi * (index % SIDE) / SIDE)
    least = np.full(index.shape[0], np.inf)
    table = np.zeros_like(exact)
    gain = np.ones(index.shape[0])
    for scale in np.linspace(1.0, 2.0, 2001)[:-1]:
        parts = [(x * scale).astype(jnp.bfloat16).astype(np.float64) for x in (exact.real, exact.imag)]
        tried = parts[0] + 1j * parts[1]
        level = (tried * exact.conj()).mean(1).real
        rest = (np.abs(tried / level[:, None] - exact) ** 2).mean(1)
        better = rest < least - 1e-15
        least = np.where(better, rest, least)
        table = np.where(better[:, None], tried, table)
        gain = np.where(better, level, gain)
    return table, gain


def tables():
    side = np.arange(SIDE)
    root, gain = rounded_roots(side[:, None] * np.arange(ACROSS)[None, :])
    first = np.stack([np.concatenate([root.real, -root.imag], 1), np.concatenate([root.imag, root.real], 1)], 0)
    first = np.tile(first, (1, 2, 1))
    lag = np.arange(2 * SIDE)
    turn = np.exp(2j * np.pi * lag[:, None] * side[None, :] / N) / np.tile(gain, 2)[:, None]
    turn = np.tile(np.stack([turn.real, turn.imag], 0), (1, 1, 2))
    root, gain = rounded_roots(side[:VALID // SIDE, None] * side[None, :])
    c, s = np.kron(np.eye(2), root.real.T), np.kron(np.eye(2), root.imag.T)
    none = np.zeros_like(c)
    second = np.concatenate(
        [
            np.concatenate([c, none, s, none], 1), np.concatenate([-s, none, c, none], 1),
            np.concatenate([none, c, none, s], 1), np.concatenate([none, -s, none, c], 1),
        ], 0,
    )
    jump = np.exp(2j * np.pi * np.arange(40)[:, None] * side[None, :] / SIDE)
    jump = np.tile(np.stack([jump.real, jump.imag], 0), (1, 1, 2))
    weight = np.tile(1.0 / gain ** 2, (2, 8, 4))
    jump = np.concatenate([jump, weight], 1)
    return jnp.asarray(first, F32), jnp.asarray(turn, F32), jnp.asarray(jump, F32), jnp.asarray(second, BF16)


def far_first(kinds):
    def hops(entry):
        (kind, (dz, dx, dy)) = entry
        return min(dz, 4 - dz) + min(dx, 4 - dx) + (2 - dy if kind == FAR else dy)

    offsets = [(dz, dx, dy) for dz in range(4) for dx in range(4) for dy in range(2)]
    entries = [(kind, o) for o in offsets for kind in kinds if (kind, o) != (GROUP, (0, 0, 0))]
    return sorted(entries, key=lambda entry: (-hops(entry), kinds.index(entry[0])))


GROUP, FAR = range(2)


def kernel(
    start_hbm, tpl_hbm, spec_hbm, first_hbm, turn_hbm, jump_hbm, second_hbm, out_ref,
    start, tpl, spec, first, turn, jump, second, rows, mine, got, chunk, wings, flat, loose,
    bank, strain, firsts, turns, mid, mid2, peak, norm, total, sent, back, wide,
    load_sem, send_sem, recv_sem,
):
    g = lax.axis_index("group")
    f = lax.axis_index("freq")
    far = lax.rem(g + 2, 4)
    near = g + 1 - 2 * lax.rem(g, 2)
    count = 32
    peers = count - 1
    z, x, y = f // 8, lax.rem(f, 8) // 2, lax.rem(f, 2)
    part_z = [8 * lax.rem(z + d, 4) for d in range(4)]
    part_x = [2 * lax.rem(x + d, 4) for d in range(4)]
    part_y = [y, 1 - y]

    def at(offset):
        return part_z[offset[0]] + part_x[offset[1]] + part_y[offset[2]]

    loads = [
        pltpu.make_async_copy(src, dst, load_sem.at[i])
        for i, (src, dst) in enumerate(
            [
                (tpl_hbm, tpl), (spec_hbm, spec), (start_hbm, start),
                (first_hbm, first), (turn_hbm, turn), (jump_hbm, jump), (second_hbm, second),
            ]
        )
    ]
    for load in loads:
        load.start()

    barrier = pltpu.get_barrier_semaphore()
    across_g = lax.rem(near + 2, 4)
    late = g // 2
    core = lax.rem(g, 2)
    swap = core * (1 - late)
    other, beside, beside2 = (wings.at[k] for k in range(3))
    group_of = (g, far)
    pl.semaphore_signal(barrier, inc=1, device_id=(far, f), device_id_type=MESH)
    for _, o in far_first((GROUP,)):
        pl.semaphore_signal(barrier, inc=1, device_id=(g, at(o)), device_id_type=MESH)
    pl.semaphore_signal(barrier, inc=1, device_id=(near, f), device_id_type=MESH)

    @pl.when(late == 0)
    def _():
        for _, o in far_first((FAR,)):
            if o != (0, 0, 0):
                pl.semaphore_signal(barrier, inc=1, device_id=(far, at(o)), device_id_type=MESH)

    for load in loads:
        load.wait()

    peak[...] = jnp.zeros_like(peak)
    norm[...] = jnp.ones_like(norm)

    for j in range(5):
        block = jnp.concatenate(
            [tpl[:, q, 128 * j:128 * (j + 1)].astype(F32) for q in range(2)], 0
        )
        rows[128 * j:128 * (j + 1), :] = block.T
    own = jnp.concatenate([spec[0].astype(F32), spec[1].astype(F32)], 1).astype(BF16)

    def fill(i, carry):
        for q in range(5):
            mine[i, q] = rows[pl.ds(i + 128 * q, 4, stride=32), :].astype(BF16)
        mine[i, 5] = own
        return carry

    lax.fori_loop(0, count, fill, 0)

    got[f] = mine[f]

    pl.semaphore_wait(barrier, count + 1 + peers * late)

    def copy(src, dst, kind, to):
        return pltpu.make_async_remote_copy(
            src_ref=src, dst_ref=dst, send_sem=send_sem.at[kind], recv_sem=recv_sem.at[kind],
            device_id=to, device_id_type=MESH,
        )

    own_chunk = mine.at[f, 5]
    to_far = copy(own_chunk, chunk, 0, (far, f))

    def give(kind, to):
        if kind == GROUP:
            return copy(mine.at[to], got.at[f], 1, (g, to))
        return copy(own_chunk, beside.at[f], 3, (far, to))

    @pl.when(late == 0)
    def _():
        to_far.start()
        for kind, o in far_first((GROUP,)):
            give(kind, at(o)).start()

    @pl.when(late == 1)
    def _():
        for kind, o in far_first((GROUP, FAR)):
            give(kind, at(o)).start()

    all_group = copy(mine.at[pl.ds(0, peers)], got.at[pl.ds(0, peers)], 1, (near, f))
    all_beside = copy(beside, beside, 3, (near, f))
    most_beside = copy(beside.at[pl.ds(0, peers)], beside.at[pl.ds(0, peers)], 3, (near, f))
    all_shared = copy(back.at[pl.ds(0, peers)], back.at[pl.ds(0, peers)], 5, (near, f))
    own_over = copy(got.at[:, 5], other, 2, (near, f))
    far_over = copy(beside, beside2, 4, (near, f))

    def shift(s, carry):
        begin = start[s]
        low, high = lax.rem(begin, SIDE), lax.div(begin, SIDE)
        for q in range(2):
            firsts[s, SIDE * q:SIDE * (q + 1), :] = first[q, pl.ds(low, SIDE), :].astype(BF16)
        w0, w1 = turn[0, pl.ds(low, SIDE), :], turn[1, pl.ds(low, SIDE), :]
        r0, r1 = jump[0, pl.ds(high, 1), :], jump[1, pl.ds(high, 1), :]
        turns[s, 0] = w0 * r0 - w1 * r1
        turns[s, 1] = w0 * r1 + w1 * r0
        return carry

    lax.fori_loop(0, SEGS, shift, 0)

    @pl.when(late == 1)
    def _():
        to_far.wait_recv()
        for _, o in far_first((GROUP,)):
            copy(chunk, beside.at[f], 3, (g, at(o))).start()
        wings[1, f] = chunk[...]

    all_group.wait_recv()
    own_over.start()

    left = lax.broadcasted_iota(jnp.int32, (ACROSS, 128), 1) < SIDE

    def swapped(x):
        return pltpu.roll(x, SIDE, 1)

    def prepare(u, unpacked):
        for p in (2 * u, 2 * u + 1):
            for q in sorted({p // 4, (p + PAIRS) // 4} - unpacked):
                unpacked.add(q)
                for i in range(ACROSS):
                    flat[24 * i + 4 * q:24 * i + 4 * q + 4, :] = got[i, q].astype(F32)
            one = flat[pl.ds(p, ACROSS, stride=24), :]
            two = flat[pl.ds(p + PAIRS, ACROSS, stride=24), :]
            re = jnp.where(left, one, swapped(two))
            im = jnp.where(left, swapped(one), two)
            bank[p, 0] = re
            bank[p, 1] = im
            level = jnp.sum(re * re + im * im, axis=0, keepdims=True)
            norm[8 * p:8 * (p + 1), :] = jnp.broadcast_to(level, (8, 128))

    def place(source, home):
        for i in range(ACROSS):
            loose[4 * i:4 * i + 4, :] = source(i).astype(F32)
        for q in range(4):
            row = loose[pl.ds(q, ACROSS, stride=4), :]
            turned = swapped(row)
            strain[4 * home + q, 0] = jnp.where(left, row, turned)
            strain[4 * home + q, 1] = jnp.where(left, turned, row)

    table2 = second[...]

    def across(u, home, dst):
        held = [(bank[2 * u + i, 0], bank[2 * u + i, 1]) for i in range(2)]
        for q in range(2):
            for k in range(2):
                s = 4 * home + q + 2 * k
                d0, d1 = strain[s, 0], strain[s, 1]
                crosses = [
                    jnp.concatenate([h0 * d0 + h1 * d1, h0 * d1 - h1 * d0], 0).astype(BF16) for h0, h1 in held
                ]
                y = jnp.dot(firsts[s], jnp.concatenate(crosses, 1), preferred_element_type=F32)
                w0, w1 = turns[s, 0], turns[s, 1]
                for i in range(2):
                    re, im = y[:SIDE, 128 * i:128 * (i + 1)], y[SIDE:, 128 * i:128 * (i + 1)]
                    dst[2 * i + q, :, 256 * k:256 * k + 128] = (re * w0 - im * w1).astype(BF16)
                    dst[2 * i + q, :, 256 * k + 128:256 * k + 256] = (re * w1 + im * w0).astype(BF16)

    def along(u, home, src):
        z = jnp.dot(src[...].reshape(4 * SIDE, 512), table2, preferred_element_type=F32)
        for n in range(4):
            re, im = z[SIDE * n:SIDE * (n + 1), 0:128], z[SIDE * n:SIDE * (n + 1), 128:256]
            row = 16 * u + 8 * (n // 2) + 2 * home + n % 2
            peak[pl.ds(row, 1), :] = jnp.max(re * re + im * im, axis=0, keepdims=True)

    def far_arrived():
        @pl.when(late == 0)
        def _():
            all_beside.wait_recv()

        @pl.when(late == 1)
        def _():
            most_beside.wait_recv()

        far_over.start()

    def run(order, arrive):
        unpacked = set()
        steps = [(u, n) for n in range(4) for u in range(PAIRS // 2)]
        mids = (mid, mid2)
        for step, (u, n) in enumerate(steps):
            home, part = order[n]
            if u == 0:
                arrive(n)
                place(part, home)
            if n == 0:
                prepare(u, unpacked)
            across(u, home, mids[step % 2])
            if step > 0:
                along(steps[step - 1][0], order[steps[step - 1][1]][0], mids[(step - 1) % 2])
            if step == 12:
                power = norm[...].T
                for k in range(2):
                    total[k:k + 1, :] = jnp.sum(power[SIDE * k:SIDE * (k + 1)], axis=0, keepdims=True)
        along(PAIRS // 2 - 1, order[3][0], mids[(len(steps) - 1) % 2])

    @pl.when(core == 0)
    def _():
        def arrive(n):
            if n == 0:
                own_over.wait_recv()
            if n == 2:
                far_arrived()
            if n == 3:
                far_over.wait_recv()

        run(
            (
                (g, lambda i: got[i, 5]), (near, lambda i: wings[0, i]),
                (far, lambda i: wings[1, i]), (across_g, lambda i: wings[2, i]),
            ), arrive,
        )

    @pl.when(core == 1)
    def _():
        def arrive(n):
            if n == 1:
                @pl.when(late == 1)
                def _():
                    own_over.wait_recv()

                @pl.when(late == 0)
                def _():
                    all_beside.wait_recv()
                    far_over.start()

            if n == 2:
                @pl.when(late == 1)
                def _():
                    most_beside.wait_recv()
                    far_over.start()

                @pl.when(late == 0)
                def _():
                    own_over.wait_recv()

            if n == 3:
                far_over.wait_recv()

        run(
            (
                (g, lambda i: got[i, 5]), (near + swap * (far - near), lambda i: wings[swap, i]),
                (far + swap * (near - far), lambda i: wings[1 - swap, i]), (across_g, lambda i: wings[2, i]),
            ), arrive,
        )

    best = (peak[...] * jump[0, 40:41, :]).T
    for k in range(4):
        sent[k:k + 1, :] = jnp.max(best[32 * k:32 * (k + 1)], axis=0, keepdims=True) / total[k % 2:k % 2 + 1, :]
    back[f] = sent[...]

    for _, o in far_first((GROUP,)):
        copy(sent, back.at[f], 5, (g, at(o))).start()
    for whole in (all_group, own_over, far_over):
        whole.wait_send()

    @pl.when(late == 0)
    def _():
        to_far.wait_send()

    @pl.when(late == 1)
    def _():
        all_beside.wait_send()
        most_beside.wait_send()

    all_shared.wait_recv()

    for i in range(count):
        for k in range(4):
            wide[32 * k + i:32 * k + i + 1, :] = back[i, k:k + 1, :]
    turned = wide[...].T
    lane = lax.broadcasted_iota(jnp.int32, (8, 128), 1)
    row = lax.broadcasted_iota(jnp.int32, (8, 128), 0)
    for c in range(5):
        blocks = []
        for k in range(2):
            block = None
            for n in range(4):
                q, p = divmod(4 * c + n, PAIRS)
                piece = turned[8 * p:8 * (p + 1), :]
                shift = (32 * n - 32 * q - 64 * k) % 128
                piece = pltpu.roll(piece, shift, 1) if shift else piece
                block = piece if block is None else jnp.where(lane >= 32 * n, piece, block)
            blocks.append(block)
        one, two = blocks
        for n, shifts in enumerate(((0, 2, 2, 4), (4, 6, 6, 0))):
            moved = [pltpu.roll(x, d, 0) if d else x for x, d in zip((one, two, one, two), shifts)]
            low = jnp.where(row < 2, moved[0], moved[1])
            high = jnp.where(row < 6, moved[2], moved[3])
            out_ref[8 * n:8 * (n + 1), 128 * c:128 * (c + 1)] = jnp.where(row < 4, low, high)

    all_shared.wait_send()


def on_device(spectra, templates, valid_start):
    first, turn, jump, second = tables()
    anywhere = pl.BlockSpec(memory_space=pl.ANY)
    dma = pltpu.SemaphoreType.DMA
    out = pl.pallas_call(
        kernel,
        out_shape=pltpu.VMEM((SEGS, 640), F32),
        in_specs=[anywhere] * 7,
        out_specs=pl.BlockSpec(memory_space=pltpu.VMEM),
        scratch_shapes=[
            pltpu.SMEM((SEGS,), jnp.int32),
            pltpu.VMEM((64, 2, 640), BF16),
            pltpu.VMEM((2, 4, 64), BF16),
            pltpu.VMEM(first.shape, F32),
            pltpu.VMEM(turn.shape, F32),
            pltpu.VMEM(jump.shape, F32),
            pltpu.VMEM(second.shape, BF16),
            pltpu.VMEM((640, 128), F32),
            pltpu.VMEM((32, 6, 4, 128), BF16),
            pltpu.VMEM((32, 6, 4, 128), BF16),
            pltpu.VMEM((4, 128), BF16),
            pltpu.VMEM((3, 32, 4, 128), BF16),
            pltpu.VMEM((32 * 24, 128), F32),
            pltpu.VMEM((32 * 4, 128), F32),
            pltpu.VMEM((PAIRS, 2, ACROSS, 128), F32),
            pltpu.VMEM((SEGS, 2, ACROSS, 128), F32),
            pltpu.VMEM((SEGS, 128, 64), BF16),
            pltpu.VMEM((SEGS, 2, SIDE, 128), F32),
            pltpu.VMEM((4, SIDE, 512), BF16),
            pltpu.VMEM((4, SIDE, 512), BF16),
            pltpu.VMEM((128, 128), F32),
            pltpu.VMEM((128, 128), F32),
            pltpu.VMEM((2, 128), F32),
            pltpu.VMEM((4, 128), F32),
            pltpu.VMEM((32, 4, 128), F32),
            pltpu.VMEM((128, 128), F32),
            dma((7,)),
            dma((6,)),
            dma((6,)),
        ],
        compiler_params=pltpu.CompilerParams(collective_id=0, has_side_effects=True),
        name="matched_filter",
    )(valid_start, templates, jnp.transpose(spectra, (1, 2, 0)), first, turn, jump, second)
    return out.T


def solution(mesh):
    return jax.shard_map(
        on_device, mesh=mesh, in_specs=(P("freq", None, "group"), P("freq", None, "group"), P()),
        out_specs=P("group", None), check_vma=False,
    )
```

```python
import math

import jax
import jax.numpy as jnp
import numpy as np
from jax import lax
from jax.experimental import pallas as pl
from jax.experimental.pallas import tpu as pltpu
from jax.sharding import PartitionSpec as P

N = 4096
VALID = 2048
SIDE = 64
ACROSS = 32
PAIRS = 10
SEGS = 16
MESH = pl.DeviceIdType.MESH
F32 = jnp.float32
BF16 = jnp.bfloat16


def rounded_roots(index):
    exact = np.exp(2j * np.pi * (index % SIDE) / SIDE)
    least = np.full(index.shape[0], np.inf)
    table = np.zeros_like(exact)
    gain = np.ones(index.shape[0])
    for scale in np.linspace(1.0, 2.0, 2001)[:-1]:
        parts = [(x * scale).astype(jnp.bfloat16).astype(np.float64) for x in (exact.real, exact.imag)]
        tried = parts[0] + 1j * parts[1]
        level = (tried * exact.conj()).mean(1).real
        rest = (np.abs(tried / level[:, None] - exact) ** 2).mean(1)
        better = rest < least - 1e-15
        least = np.where(better, rest, least)
        table = np.where(better[:, None], tried, table)
        gain = np.where(better, level, gain)
    return table, gain


def tables():
    side = np.arange(SIDE)
    root, gain = rounded_roots(side[:, None] * np.arange(ACROSS)[None, :])
    first = np.stack([np.concatenate([root.real, -root.imag], 1), np.concatenate([root.imag, root.real], 1)], 0)
    first = np.tile(first, (1, 2, 1))
    lag = np.arange(2 * SIDE)
    turn = np.exp(2j * np.pi * lag[:, None] * side[None, :] / N) / np.tile(gain, 2)[:, None]
    turn = np.tile(np.stack([turn.real, turn.imag], 0), (1, 1, 2))
    root, gain = rounded_roots(side[:VALID // SIDE, None] * side[None, :])
    c, s = np.kron(np.eye(2), root.real.T), np.kron(np.eye(2), root.imag.T)
    none = np.zeros_like(c)
    second = np.concatenate(
        [
            np.concatenate([c, none, s, none], 1), np.concatenate([-s, none, c, none], 1),
            np.concatenate([none, c, none, s], 1), np.concatenate([none, -s, none, c], 1),
        ], 0,
    )
    jump = np.exp(2j * np.pi * np.arange(40)[:, None] * side[None, :] / SIDE)
    jump = np.tile(np.stack([jump.real, jump.imag], 0), (1, 1, 2))
    weight = np.tile(1.0 / gain ** 2, (2, 8, 4))
    jump = np.concatenate([jump, weight], 1)
    return jnp.asarray(first, F32), jnp.asarray(turn, F32), jnp.asarray(jump, F32), jnp.asarray(second, BF16)


def far_first(kinds):
    def hops(entry):
        (kind, (dz, dx, dy)) = entry
        return min(dz, 4 - dz) + min(dx, 4 - dx) + (2 - dy if kind == FAR else dy)

    offsets = [(dz, dx, dy) for dz in range(4) for dx in range(4) for dy in range(2)]
    entries = [(kind, o) for o in offsets for kind in kinds if (kind, o) != (GROUP, (0, 0, 0))]
    def order(entry):
        (kind, (dz, dx, _)) = entry
        return -hops(entry) - 0.6 * (dz == 3) - 0.6 * (dx == 3), kinds.index(kind)

    return sorted(entries, key=order)


GROUP, FAR = range(2)


def kernel(
    start_hbm, tpl_hbm, spec_hbm, first_hbm, turn_hbm, jump_hbm, second_hbm, out_ref,
    start, tpl, spec, first, turn, jump, second, rows, mine, got, chunk, wings, flat, loose,
    bank, strain, firsts, turns, mid, mid2, peak, norm, total, sent, back, wide,
    load_sem, send_sem, recv_sem,
):
    g = lax.axis_index("group")
    f = lax.axis_index("freq")
    far = lax.rem(g + 2, 4)
    near = g + 1 - 2 * lax.rem(g, 2)
    count = 32
    peers = count - 1
    z, x, y = f // 8, lax.rem(f, 8) // 2, lax.rem(f, 2)
    part_z = [8 * lax.rem(z + d, 4) for d in range(4)]
    part_x = [2 * lax.rem(x + d, 4) for d in range(4)]
    part_y = [y, 1 - y]

    def at(offset):
        return part_z[offset[0]] + part_x[offset[1]] + part_y[offset[2]]

    loads = [
        pltpu.make_async_copy(src, dst, load_sem.at[i])
        for i, (src, dst) in enumerate(
            [
                (tpl_hbm, tpl), (spec_hbm, spec), (start_hbm, start),
                (first_hbm, first), (turn_hbm, turn), (jump_hbm, jump), (second_hbm, second),
            ]
        )
    ]
    for load in loads:
        load.start()

    barrier = pltpu.get_barrier_semaphore()
    across_g = lax.rem(near + 2, 4)
    late = g // 2
    core = lax.rem(g, 2)
    swap = core * (1 - late)
    other, beside, beside2 = (wings.at[k] for k in range(3))
    group_of = (g, far)
    pl.semaphore_signal(barrier, inc=1, device_id=(far, f), device_id_type=MESH)
    for _, o in far_first((GROUP,)):
        pl.semaphore_signal(barrier, inc=1, device_id=(g, at(o)), device_id_type=MESH)
    pl.semaphore_signal(barrier, inc=1, device_id=(near, f), device_id_type=MESH)

    @pl.when(late == 0)
    def _():
        for _, o in far_first((FAR,)):
            if o != (0, 0, 0):
                pl.semaphore_signal(barrier, inc=1, device_id=(far, at(o)), device_id_type=MESH)

    for load in loads:
        load.wait()

    peak[...] = jnp.zeros_like(peak)
    norm[...] = jnp.ones_like(norm)

    for j in range(5):
        block = jnp.concatenate(
            [tpl[:, q, 128 * j:128 * (j + 1)].astype(F32) for q in range(2)], 0
        )
        rows[128 * j:128 * (j + 1), :] = block.T
    own = jnp.concatenate([spec[0].astype(F32), spec[1].astype(F32)], 1).astype(BF16)

    def fill(i, carry):
        for q in range(5):
            mine[i, q] = rows[pl.ds(i + 128 * q, 4, stride=32), :].astype(BF16)
        mine[i, 5] = own
        return carry

    lax.fori_loop(0, count, fill, 0)

    got[f] = mine[f]

    pl.semaphore_wait(barrier, count + 1 + peers * late)

    def copy(src, dst, kind, to):
        return pltpu.make_async_remote_copy(
            src_ref=src, dst_ref=dst, send_sem=send_sem.at[kind], recv_sem=recv_sem.at[kind],
            device_id=to, device_id_type=MESH,
        )

    own_chunk = mine.at[f, 5]
    to_far = copy(own_chunk, chunk, 0, (far, f))

    def give(kind, to):
        if kind == GROUP:
            return copy(mine.at[to], got.at[f], 1, (g, to))
        return copy(own_chunk, beside.at[f], 3, (far, to))

    @pl.when(late == 0)
    def _():
        to_far.start()
        for kind, o in far_first((GROUP,)):
            give(kind, at(o)).start()

    @pl.when(late == 1)
    def _():
        for kind, o in far_first((GROUP, FAR)):
            give(kind, at(o)).start()

    all_group = copy(mine.at[pl.ds(0, peers)], got.at[pl.ds(0, peers)], 1, (near, f))
    all_beside = copy(beside, beside, 3, (near, f))
    most_beside = copy(beside.at[pl.ds(0, peers)], beside.at[pl.ds(0, peers)], 3, (near, f))
    all_shared = copy(back.at[pl.ds(0, peers)], back.at[pl.ds(0, peers)], 5, (near, f))
    own_over = copy(got.at[:, 5], other, 2, (near, f))
    far_over = copy(beside, beside2, 4, (near, f))

    def shift(s, carry):
        begin = start[s]
        low, high = lax.rem(begin, SIDE), lax.div(begin, SIDE)
        for q in range(2):
            firsts[s, SIDE * q:SIDE * (q + 1), :] = first[q, pl.ds(low, SIDE), :].astype(BF16)
        w0, w1 = turn[0, pl.ds(low, SIDE), :], turn[1, pl.ds(low, SIDE), :]
        r0, r1 = jump[0, pl.ds(high, 1), :], jump[1, pl.ds(high, 1), :]
        turns[s, 0] = w0 * r0 - w1 * r1
        turns[s, 1] = w0 * r1 + w1 * r0
        return carry

    lax.fori_loop(0, SEGS, shift, 0)

    @pl.when(late == 1)
    def _():
        to_far.wait_recv()
        for _, o in far_first((GROUP,)):
            copy(chunk, beside.at[f], 3, (g, at(o))).start()
        wings[1, f] = chunk[...]

    all_group.wait_recv()
    own_over.start()

    left = lax.broadcasted_iota(jnp.int32, (ACROSS, 128), 1) < SIDE

    def swapped(x):
        return pltpu.roll(x, SIDE, 1)

    def prepare(u, unpacked):
        for p in (2 * u, 2 * u + 1):
            for q in sorted({p // 4, (p + PAIRS) // 4} - unpacked):
                unpacked.add(q)
                for i in range(ACROSS):
                    flat[24 * i + 4 * q:24 * i + 4 * q + 4, :] = got[i, q].astype(F32)
            one = flat[pl.ds(p, ACROSS, stride=24), :]
            two = flat[pl.ds(p + PAIRS, ACROSS, stride=24), :]
            re = jnp.where(left, one, swapped(two))
            im = jnp.where(left, swapped(one), two)
            bank[p, 0] = re
            bank[p, 1] = im
            level = jnp.sum(re * re + im * im, axis=0, keepdims=True)
            norm[8 * p:8 * (p + 1), :] = jnp.broadcast_to(level, (8, 128))

    def place(source, home):
        for i in range(ACROSS):
            loose[4 * i:4 * i + 4, :] = source(i).astype(F32)
        for q in range(4):
            row = loose[pl.ds(q, ACROSS, stride=4), :]
            turned = swapped(row)
            strain[4 * home + q, 0] = jnp.where(left, row, turned)
            strain[4 * home + q, 1] = jnp.where(left, turned, row)

    table2 = second[...]

    def across(u, home, dst):
        held = [(bank[2 * u + i, 0], bank[2 * u + i, 1]) for i in range(2)]
        for q in range(2):
            for k in range(2):
                s = 4 * home + q + 2 * k
                d0, d1 = strain[s, 0], strain[s, 1]
                crosses = [
                    jnp.concatenate([h0 * d0 + h1 * d1, h0 * d1 - h1 * d0], 0).astype(BF16) for h0, h1 in held
                ]
                y = jnp.dot(firsts[s], jnp.concatenate(crosses, 1), preferred_element_type=F32)
                w0, w1 = turns[s, 0], turns[s, 1]
                for i in range(2):
                    re, im = y[:SIDE, 128 * i:128 * (i + 1)], y[SIDE:, 128 * i:128 * (i + 1)]
                    dst[2 * i + q, :, 256 * k:256 * k + 128] = (re * w0 - im * w1).astype(BF16)
                    dst[2 * i + q, :, 256 * k + 128:256 * k + 256] = (re * w1 + im * w0).astype(BF16)

    def along(u, home, src):
        z = jnp.dot(src[...].reshape(4 * SIDE, 512), table2, preferred_element_type=F32)
        for n in range(4):
            re, im = z[SIDE * n:SIDE * (n + 1), 0:128], z[SIDE * n:SIDE * (n + 1), 128:256]
            row = 16 * u + 8 * (n // 2) + 2 * home + n % 2
            peak[pl.ds(row, 1), :] = jnp.max(re * re + im * im, axis=0, keepdims=True)

    def far_arrived():
        @pl.when(late == 0)
        def _():
            all_beside.wait_recv()

        @pl.when(late == 1)
        def _():
            most_beside.wait_recv()

        far_over.start()

    def run(order, arrive):
        unpacked = set()
        steps = [(u, n) for n in range(4) for u in range(PAIRS // 2)]
        mids = (mid, mid2)
        for step, (u, n) in enumerate(steps):
            home, part = order[n]
            if u == 0:
                arrive(n)
                place(part, home)
            if n == 0:
                prepare(u, unpacked)
            across(u, home, mids[step % 2])
            if step > 0:
                along(steps[step - 1][0], order[steps[step - 1][1]][0], mids[(step - 1) % 2])
            if step == 12:
                power = norm[...].T
                for k in range(2):
                    total[k:k + 1, :] = jnp.sum(power[SIDE * k:SIDE * (k + 1)], axis=0, keepdims=True)
        along(PAIRS // 2 - 1, order[3][0], mids[(len(steps) - 1) % 2])

    @pl.when(core == 0)
    def _():
        def arrive(n):
            if n == 0:
                own_over.wait_recv()
            if n == 2:
                far_arrived()
            if n == 3:
                far_over.wait_recv()

        run(
            (
                (g, lambda i: got[i, 5]), (near, lambda i: wings[0, i]),
                (far, lambda i: wings[1, i]), (across_g, lambda i: wings[2, i]),
            ), arrive,
        )

    @pl.when(core == 1)
    def _():
        def arrive(n):
            if n == 1:
                @pl.when(late == 1)
                def _():
                    own_over.wait_recv()

                @pl.when(late == 0)
                def _():
                    all_beside.wait_recv()
                    far_over.start()

            if n == 2:
                @pl.when(late == 1)
                def _():
                    most_beside.wait_recv()
                    far_over.start()

                @pl.when(late == 0)
                def _():
                    own_over.wait_recv()

            if n == 3:
                far_over.wait_recv()

        run(
            (
                (g, lambda i: got[i, 5]), (near + swap * (far - near), lambda i: wings[swap, i]),
                (far + swap * (near - far), lambda i: wings[1 - swap, i]), (across_g, lambda i: wings[2, i]),
            ), arrive,
        )

    best = (peak[...] * jump[0, 40:41, :]).T
    for k in range(4):
        sent[k:k + 1, :] = jnp.max(best[32 * k:32 * (k + 1)], axis=0, keepdims=True) / total[k % 2:k % 2 + 1, :]
    back[f] = sent[...]

    for _, o in far_first((GROUP,)):
        copy(sent, back.at[f], 5, (g, at(o))).start()
    for whole in (all_group, own_over, far_over):
        whole.wait_send()

    @pl.when(late == 0)
    def _():
        to_far.wait_send()

    @pl.when(late == 1)
    def _():
        all_beside.wait_send()
        most_beside.wait_send()

    all_shared.wait_recv()

    for i in range(count):
        for k in range(4):
            wide[32 * k + i:32 * k + i + 1, :] = back[i, k:k + 1, :]
    turned = wide[...].T
    lane = lax.broadcasted_iota(jnp.int32, (8, 128), 1)
    row = lax.broadcasted_iota(jnp.int32, (8, 128), 0)
    for c in range(5):
        blocks = []
        for k in range(2):
            block = None
            for n in range(4):
                q, p = divmod(4 * c + n, PAIRS)
                piece = turned[8 * p:8 * (p + 1), :]
                shift = (32 * n - 32 * q - 64 * k) % 128
                piece = pltpu.roll(piece, shift, 1) if shift else piece
                block = piece if block is None else jnp.where(lane >= 32 * n, piece, block)
            blocks.append(block)
        one, two = blocks
        for n, shifts in enumerate(((0, 2, 2, 4), (4, 6, 6, 0))):
            moved = [pltpu.roll(x, d, 0) if d else x for x, d in zip((one, two, one, two), shifts)]
            low = jnp.where(row < 2, moved[0], moved[1])
            high = jnp.where(row < 6, moved[2], moved[3])
            out_ref[8 * n:8 * (n + 1), 128 * c:128 * (c + 1)] = jnp.where(row < 4, low, high)

    all_shared.wait_send()


def on_device(spectra, templates, valid_start):
    first, turn, jump, second = tables()
    anywhere = pl.BlockSpec(memory_space=pl.ANY)
    dma = pltpu.SemaphoreType.DMA
    out = pl.pallas_call(
        kernel,
        out_shape=pltpu.VMEM((SEGS, 640), F32),
        in_specs=[anywhere] * 7,
        out_specs=pl.BlockSpec(memory_space=pltpu.VMEM),
        scratch_shapes=[
            pltpu.SMEM((SEGS,), jnp.int32),
            pltpu.VMEM((64, 2, 640), BF16),
            pltpu.VMEM((2, 4, 64), BF16),
            pltpu.VMEM(first.shape, F32),
            pltpu.VMEM(turn.shape, F32),
            pltpu.VMEM(jump.shape, F32),
            pltpu.VMEM(second.shape, BF16),
            pltpu.VMEM((640, 128), F32),
            pltpu.VMEM((32, 6, 4, 128), BF16),
            pltpu.VMEM((32, 6, 4, 128), BF16),
            pltpu.VMEM((4, 128), BF16),
            pltpu.VMEM((3, 32, 4, 128), BF16),
            pltpu.VMEM((32 * 24, 128), F32),
            pltpu.VMEM((32 * 4, 128), F32),
            pltpu.VMEM((PAIRS, 2, ACROSS, 128), F32),
            pltpu.VMEM((SEGS, 2, ACROSS, 128), F32),
            pltpu.VMEM((SEGS, 128, 64), BF16),
            pltpu.VMEM((SEGS, 2, SIDE, 128), F32),
            pltpu.VMEM((4, SIDE, 512), BF16),
            pltpu.VMEM((4, SIDE, 512), BF16),
            pltpu.VMEM((128, 128), F32),
            pltpu.VMEM((128, 128), F32),
            pltpu.VMEM((2, 128), F32),
            pltpu.VMEM((4, 128), F32),
            pltpu.VMEM((32, 4, 128), F32),
            pltpu.VMEM((128, 128), F32),
            dma((7,)),
            dma((6,)),
            dma((6,)),
        ],
        compiler_params=pltpu.CompilerParams(collective_id=0, has_side_effects=True),
        name="matched_filter",
    )(valid_start, templates, jnp.transpose(spectra, (1, 2, 0)), first, turn, jump, second)
    return out.T


def solution(mesh):
    return jax.shard_map(
        on_device, mesh=mesh, in_specs=(P("freq", None, "group"), P("freq", None, "group"), P()),
        out_specs=P("group", None), check_vma=False,
    )
```

```python
import math

import jax
import jax.numpy as jnp
import numpy as np
from jax import lax
from jax.experimental import pallas as pl
from jax.experimental.pallas import tpu as pltpu
from jax.sharding import PartitionSpec as P

N = 4096
VALID = 2048
SIDE = 64
ACROSS = 32
PAIRS = 10
SEGS = 16
MESH = pl.DeviceIdType.MESH
F32 = jnp.float32
BF16 = jnp.bfloat16


def rounded_roots(index):
    exact = np.exp(2j * np.pi * (index % SIDE) / SIDE)
    least = np.full(index.shape[0], np.inf)
    table = np.zeros_like(exact)
    gain = np.ones(index.shape[0])
    for scale in np.linspace(1.0, 2.0, 2001)[:-1]:
        parts = [(x * scale).astype(jnp.bfloat16).astype(np.float64) for x in (exact.real, exact.imag)]
        tried = parts[0] + 1j * parts[1]
        level = (tried * exact.conj()).mean(1).real
        rest = (np.abs(tried / level[:, None] - exact) ** 2).mean(1)
        better = rest < least - 1e-15
        least = np.where(better, rest, least)
        table = np.where(better[:, None], tried, table)
        gain = np.where(better, level, gain)
    return table, gain


def tables():
    side = np.arange(SIDE)
    root, gain = rounded_roots(side[:, None] * np.arange(ACROSS)[None, :])
    first = np.stack([np.concatenate([root.real, -root.imag], 1), np.concatenate([root.imag, root.real], 1)], 0)
    first = np.tile(first, (1, 2, 1))
    lag = np.arange(2 * SIDE)
    turn = np.exp(2j * np.pi * lag[:, None] * side[None, :] / N) / np.tile(gain, 2)[:, None]
    turn = np.tile(np.stack([turn.real, turn.imag], 0), (1, 1, 2))
    root, gain = rounded_roots(side[:VALID // SIDE, None] * side[None, :])
    c, s = np.kron(np.eye(2), root.real.T), np.kron(np.eye(2), root.imag.T)
    none = np.zeros_like(c)
    second = np.concatenate(
        [
            np.concatenate([c, none, s, none], 1), np.concatenate([-s, none, c, none], 1),
            np.concatenate([none, c, none, s], 1), np.concatenate([none, -s, none, c], 1),
        ], 0,
    )
    jump = np.exp(2j * np.pi * np.arange(40)[:, None] * side[None, :] / SIDE)
    jump = np.tile(np.stack([jump.real, jump.imag], 0), (1, 1, 2))
    weight = np.tile(1.0 / gain ** 2, (2, 8, 4))
    jump = np.concatenate([jump, weight], 1)
    return jnp.asarray(first, F32), jnp.asarray(turn, F32), jnp.asarray(jump, F32), jnp.asarray(second, BF16)


def far_first(kinds, first=3):
    def hops(entry):
        (kind, (dz, dx, dy)) = entry
        return min(dz, 4 - dz) + min(dx, 4 - dx) + (2 - dy if kind == FAR else dy)

    offsets = [(dz, dx, dy) for dz in range(4) for dx in range(4) for dy in range(2)]
    entries = [(kind, o) for o in offsets for kind in kinds if (kind, o) != (GROUP, (0, 0, 0))]
    def order(entry):
        (kind, (dz, dx, _)) = entry
        return -hops(entry) - 0.6 * (dz == first) - 0.6 * (dx == first), kinds.index(kind)

    return sorted(entries, key=order)


GROUP, FAR = range(2)


def kernel(
    start_hbm, tpl_hbm, spec_hbm, first_hbm, turn_hbm, jump_hbm, second_hbm, out_ref,
    start, tpl, spec, first, turn, jump, second, rows, mine, got, chunk, wings, flat, loose,
    bank, strain, firsts, turns, mid, mid2, peak, norm, total, sent, back, wide,
    load_sem, send_sem, recv_sem,
):
    g = lax.axis_index("group")
    f = lax.axis_index("freq")
    far = lax.rem(g + 2, 4)
    near = g + 1 - 2 * lax.rem(g, 2)
    count = 32
    peers = count - 1
    z, x, y = f // 8, lax.rem(f, 8) // 2, lax.rem(f, 2)
    part_z = [8 * lax.rem(z + d, 4) for d in range(4)]
    part_x = [2 * lax.rem(x + d, 4) for d in range(4)]
    part_y = [y, 1 - y]

    def at(offset):
        return part_z[offset[0]] + part_x[offset[1]] + part_y[offset[2]]

    loads = [
        pltpu.make_async_copy(src, dst, load_sem.at[i])
        for i, (src, dst) in enumerate(
            [
                (tpl_hbm, tpl), (spec_hbm, spec), (start_hbm, start),
                (first_hbm, first), (turn_hbm, turn), (jump_hbm, jump), (second_hbm, second),
            ]
        )
    ]
    for load in loads:
        load.start()

    barrier = pltpu.get_barrier_semaphore()
    across_g = lax.rem(near + 2, 4)
    late = g // 2
    core = lax.rem(g, 2)
    swap = core * (1 - late)
    other, beside, beside2 = (wings.at[k] for k in range(3))
    group_of = (g, far)
    pl.semaphore_signal(barrier, inc=1, device_id=(far, f), device_id_type=MESH)
    for _, o in far_first((GROUP,), 1):
        pl.semaphore_signal(barrier, inc=1, device_id=(g, at(o)), device_id_type=MESH)
    pl.semaphore_signal(barrier, inc=1, device_id=(near, f), device_id_type=MESH)

    @pl.when(late == 0)
    def _():
        for _, o in far_first((FAR,), 1):
            if o != (0, 0, 0):
                pl.semaphore_signal(barrier, inc=1, device_id=(far, at(o)), device_id_type=MESH)

    for load in loads:
        load.wait()

    peak[...] = jnp.zeros_like(peak)
    norm[...] = jnp.ones_like(norm)

    for j in range(5):
        block = jnp.concatenate(
            [tpl[:, q, 128 * j:128 * (j + 1)].astype(F32) for q in range(2)], 0
        )
        rows[128 * j:128 * (j + 1), :] = block.T
    own = jnp.concatenate([spec[0].astype(F32), spec[1].astype(F32)], 1).astype(BF16)

    def fill(i, carry):
        for q in range(5):
            mine[i, q] = rows[pl.ds(i + 128 * q, 4, stride=32), :].astype(BF16)
        mine[i, 5] = own
        return carry

    lax.fori_loop(0, count, fill, 0)

    got[f] = mine[f]

    pl.semaphore_wait(barrier, count + 1 + peers * late)

    def copy(src, dst, kind, to):
        return pltpu.make_async_remote_copy(
            src_ref=src, dst_ref=dst, send_sem=send_sem.at[kind], recv_sem=recv_sem.at[kind],
            device_id=to, device_id_type=MESH,
        )

    own_chunk = mine.at[f, 5]
    to_far = copy(own_chunk, chunk, 0, (far, f))

    def give(kind, to):
        if kind == GROUP:
            return copy(mine.at[to], got.at[f], 1, (g, to))
        return copy(own_chunk, beside.at[f], 3, (far, to))

    @pl.when(late == 0)
    def _():
        to_far.start()
        for kind, o in far_first((GROUP,)):
            give(kind, at(o)).start()

    @pl.when(late == 1)
    def _():
        for kind, o in far_first((GROUP, FAR)):
            give(kind, at(o)).start()

    all_group = copy(mine.at[pl.ds(0, peers)], got.at[pl.ds(0, peers)], 1, (near, f))
    all_beside = copy(beside, beside, 3, (near, f))
    most_beside = copy(beside.at[pl.ds(0, peers)], beside.at[pl.ds(0, peers)], 3, (near, f))
    all_shared = copy(back.at[pl.ds(0, peers)], back.at[pl.ds(0, peers)], 5, (near, f))
    own_over = copy(got.at[:, 5], other, 2, (near, f))
    far_over = copy(beside, beside2, 4, (near, f))

    def shift(s, carry):
        begin = start[s]
        low, high = lax.rem(begin, SIDE), lax.div(begin, SIDE)
        for q in range(2):
            firsts[s, SIDE * q:SIDE * (q + 1), :] = first[q, pl.ds(low, SIDE), :].astype(BF16)
        w0, w1 = turn[0, pl.ds(low, SIDE), :], turn[1, pl.ds(low, SIDE), :]
        r0, r1 = jump[0, pl.ds(high, 1), :], jump[1, pl.ds(high, 1), :]
        turns[s, 0] = w0 * r0 - w1 * r1
        turns[s, 1] = w0 * r1 + w1 * r0
        return carry

    lax.fori_loop(0, SEGS, shift, 0)

    @pl.when(late == 1)
    def _():
        to_far.wait_recv()
        for _, o in far_first((GROUP,)):
            copy(chunk, beside.at[f], 3, (g, at(o))).start()
        wings[1, f] = chunk[...]

    all_group.wait_recv()
    own_over.start()

    left = lax.broadcasted_iota(jnp.int32, (ACROSS, 128), 1) < SIDE

    def swapped(x):
        return pltpu.roll(x, SIDE, 1)

    def prepare(u, unpacked):
        for p in (2 * u, 2 * u + 1):
            for q in sorted({p // 4, (p + PAIRS) // 4} - unpacked):
                unpacked.add(q)
                for i in range(ACROSS):
                    flat[24 * i + 4 * q:24 * i + 4 * q + 4, :] = got[i, q].astype(F32)
            one = flat[pl.ds(p, ACROSS, stride=24), :]
            two = flat[pl.ds(p + PAIRS, ACROSS, stride=24), :]
            re = jnp.where(left, one, swapped(two))
            im = jnp.where(left, swapped(one), two)
            bank[p, 0] = re
            bank[p, 1] = im
            level = jnp.sum(re * re + im * im, axis=0, keepdims=True)
            norm[8 * p:8 * (p + 1), :] = jnp.broadcast_to(level, (8, 128))

    def place(source, home):
        for i in range(ACROSS):
            loose[4 * i:4 * i + 4, :] = source(i).astype(F32)
        for q in range(4):
            row = loose[pl.ds(q, ACROSS, stride=4), :]
            turned = swapped(row)
            strain[4 * home + q, 0] = jnp.where(left, row, turned)
            strain[4 * home + q, 1] = jnp.where(left, turned, row)

    table2 = second[...]

    def across(u, home, dst):
        held = [(bank[2 * u + i, 0], bank[2 * u + i, 1]) for i in range(2)]
        for q in range(2):
            for k in range(2):
                s = 4 * home + q + 2 * k
                d0, d1 = strain[s, 0], strain[s, 1]
                crosses = [
                    jnp.concatenate([h0 * d0 + h1 * d1, h0 * d1 - h1 * d0], 0).astype(BF16) for h0, h1 in held
                ]
                y = jnp.dot(firsts[s], jnp.concatenate(crosses, 1), preferred_element_type=F32)
                w0, w1 = turns[s, 0], turns[s, 1]
                for i in range(2):
                    re, im = y[:SIDE, 128 * i:128 * (i + 1)], y[SIDE:, 128 * i:128 * (i + 1)]
                    dst[2 * i + q, :, 256 * k:256 * k + 128] = (re * w0 - im * w1).astype(BF16)
                    dst[2 * i + q, :, 256 * k + 128:256 * k + 256] = (re * w1 + im * w0).astype(BF16)

    def along(u, home, src):
        z = jnp.dot(src[...].reshape(4 * SIDE, 512), table2, preferred_element_type=F32)
        for n in range(4):
            re, im = z[SIDE * n:SIDE * (n + 1), 0:128], z[SIDE * n:SIDE * (n + 1), 128:256]
            row = 16 * u + 8 * (n // 2) + 2 * home + n % 2
            peak[pl.ds(row, 1), :] = jnp.max(re * re + im * im, axis=0, keepdims=True)

    def far_arrived():
        @pl.when(late == 0)
        def _():
            all_beside.wait_recv()

        @pl.when(late == 1)
        def _():
            most_beside.wait_recv()

        far_over.start()

    def run(order, arrive):
        unpacked = set()
        steps = [(u, n) for n in range(4) for u in range(PAIRS // 2)]
        mids = (mid, mid2)
        for step, (u, n) in enumerate(steps):
            home, part = order[n]
            if u == 0:
                arrive(n)
                place(part, home)
            if n == 0:
                prepare(u, unpacked)
            across(u, home, mids[step % 2])
            if step > 0:
                along(steps[step - 1][0], order[steps[step - 1][1]][0], mids[(step - 1) % 2])
            if step == 12:
                power = norm[...].T
                for k in range(2):
                    total[k:k + 1, :] = jnp.sum(power[SIDE * k:SIDE * (k + 1)], axis=0, keepdims=True)
        along(PAIRS // 2 - 1, order[3][0], mids[(len(steps) - 1) % 2])

    @pl.when(core == 0)
    def _():
        def arrive(n):
            if n == 0:
                own_over.wait_recv()
            if n == 2:
                far_arrived()
            if n == 3:
                far_over.wait_recv()

        run(
            (
                (g, lambda i: got[i, 5]), (near, lambda i: wings[0, i]),
                (far, lambda i: wings[1, i]), (across_g, lambda i: wings[2, i]),
            ), arrive,
        )

    @pl.when(core == 1)
    def _():
        def arrive(n):
            if n == 1:
                @pl.when(late == 1)
                def _():
                    own_over.wait_recv()

                @pl.when(late == 0)
                def _():
                    all_beside.wait_recv()
                    far_over.start()

            if n == 2:
                @pl.when(late == 1)
                def _():
                    most_beside.wait_recv()
                    far_over.start()

                @pl.when(late == 0)
                def _():
                    own_over.wait_recv()

            if n == 3:
                far_over.wait_recv()

        run(
            (
                (g, lambda i: got[i, 5]), (near + swap * (far - near), lambda i: wings[swap, i]),
                (far + swap * (near - far), lambda i: wings[1 - swap, i]), (across_g, lambda i: wings[2, i]),
            ), arrive,
        )

    best = (peak[...] * jump[0, 40:41, :]).T
    for k in range(4):
        sent[k:k + 1, :] = jnp.max(best[32 * k:32 * (k + 1)], axis=0, keepdims=True) / total[k % 2:k % 2 + 1, :]
    back[f] = sent[...]

    for _, o in far_first((GROUP,), 1):
        copy(sent, back.at[f], 5, (g, at(o))).start()
    for whole in (all_group, own_over, far_over):
        whole.wait_send()

    @pl.when(late == 0)
    def _():
        to_far.wait_send()

    @pl.when(late == 1)
    def _():
        all_beside.wait_send()
        most_beside.wait_send()

    all_shared.wait_recv()

    for i in range(count):
        for k in range(4):
            wide[32 * k + i:32 * k + i + 1, :] = back[i, k:k + 1, :]
    turned = wide[...].T
    lane = lax.broadcasted_iota(jnp.int32, (8, 128), 1)
    row = lax.broadcasted_iota(jnp.int32, (8, 128), 0)
    for c in range(5):
        blocks = []
        for k in range(2):
            block = None
            for n in range(4):
                q, p = divmod(4 * c + n, PAIRS)
                piece = turned[8 * p:8 * (p + 1), :]
                shift = (32 * n - 32 * q - 64 * k) % 128
                piece = pltpu.roll(piece, shift, 1) if shift else piece
                block = piece if block is None else jnp.where(lane >= 32 * n, piece, block)
            blocks.append(block)
        one, two = blocks
        for n, shifts in enumerate(((0, 2, 2, 4), (4, 6, 6, 0))):
            moved = [pltpu.roll(x, d, 0) if d else x for x, d in zip((one, two, one, two), shifts)]
            low = jnp.where(row < 2, moved[0], moved[1])
            high = jnp.where(row < 6, moved[2], moved[3])
            out_ref[8 * n:8 * (n + 1), 128 * c:128 * (c + 1)] = jnp.where(row < 4, low, high)

    all_shared.wait_send()


def on_device(spectra, templates, valid_start):
    first, turn, jump, second = tables()
    anywhere = pl.BlockSpec(memory_space=pl.ANY)
    dma = pltpu.SemaphoreType.DMA
    out = pl.pallas_call(
        kernel,
        out_shape=pltpu.VMEM((SEGS, 640), F32),
        in_specs=[anywhere] * 7,
        out_specs=pl.BlockSpec(memory_space=pltpu.VMEM),
        scratch_shapes=[
            pltpu.SMEM((SEGS,), jnp.int32),
            pltpu.VMEM((64, 2, 640), BF16),
            pltpu.VMEM((2, 4, 64), BF16),
            pltpu.VMEM(first.shape, F32),
            pltpu.VMEM(turn.shape, F32),
            pltpu.VMEM(jump.shape, F32),
            pltpu.VMEM(second.shape, BF16),
            pltpu.VMEM((640, 128), F32),
            pltpu.VMEM((32, 6, 4, 128), BF16),
            pltpu.VMEM((32, 6, 4, 128), BF16),
            pltpu.VMEM((4, 128), BF16),
            pltpu.VMEM((3, 32, 4, 128), BF16),
            pltpu.VMEM((32 * 24, 128), F32),
            pltpu.VMEM((32 * 4, 128), F32),
            pltpu.VMEM((PAIRS, 2, ACROSS, 128), F32),
            pltpu.VMEM((SEGS, 2, ACROSS, 128), F32),
            pltpu.VMEM((SEGS, 128, 64), BF16),
            pltpu.VMEM((SEGS, 2, SIDE, 128), F32),
            pltpu.VMEM((4, SIDE, 512), BF16),
            pltpu.VMEM((4, SIDE, 512), BF16),
            pltpu.VMEM((128, 128), F32),
            pltpu.VMEM((128, 128), F32),
            pltpu.VMEM((2, 128), F32),
            pltpu.VMEM((4, 128), F32),
            pltpu.VMEM((32, 4, 128), F32),
            pltpu.VMEM((128, 128), F32),
            dma((7,)),
            dma((6,)),
            dma((6,)),
        ],
        compiler_params=pltpu.CompilerParams(collective_id=0, has_side_effects=True),
        name="matched_filter",
    )(valid_start, templates, jnp.transpose(spectra, (1, 2, 0)), first, turn, jump, second)
    return out.T


def solution(mesh):
    return jax.shard_map(
        on_device, mesh=mesh, in_specs=(P("freq", None, "group"), P("freq", None, "group"), P()),
        out_specs=P("group", None), check_vma=False,
    )
```

```python
import math

import jax
import jax.numpy as jnp
import numpy as np
from jax import lax
from jax.experimental import pallas as pl
from jax.experimental.pallas import tpu as pltpu
from jax.sharding import PartitionSpec as P

N = 4096
VALID = 2048
SIDE = 64
ACROSS = 32
PAIRS = 10
SEGS = 16
MESH = pl.DeviceIdType.MESH
F32 = jnp.float32
BF16 = jnp.bfloat16


def rounded_roots(index):
    exact = np.exp(2j * np.pi * (index % SIDE) / SIDE)
    least = np.full(index.shape[0], np.inf)
    table = np.zeros_like(exact)
    gain = np.ones(index.shape[0])
    for scale in np.linspace(1.0, 2.0, 2001)[:-1]:
        parts = [(x * scale).astype(jnp.bfloat16).astype(np.float64) for x in (exact.real, exact.imag)]
        tried = parts[0] + 1j * parts[1]
        level = (tried * exact.conj()).mean(1).real
        rest = (np.abs(tried / level[:, None] - exact) ** 2).mean(1)
        better = rest < least - 1e-15
        least = np.where(better, rest, least)
        table = np.where(better[:, None], tried, table)
        gain = np.where(better, level, gain)
    return table, gain


def tables():
    side = np.arange(SIDE)
    root, gain = rounded_roots(side[:, None] * np.arange(ACROSS)[None, :])
    first = np.stack([np.concatenate([root.real, -root.imag], 1), np.concatenate([root.imag, root.real], 1)], 0)
    first = np.tile(first, (1, 2, 1))
    lag = np.arange(2 * SIDE)
    turn = np.exp(2j * np.pi * lag[:, None] * side[None, :] / N) / np.tile(gain, 2)[:, None]
    turn = np.tile(np.stack([turn.real, turn.imag], 0), (1, 1, 2))
    root, gain = rounded_roots(side[:VALID // SIDE, None] * side[None, :])
    c, s = np.kron(np.eye(2), root.real.T), np.kron(np.eye(2), root.imag.T)
    none = np.zeros_like(c)
    second = np.concatenate(
        [
            np.concatenate([c, none, s, none], 1), np.concatenate([-s, none, c, none], 1),
            np.concatenate([none, c, none, s], 1), np.concatenate([none, -s, none, c], 1),
        ], 0,
    )
    jump = np.exp(2j * np.pi * np.arange(40)[:, None] * side[None, :] / SIDE)
    jump = np.tile(np.stack([jump.real, jump.imag], 0), (1, 1, 2))
    weight = np.tile(1.0 / gain ** 2, (2, 8, 4))
    jump = np.concatenate([jump, weight], 1)
    return jnp.asarray(first, F32), jnp.asarray(turn, F32), jnp.asarray(jump, F32), jnp.asarray(second, BF16)


def far_first(kinds, first=3):
    def hops(entry):
        (kind, (dz, dx, dy)) = entry
        return min(dz, 4 - dz) + min(dx, 4 - dx) + (2 - dy if kind == FAR else dy)

    offsets = [(dz, dx, dy) for dz in range(4) for dx in range(4) for dy in range(2)]
    entries = [(kind, o) for o in offsets for kind in kinds if (kind, o) != (GROUP, (0, 0, 0))]
    def order(entry):
        (kind, (dz, dx, _)) = entry
        return -hops(entry) - 0.45 * (dz == first) - 0.45 * (dx == first), kinds.index(kind)

    return sorted(entries, key=order)


GROUP, FAR = range(2)


def kernel(
    start_hbm, tpl_hbm, spec_hbm, first_hbm, turn_hbm, jump_hbm, second_hbm, out_ref,
    start, tpl, spec, first, turn, jump, second, rows, mine, got, chunk, wings, flat, loose,
    bank, strain, firsts, turns, mid, mid2, peak, norm, total, sent, back, wide,
    load_sem, send_sem, recv_sem,
):
    g = lax.axis_index("group")
    f = lax.axis_index("freq")
    far = lax.rem(g + 2, 4)
    near = g + 1 - 2 * lax.rem(g, 2)
    count = 32
    peers = count - 1
    z, x, y = f // 8, lax.rem(f, 8) // 2, lax.rem(f, 2)
    part_z = [8 * lax.rem(z + d, 4) for d in range(4)]
    part_x = [2 * lax.rem(x + d, 4) for d in range(4)]
    part_y = [y, 1 - y]

    def at(offset):
        return part_z[offset[0]] + part_x[offset[1]] + part_y[offset[2]]

    loads = [
        pltpu.make_async_copy(src, dst, load_sem.at[i])
        for i, (src, dst) in enumerate(
            [
                (tpl_hbm, tpl), (spec_hbm, spec), (start_hbm, start),
                (first_hbm, first), (turn_hbm, turn), (jump_hbm, jump), (second_hbm, second),
            ]
        )
    ]
    for load in loads:
        load.start()

    barrier = pltpu.get_barrier_semaphore()
    across_g = lax.rem(near + 2, 4)
    late = g // 2
    core = lax.rem(g, 2)
    swap = core * (1 - late)
    other, beside, beside2 = (wings.at[k] for k in range(3))
    group_of = (g, far)
    pl.semaphore_signal(barrier, inc=1, device_id=(far, f), device_id_type=MESH)
    for _, o in far_first((GROUP,), 1):
        pl.semaphore_signal(barrier, inc=1, device_id=(g, at(o)), device_id_type=MESH)
    pl.semaphore_signal(barrier, inc=1, device_id=(near, f), device_id_type=MESH)

    @pl.when(late == 0)
    def _():
        for _, o in far_first((FAR,), 1):
            if o != (0, 0, 0):
                pl.semaphore_signal(barrier, inc=1, device_id=(far, at(o)), device_id_type=MESH)

    for load in loads:
        load.wait()

    peak[...] = jnp.zeros_like(peak)
    norm[...] = jnp.ones_like(norm)

    for j in range(5):
        block = jnp.concatenate(
            [tpl[:, q, 128 * j:128 * (j + 1)].astype(F32) for q in range(2)], 0
        )
        rows[128 * j:128 * (j + 1), :] = block.T
    own = jnp.concatenate([spec[0].astype(F32), spec[1].astype(F32)], 1).astype(BF16)

    def fill(i, carry):
        for q in range(5):
            mine[i, q] = rows[pl.ds(i + 128 * q, 4, stride=32), :].astype(BF16)
        mine[i, 5] = own
        return carry

    lax.fori_loop(0, count, fill, 0)

    got[f] = mine[f]

    pl.semaphore_wait(barrier, count + 1 + peers * late)

    def copy(src, dst, kind, to):
        return pltpu.make_async_remote_copy(
            src_ref=src, dst_ref=dst, send_sem=send_sem.at[kind], recv_sem=recv_sem.at[kind],
            device_id=to, device_id_type=MESH,
        )

    own_chunk = mine.at[f, 5]
    to_far = copy(own_chunk, chunk, 0, (far, f))

    def give(kind, to):
        if kind == GROUP:
            return copy(mine.at[to], got.at[f], 1, (g, to))
        return copy(own_chunk, beside.at[f], 3, (far, to))

    @pl.when(late == 0)
    def _():
        to_far.start()
        for kind, o in far_first((GROUP,)):
            give(kind, at(o)).start()

    @pl.when(late == 1)
    def _():
        for kind, o in far_first((GROUP, FAR)):
            give(kind, at(o)).start()

    all_group = copy(mine.at[pl.ds(0, peers)], got.at[pl.ds(0, peers)], 1, (near, f))
    all_beside = copy(beside, beside, 3, (near, f))
    most_beside = copy(beside.at[pl.ds(0, peers)], beside.at[pl.ds(0, peers)], 3, (near, f))
    all_shared = copy(back.at[pl.ds(0, peers)], back.at[pl.ds(0, peers)], 5, (near, f))
    own_over = copy(got.at[:, 5], other, 2, (near, f))
    far_over = copy(beside, beside2, 4, (near, f))

    def shift(s, carry):
        begin = start[s]
        low, high = lax.rem(begin, SIDE), lax.div(begin, SIDE)
        for q in range(2):
            firsts[s, SIDE * q:SIDE * (q + 1), :] = first[q, pl.ds(low, SIDE), :].astype(BF16)
        w0, w1 = turn[0, pl.ds(low, SIDE), :], turn[1, pl.ds(low, SIDE), :]
        r0, r1 = jump[0, pl.ds(high, 1), :], jump[1, pl.ds(high, 1), :]
        turns[s, 0] = w0 * r0 - w1 * r1
        turns[s, 1] = w0 * r1 + w1 * r0
        return carry

    lax.fori_loop(0, SEGS, shift, 0)

    @pl.when(late == 1)
    def _():
        to_far.wait_recv()
        for _, o in far_first((GROUP,)):
            copy(chunk, beside.at[f], 3, (g, at(o))).start()
        wings[1, f] = chunk[...]

    all_group.wait_recv()
    own_over.start()

    left = lax.broadcasted_iota(jnp.int32, (ACROSS, 128), 1) < SIDE

    def swapped(x):
        return pltpu.roll(x, SIDE, 1)

    def prepare(u, unpacked):
        for p in (2 * u, 2 * u + 1):
            for q in sorted({p // 4, (p + PAIRS) // 4} - unpacked):
                unpacked.add(q)
                for i in range(ACROSS):
                    flat[24 * i + 4 * q:24 * i + 4 * q + 4, :] = got[i, q].astype(F32)
            one = flat[pl.ds(p, ACROSS, stride=24), :]
            two = flat[pl.ds(p + PAIRS, ACROSS, stride=24), :]
            re = jnp.where(left, one, swapped(two))
            im = jnp.where(left, swapped(one), two)
            bank[p, 0] = re
            bank[p, 1] = im
            level = jnp.sum(re * re + im * im, axis=0, keepdims=True)
            norm[8 * p:8 * (p + 1), :] = jnp.broadcast_to(level, (8, 128))

    def place(source, home):
        for i in range(ACROSS):
            loose[4 * i:4 * i + 4, :] = source(i).astype(F32)
        for q in range(4):
            row = loose[pl.ds(q, ACROSS, stride=4), :]
            turned = swapped(row)
            strain[4 * home + q, 0] = jnp.where(left, row, turned)
            strain[4 * home + q, 1] = jnp.where(left, turned, row)

    table2 = second[...]

    def across(u, home, dst):
        held = [(bank[2 * u + i, 0], bank[2 * u + i, 1]) for i in range(2)]
        for q in range(2):
            for k in range(2):
                s = 4 * home + q + 2 * k
                d0, d1 = strain[s, 0], strain[s, 1]
                crosses = [
                    jnp.concatenate([h0 * d0 + h1 * d1, h0 * d1 - h1 * d0], 0).astype(BF16) for h0, h1 in held
                ]
                y = jnp.dot(firsts[s], jnp.concatenate(crosses, 1), preferred_element_type=F32)
                w0, w1 = turns[s, 0], turns[s, 1]
                for i in range(2):
                    re, im = y[:SIDE, 128 * i:128 * (i + 1)], y[SIDE:, 128 * i:128 * (i + 1)]
                    dst[2 * i + q, :, 256 * k:256 * k + 128] = (re * w0 - im * w1).astype(BF16)
                    dst[2 * i + q, :, 256 * k + 128:256 * k + 256] = (re * w1 + im * w0).astype(BF16)

    def along(u, home, src):
        z = jnp.dot(src[...].reshape(4 * SIDE, 512), table2, preferred_element_type=F32)
        for n in range(4):
            re, im = z[SIDE * n:SIDE * (n + 1), 0:128], z[SIDE * n:SIDE * (n + 1), 128:256]
            row = 16 * u + 8 * (n // 2) + 2 * home + n % 2
            peak[pl.ds(row, 1), :] = jnp.max(re * re + im * im, axis=0, keepdims=True)

    def far_arrived():
        @pl.when(late == 0)
        def _():
            all_beside.wait_recv()

        @pl.when(late == 1)
        def _():
            most_beside.wait_recv()

        far_over.start()

    def run(order, arrive):
        unpacked = set()
        steps = [(u, n) for n in range(4) for u in range(PAIRS // 2)]
        mids = (mid, mid2)
        for step, (u, n) in enumerate(steps):
            home, part = order[n]
            if u == 0:
                arrive(n)
                place(part, home)
            if n == 0:
                prepare(u, unpacked)
            across(u, home, mids[step % 2])
            if step > 0:
                along(steps[step - 1][0], order[steps[step - 1][1]][0], mids[(step - 1) % 2])
            if step == 12:
                power = norm[...].T
                for k in range(2):
                    total[k:k + 1, :] = jnp.sum(power[SIDE * k:SIDE * (k + 1)], axis=0, keepdims=True)
        along(PAIRS // 2 - 1, order[3][0], mids[(len(steps) - 1) % 2])

    @pl.when(core == 0)
    def _():
        def arrive(n):
            if n == 0:
                own_over.wait_recv()
            if n == 2:
                far_arrived()
            if n == 3:
                far_over.wait_recv()

        run(
            (
                (g, lambda i: got[i, 5]), (near, lambda i: wings[0, i]),
                (far, lambda i: wings[1, i]), (across_g, lambda i: wings[2, i]),
            ), arrive,
        )

    @pl.when(core == 1)
    def _():
        def arrive(n):
            if n == 1:
                @pl.when(late == 1)
                def _():
                    own_over.wait_recv()

                @pl.when(late == 0)
                def _():
                    all_beside.wait_recv()
                    far_over.start()

            if n == 2:
                @pl.when(late == 1)
                def _():
                    most_beside.wait_recv()
                    far_over.start()

                @pl.when(late == 0)
                def _():
                    own_over.wait_recv()

            if n == 3:
                far_over.wait_recv()

        run(
            (
                (g, lambda i: got[i, 5]), (near + swap * (far - near), lambda i: wings[swap, i]),
                (far + swap * (near - far), lambda i: wings[1 - swap, i]), (across_g, lambda i: wings[2, i]),
            ), arrive,
        )

    best = (peak[...] * jump[0, 40:41, :]).T
    for k in range(4):
        sent[k:k + 1, :] = jnp.max(best[32 * k:32 * (k + 1)], axis=0, keepdims=True) / total[k % 2:k % 2 + 1, :]
    back[f] = sent[...]

    for _, o in far_first((GROUP,), 1):
        copy(sent, back.at[f], 5, (g, at(o))).start()
    for whole in (all_group, own_over, far_over):
        whole.wait_send()

    @pl.when(late == 0)
    def _():
        to_far.wait_send()

    @pl.when(late == 1)
    def _():
        all_beside.wait_send()
        most_beside.wait_send()

    all_shared.wait_recv()

    for i in range(count):
        for k in range(4):
            wide[32 * k + i:32 * k + i + 1, :] = back[i, k:k + 1, :]
    turned = wide[...].T
    lane = lax.broadcasted_iota(jnp.int32, (8, 128), 1)
    row = lax.broadcasted_iota(jnp.int32, (8, 128), 0)
    for c in range(5):
        blocks = []
        for k in range(2):
            block = None
            for n in range(4):
                q, p = divmod(4 * c + n, PAIRS)
                piece = turned[8 * p:8 * (p + 1), :]
                shift = (32 * n - 32 * q - 64 * k) % 128
                piece = pltpu.roll(piece, shift, 1) if shift else piece
                block = piece if block is None else jnp.where(lane >= 32 * n, piece, block)
            blocks.append(block)
        one, two = blocks
        for n, shifts in enumerate(((0, 2, 2, 4), (4, 6, 6, 0))):
            moved = [pltpu.roll(x, d, 0) if d else x for x, d in zip((one, two, one, two), shifts)]
            low = jnp.where(row < 2, moved[0], moved[1])
            high = jnp.where(row < 6, moved[2], moved[3])
            out_ref[8 * n:8 * (n + 1), 128 * c:128 * (c + 1)] = jnp.where(row < 4, low, high)

    all_shared.wait_send()


def on_device(spectra, templates, valid_start):
    first, turn, jump, second = tables()
    anywhere = pl.BlockSpec(memory_space=pl.ANY)
    dma = pltpu.SemaphoreType.DMA
    out = pl.pallas_call(
        kernel,
        out_shape=pltpu.VMEM((SEGS, 640), F32),
        in_specs=[anywhere] * 7,
        out_specs=pl.BlockSpec(memory_space=pltpu.VMEM),
        scratch_shapes=[
            pltpu.SMEM((SEGS,), jnp.int32),
            pltpu.VMEM((64, 2, 640), BF16),
            pltpu.VMEM((2, 4, 64), BF16),
            pltpu.VMEM(first.shape, F32),
            pltpu.VMEM(turn.shape, F32),
            pltpu.VMEM(jump.shape, F32),
            pltpu.VMEM(second.shape, BF16),
            pltpu.VMEM((640, 128), F32),
            pltpu.VMEM((32, 6, 4, 128), BF16),
            pltpu.VMEM((32, 6, 4, 128), BF16),
            pltpu.VMEM((4, 128), BF16),
            pltpu.VMEM((3, 32, 4, 128), BF16),
            pltpu.VMEM((32 * 24, 128), F32),
            pltpu.VMEM((32 * 4, 128), F32),
            pltpu.VMEM((PAIRS, 2, ACROSS, 128), F32),
            pltpu.VMEM((SEGS, 2, ACROSS, 128), F32),
            pltpu.VMEM((SEGS, 128, 64), BF16),
            pltpu.VMEM((SEGS, 2, SIDE, 128), F32),
            pltpu.VMEM((4, SIDE, 512), BF16),
            pltpu.VMEM((4, SIDE, 512), BF16),
            pltpu.VMEM((128, 128), F32),
            pltpu.VMEM((128, 128), F32),
            pltpu.VMEM((2, 128), F32),
            pltpu.VMEM((4, 128), F32),
            pltpu.VMEM((32, 4, 128), F32),
            pltpu.VMEM((128, 128), F32),
            dma((7,)),
            dma((6,)),
            dma((6,)),
        ],
        compiler_params=pltpu.CompilerParams(collective_id=0, has_side_effects=True),
        name="matched_filter",
    )(valid_start, templates, jnp.transpose(spectra, (1, 2, 0)), first, turn, jump, second)
    return out.T


def solution(mesh):
    return jax.shard_map(
        on_device, mesh=mesh, in_specs=(P("freq", None, "group"), P("freq", None, "group"), P()),
        out_specs=P("group", None), check_vma=False,
    )
```

```python
import math

import jax
import jax.numpy as jnp
import numpy as np
from jax import lax
from jax.experimental import pallas as pl
from jax.experimental.pallas import tpu as pltpu
from jax.sharding import PartitionSpec as P

N = 4096
VALID = 2048
SIDE = 64
ACROSS = 32
PAIRS = 10
SEGS = 16
MESH = pl.DeviceIdType.MESH
F32 = jnp.float32
BF16 = jnp.bfloat16


def rounded_roots(index):
    exact = np.exp(2j * np.pi * (index % SIDE) / SIDE)
    least = np.full(index.shape[0], np.inf)
    table = np.zeros_like(exact)
    gain = np.ones(index.shape[0])
    for scale in np.linspace(1.0, 2.0, 2001)[:-1]:
        parts = [(x * scale).astype(jnp.bfloat16).astype(np.float64) for x in (exact.real, exact.imag)]
        tried = parts[0] + 1j * parts[1]
        level = (tried * exact.conj()).mean(1).real
        rest = (np.abs(tried / level[:, None] - exact) ** 2).mean(1)
        better = rest < least - 1e-15
        least = np.where(better, rest, least)
        table = np.where(better[:, None], tried, table)
        gain = np.where(better, level, gain)
    return table, gain


def tables():
    side = np.arange(SIDE)
    root, gain = rounded_roots(side[:, None] * np.arange(ACROSS)[None, :])
    first = np.stack([np.concatenate([root.real, -root.imag], 1), np.concatenate([root.imag, root.real], 1)], 0)
    first = np.tile(first, (1, 2, 1))
    lag = np.arange(2 * SIDE)
    turn = np.exp(2j * np.pi * lag[:, None] * side[None, :] / N) / np.tile(gain, 2)[:, None]
    turn = np.tile(np.stack([turn.real, turn.imag], 0), (1, 1, 2))
    root, gain = rounded_roots(side[:VALID // SIDE, None] * side[None, :])
    c, s = np.kron(np.eye(2), root.real.T), np.kron(np.eye(2), root.imag.T)
    none = np.zeros_like(c)
    second = np.concatenate(
        [
            np.concatenate([c, none, s, none], 1), np.concatenate([-s, none, c, none], 1),
            np.concatenate([none, c, none, s], 1), np.concatenate([none, -s, none, c], 1),
        ], 0,
    )
    jump = np.exp(2j * np.pi * np.arange(40)[:, None] * side[None, :] / SIDE)
    jump = np.tile(np.stack([jump.real, jump.imag], 0), (1, 1, 2))
    weight = np.tile(1.0 / gain ** 2, (2, 8, 4))
    jump = np.concatenate([jump, weight], 1)
    return jnp.asarray(first, F32), jnp.asarray(turn, F32), jnp.asarray(jump, F32), jnp.asarray(second, BF16)


def far_first(kinds, first=3):
    def hops(entry):
        (kind, (dz, dx, dy)) = entry
        return min(dz, 4 - dz) + min(dx, 4 - dx) + (2 - dy if kind == FAR else dy)

    offsets = [(dz, dx, dy) for dz in range(4) for dx in range(4) for dy in range(2)]
    entries = [(kind, o) for o in offsets for kind in kinds if (kind, o) != (GROUP, (0, 0, 0))]
    def order(entry):
        (kind, (dz, dx, _)) = entry
        return -hops(entry) - 0.6 * (dz == first) - 0.6 * (dx == first), kinds.index(kind)

    return sorted(entries, key=order)


GROUP, FAR = range(2)


def kernel(
    start_hbm, tpl_hbm, spec_hbm, first_hbm, turn_hbm, jump_hbm, second_hbm, out_ref,
    start, tpl, spec, first, turn, jump, second, rows, mine, got, chunk, wings, flat, loose,
    bank, strain, firsts, turns, mid, mid2, peak, norm, total, sent, back,
    load_sem, send_sem, recv_sem,
):
    g = lax.axis_index("group")
    f = lax.axis_index("freq")
    far = lax.rem(g + 2, 4)
    near = g + 1 - 2 * lax.rem(g, 2)
    count = 32
    peers = count - 1
    z, x, y = f // 8, lax.rem(f, 8) // 2, lax.rem(f, 2)
    part_z = [8 * lax.rem(z + d, 4) for d in range(4)]
    part_x = [2 * lax.rem(x + d, 4) for d in range(4)]
    part_y = [y, 1 - y]

    def at(offset):
        return part_z[offset[0]] + part_x[offset[1]] + part_y[offset[2]]

    loads = [
        pltpu.make_async_copy(src, dst, load_sem.at[i])
        for i, (src, dst) in enumerate(
            [
                (tpl_hbm, tpl), (spec_hbm, spec), (start_hbm, start),
                (first_hbm, first), (turn_hbm, turn), (jump_hbm, jump), (second_hbm, second),
            ]
        )
    ]
    for load in loads:
        load.start()

    barrier = pltpu.get_barrier_semaphore()
    across_g = lax.rem(near + 2, 4)
    late = g // 2
    core = lax.rem(g, 2)
    swap = core * (1 - late)
    other, beside, beside2 = (wings.at[k] for k in range(3))
    group_of = (g, far)
    pl.semaphore_signal(barrier, inc=1, device_id=(far, f), device_id_type=MESH)
    for _, o in far_first((GROUP,), 1):
        pl.semaphore_signal(barrier, inc=1, device_id=(g, at(o)), device_id_type=MESH)
    pl.semaphore_signal(barrier, inc=1, device_id=(near, f), device_id_type=MESH)

    @pl.when(late == 0)
    def _():
        for _, o in far_first((FAR,), 1):
            if o != (0, 0, 0):
                pl.semaphore_signal(barrier, inc=1, device_id=(far, at(o)), device_id_type=MESH)

    for load in loads:
        load.wait()

    peak[...] = jnp.zeros_like(peak)
    norm[...] = jnp.ones_like(norm)

    for j in range(5):
        block = jnp.concatenate(
            [tpl[:, q, 128 * j:128 * (j + 1)].astype(F32) for q in range(2)], 0
        )
        rows[128 * j:128 * (j + 1), :] = block.T
    own = jnp.concatenate([spec[0].astype(F32), spec[1].astype(F32)], 1).astype(BF16)

    def fill(i, carry):
        for q in range(5):
            mine[i, q] = rows[pl.ds(i + 128 * q, 4, stride=32), :].astype(BF16)
        mine[i, 5] = own
        return carry

    lax.fori_loop(0, count, fill, 0)

    got[f] = mine[f]

    pl.semaphore_wait(barrier, count + 1 + peers * late)

    def copy(src, dst, kind, to):
        return pltpu.make_async_remote_copy(
            src_ref=src, dst_ref=dst, send_sem=send_sem.at[kind], recv_sem=recv_sem.at[kind],
            device_id=to, device_id_type=MESH,
        )

    own_chunk = mine.at[f, 5]
    to_far = copy(own_chunk, chunk, 0, (far, f))

    def give(kind, to):
        if kind == GROUP:
            return copy(mine.at[to], got.at[f], 1, (g, to))
        return copy(own_chunk, beside.at[f], 3, (far, to))

    @pl.when(late == 0)
    def _():
        to_far.start()
        for kind, o in far_first((GROUP,)):
            give(kind, at(o)).start()

    @pl.when(late == 1)
    def _():
        for kind, o in far_first((GROUP, FAR)):
            give(kind, at(o)).start()

    all_group = copy(mine.at[pl.ds(0, peers)], got.at[pl.ds(0, peers)], 1, (near, f))
    all_beside = copy(beside, beside, 3, (near, f))
    most_beside = copy(beside.at[pl.ds(0, peers)], beside.at[pl.ds(0, peers)], 3, (near, f))
    all_shared = copy(back.at[pl.ds(0, peers)], back.at[pl.ds(0, peers)], 5, (near, f))
    own_over = copy(got.at[:, 5], other, 2, (near, f))
    far_over = copy(beside, beside2, 4, (near, f))

    def shift(s, carry):
        begin = start[s]
        low, high = lax.rem(begin, SIDE), lax.div(begin, SIDE)
        for q in range(2):
            firsts[s, SIDE * q:SIDE * (q + 1), :] = first[q, pl.ds(low, SIDE), :].astype(BF16)
        w0, w1 = turn[0, pl.ds(low, SIDE), :], turn[1, pl.ds(low, SIDE), :]
        r0, r1 = jump[0, pl.ds(high, 1), :], jump[1, pl.ds(high, 1), :]
        turns[s, 0] = w0 * r0 - w1 * r1
        turns[s, 1] = w0 * r1 + w1 * r0
        return carry

    lax.fori_loop(0, SEGS, shift, 0)

    @pl.when(late == 1)
    def _():
        to_far.wait_recv()
        for _, o in far_first((GROUP,)):
            copy(chunk, beside.at[f], 3, (g, at(o))).start()
        wings[1, f] = chunk[...]

    all_group.wait_recv()
    own_over.start()

    left = lax.broadcasted_iota(jnp.int32, (ACROSS, 128), 1) < SIDE

    def swapped(x):
        return pltpu.roll(x, SIDE, 1)

    def prepare(u, unpacked):
        for p in (2 * u, 2 * u + 1):
            for q in sorted({p // 4, (p + PAIRS) // 4} - unpacked):
                unpacked.add(q)
                for i in range(ACROSS):
                    flat[24 * i + 4 * q:24 * i + 4 * q + 4, :] = got[i, q].astype(F32)
            one = flat[pl.ds(p, ACROSS, stride=24), :]
            two = flat[pl.ds(p + PAIRS, ACROSS, stride=24), :]
            re = jnp.where(left, one, swapped(two))
            im = jnp.where(left, swapped(one), two)
            bank[p, 0] = re
            bank[p, 1] = im
            level = jnp.sum(re * re + im * im, axis=0, keepdims=True)
            norm[8 * p:8 * (p + 1), :] = jnp.broadcast_to(level, (8, 128))

    def place(source, home):
        for i in range(ACROSS):
            loose[4 * i:4 * i + 4, :] = source(i).astype(F32)
        for q in range(4):
            row = loose[pl.ds(q, ACROSS, stride=4), :]
            turned = swapped(row)
            strain[4 * home + q, 0] = jnp.where(left, row, turned)
            strain[4 * home + q, 1] = jnp.where(left, turned, row)

    table2 = second[...]

    def across(u, home, dst):
        held = [(bank[2 * u + i, 0], bank[2 * u + i, 1]) for i in range(2)]
        for q in range(2):
            for k in range(2):
                s = 4 * home + q + 2 * k
                d0, d1 = strain[s, 0], strain[s, 1]
                crosses = [
                    jnp.concatenate([h0 * d0 + h1 * d1, h0 * d1 - h1 * d0], 0).astype(BF16) for h0, h1 in held
                ]
                y = jnp.dot(firsts[s], jnp.concatenate(crosses, 1), preferred_element_type=F32)
                w0, w1 = turns[s, 0], turns[s, 1]
                for i in range(2):
                    re, im = y[:SIDE, 128 * i:128 * (i + 1)], y[SIDE:, 128 * i:128 * (i + 1)]
                    dst[2 * i + q, :, 256 * k:256 * k + 128] = (re * w0 - im * w1).astype(BF16)
                    dst[2 * i + q, :, 256 * k + 128:256 * k + 256] = (re * w1 + im * w0).astype(BF16)

    def along(u, home, src):
        z = jnp.dot(src[...].reshape(4 * SIDE, 512), table2, preferred_element_type=F32)
        for n in range(4):
            re, im = z[SIDE * n:SIDE * (n + 1), 0:128], z[SIDE * n:SIDE * (n + 1), 128:256]
            row = 16 * u + 8 * (n // 2) + 2 * home + n % 2
            peak[pl.ds(row, 1), :] = jnp.max(re * re + im * im, axis=0, keepdims=True)

    def far_arrived():
        @pl.when(late == 0)
        def _():
            all_beside.wait_recv()

        @pl.when(late == 1)
        def _():
            most_beside.wait_recv()

        far_over.start()

    def run(order, arrive):
        unpacked = set()
        steps = [(u, n) for n in range(4) for u in range(PAIRS // 2)]
        mids = (mid, mid2)
        for step, (u, n) in enumerate(steps):
            home, part = order[n]
            if u == 0:
                arrive(n)
                place(part, home)
            if n == 0:
                prepare(u, unpacked)
            across(u, home, mids[step % 2])
            if step > 0:
                along(steps[step - 1][0], order[steps[step - 1][1]][0], mids[(step - 1) % 2])
            if step == 12:
                power = norm[...].T
                for k in range(2):
                    total[k:k + 1, :] = jnp.sum(power[SIDE * k:SIDE * (k + 1)], axis=0, keepdims=True)
        along(PAIRS // 2 - 1, order[3][0], mids[(len(steps) - 1) % 2])

    @pl.when(core == 0)
    def _():
        def arrive(n):
            if n == 0:
                own_over.wait_recv()
            if n == 2:
                far_arrived()
            if n == 3:
                far_over.wait_recv()

        run(
            (
                (g, lambda i: got[i, 5]), (near, lambda i: wings[0, i]),
                (far, lambda i: wings[1, i]), (across_g, lambda i: wings[2, i]),
            ), arrive,
        )

    @pl.when(core == 1)
    def _():
        def arrive(n):
            if n == 1:
                @pl.when(late == 1)
                def _():
                    own_over.wait_recv()

                @pl.when(late == 0)
                def _():
                    all_beside.wait_recv()
                    far_over.start()

            if n == 2:
                @pl.when(late == 1)
                def _():
                    most_beside.wait_recv()
                    far_over.start()

                @pl.when(late == 0)
                def _():
                    own_over.wait_recv()

            if n == 3:
                far_over.wait_recv()

        run(
            (
                (g, lambda i: got[i, 5]), (near + swap * (far - near), lambda i: wings[swap, i]),
                (far + swap * (near - far), lambda i: wings[1 - swap, i]), (across_g, lambda i: wings[2, i]),
            ), arrive,
        )

    best = (peak[...] * jump[0, 40:41, :]).T
    for k in range(4):
        sent[k:k + 1, :] = jnp.max(best[32 * k:32 * (k + 1)], axis=0, keepdims=True) / total[k % 2:k % 2 + 1, :]
    back[f] = sent[...]

    for _, o in far_first((GROUP,), 1):
        copy(sent, back.at[f], 5, (g, at(o))).start()
    for whole in (all_group, own_over, far_over):
        whole.wait_send()

    @pl.when(late == 0)
    def _():
        to_far.wait_send()

    @pl.when(late == 1)
    def _():
        all_beside.wait_send()
        most_beside.wait_send()

    all_shared.wait_recv()

    turned = jnp.concatenate([back[:, k, :] for k in range(4)], 0).T
    lane = lax.broadcasted_iota(jnp.int32, (8, 128), 1)
    row = lax.broadcasted_iota(jnp.int32, (8, 128), 0)
    for c in range(5):
        blocks = []
        for k in range(2):
            block = None
            for n in range(4):
                q, p = divmod(4 * c + n, PAIRS)
                piece = turned[8 * p:8 * (p + 1), :]
                shift = (32 * n - 32 * q - 64 * k) % 128
                piece = pltpu.roll(piece, shift, 1) if shift else piece
                block = piece if block is None else jnp.where(lane >= 32 * n, piece, block)
            blocks.append(block)
        one, two = blocks
        for n, shifts in enumerate(((0, 2, 2, 4), (4, 6, 6, 0))):
            moved = [pltpu.roll(x, d, 0) if d else x for x, d in zip((one, two, one, two), shifts)]
            low = jnp.where(row < 2, moved[0], moved[1])
            high = jnp.where(row < 6, moved[2], moved[3])
            out_ref[8 * n:8 * (n + 1), 128 * c:128 * (c + 1)] = jnp.where(row < 4, low, high)

    all_shared.wait_send()


def on_device(spectra, templates, valid_start):
    first, turn, jump, second = tables()
    anywhere = pl.BlockSpec(memory_space=pl.ANY)
    dma = pltpu.SemaphoreType.DMA
    out = pl.pallas_call(
        kernel,
        out_shape=pltpu.VMEM((SEGS, 640), F32),
        in_specs=[anywhere] * 7,
        out_specs=pl.BlockSpec(memory_space=pltpu.VMEM),
        scratch_shapes=[
            pltpu.SMEM((SEGS,), jnp.int32),
            pltpu.VMEM((64, 2, 640), BF16),
            pltpu.VMEM((2, 4, 64), BF16),
            pltpu.VMEM(first.shape, F32),
            pltpu.VMEM(turn.shape, F32),
            pltpu.VMEM(jump.shape, F32),
            pltpu.VMEM(second.shape, BF16),
            pltpu.VMEM((640, 128), F32),
            pltpu.VMEM((32, 6, 4, 128), BF16),
            pltpu.VMEM((32, 6, 4, 128), BF16),
            pltpu.VMEM((4, 128), BF16),
            pltpu.VMEM((3, 32, 4, 128), BF16),
            pltpu.VMEM((32 * 24, 128), F32),
            pltpu.VMEM((32 * 4, 128), F32),
            pltpu.VMEM((PAIRS, 2, ACROSS, 128), F32),
            pltpu.VMEM((SEGS, 2, ACROSS, 128), F32),
            pltpu.VMEM((SEGS, 128, 64), BF16),
            pltpu.VMEM((SEGS, 2, SIDE, 128), F32),
            pltpu.VMEM((4, SIDE, 512), BF16),
            pltpu.VMEM((4, SIDE, 512), BF16),
            pltpu.VMEM((128, 128), F32),
            pltpu.VMEM((128, 128), F32),
            pltpu.VMEM((2, 128), F32),
            pltpu.VMEM((4, 128), F32),
            pltpu.VMEM((32, 4, 128), F32),
            dma((7,)),
            dma((6,)),
            dma((6,)),
        ],
        compiler_params=pltpu.CompilerParams(collective_id=0, has_side_effects=True),
        name="matched_filter",
    )(valid_start, templates, jnp.transpose(spectra, (1, 2, 0)), first, turn, jump, second)
    return out.T


def solution(mesh):
    return jax.shard_map(
        on_device, mesh=mesh, in_specs=(P("freq", None, "group"), P("freq", None, "group"), P()),
        out_specs=P("group", None), check_vma=False,
    )
```
